32 devices in a mesh: dp: 8 (over z, x), seq: 4 (over y, core).
Axes of the slice: x: 2, y: 2, z: 4, core: 2. Of those that a mesh axis runs over, the one named last changes fastest.
Arguments:
- short_input: bfloat16 [192, 128, 1024], P(('dp', 'seq')), may hold values from -6 to 6
- long_input: bfloat16 [16, 512, 1024], P('dp', 'seq'), may hold values from -6 to 6
- short_cotangent: bfloat16 [192, 128, 1024], P(('dp', 'seq')), may hold values from -6 to 6
- long_cotangent: bfloat16 [16, 512, 1024], P('dp', 'seq'), may hold values from -6 to 6
- short_lengths: int32 [192], P(('dp', 'seq')), may hold values from 32 to 128, as said below
- long_lengths: int32 [16], P('dp'), may hold values from 128 to 512, as said below
- query_weight: float32 [1024, 1024], P(('dp', 'seq')), may hold values from -0.1875 to 0.1875
- key_weight: float32 [1024, 1024], P(('dp', 'seq')), may hold values from -0.1875 to 0.1875
- value_weight: float32 [1024, 1024], P(('dp', 'seq')), may hold values from -0.1875 to 0.1875
- output_weight: float32 [1024, 1024], P(('dp', 'seq')), may hold values from -0.75 to 0.75
- upward_weight: float32 [1024, 4096], P(('dp', 'seq')), may hold values from -0.1875 to 0.1875
- downward_weight: float32 [4096, 1024], P(('dp', 'seq')), may hold values from -0.09375 to 0.09375
- query_bias: float32 [1024], replicated, may hold values from -3 to 3
- value_bias: float32 [1024], replicated, may hold values from -3 to 3
- output_bias: float32 [1024], replicated, may hold values from -3 to 3
- upward_bias: float32 [4096], replicated, may hold values from -3 to 3
- downward_bias: float32 [1024], replicated, may hold values from -3 to 3
- first_gain: float32 [1024], replicated, may hold values from 0.25 to 1.75
- first_shift: float32 [1024], replicated, may hold values from -3 to 3
- second_gain: float32 [1024], replicated, may hold values from 0.25 to 1.75
- second_shift: float32 [1024], replicated, may hold values from -3 to 3
Outputs:
- short_output: bfloat16 [192, 128, 1024], P(('dp', 'seq'))
- long_output: bfloat16 [16, 512, 1024], P('dp', 'seq')
- short_grad: bfloat16 [192, 128, 1024], P(('dp', 'seq'))
- long_grad: bfloat16 [16, 512, 1024], P('dp', 'seq')
- query_delta: float32 [1024], replicated
- value_delta: float32 [1024], replicated
- output_delta: float32 [1024], replicated
- upward_delta: float32 [4096], replicated
- downward_delta: float32 [1024], replicated
- first_delta: float32 [1024], replicated
- second_delta: float32 [1024], replicated
The draws below stay inside these ranges and needn't reach their ends.
Inputs may be any that keep to these rules, and one draw needn't show every extreme that they name: `short_lengths`: some short sequence has all 128 positions. `long_lengths`: some long sequence has all 512 positions.
All inputs are finite; a program needn't handle non-finite values.
Results may differ from the reference program's by a relative error of at most 0.013.
The reference program's roundings to bfloat16 on the way count: a program that leaves them out, or rounds other values in their place, can miss the bound.
Values may be sent and summed in bfloat16 or wider, within the bound.
A program may use at most 192 MiB of HBM per device.

```python
import math
import jax
import jax.numpy as jnp
from jax import lax

D = 1024
HEADS = 16
HEAD = 64
FF = 4096
SHORT_LEN = 128
LONG_LEN = 512
NSHORT = 192
NLONG = 16


def draw_short_lengths(key, part):
    chosen = jax.random.randint(jax.random.fold_in(key, 11), (NSHORT,), SHORT_LEN // 4, SHORT_LEN + 1)
    filled = jax.random.randint(jax.random.fold_in(key, 12), (), 0, NSHORT)
    return chosen.at[filled].set(SHORT_LEN).astype(jnp.int32)


def draw_long_lengths(key, part):
    chosen = jax.random.randint(jax.random.fold_in(key, 21), (NLONG,), LONG_LEN // 4, LONG_LEN + 1)
    filled = jax.random.randint(jax.random.fold_in(key, 22), (), 0, NLONG)
    return chosen.at[filled].set(LONG_LEN).astype(jnp.int32)


def levels(own_key, extent, cuts, smallest, largest):
    level, own = 1.0, jax.random.fold_in(own_key, 6)
    for axis_at, shards_of in cuts:
        heights = jnp.exp(jax.random.uniform(jax.random.fold_in(own, axis_at), (shards_of,), jnp.float32, smallest / len(cuts), largest / len(cuts)))
        level = level * jnp.repeat(heights, extent[axis_at] // shards_of).reshape([-1 if axis == axis_at else 1 for axis in range(len(extent))])
    return level


def centred(rng, shape, deviation, most, pieces=(), kind=jnp.bfloat16):
    level = levels(rng, shape, pieces, -0.22, 0.18) if pieces else 1.0
    values = jax.random.normal(rng, shape, jnp.float32) * deviation * level
    return jnp.minimum(jnp.maximum(values, -most), most).astype(kind)


def setup_inputs(seed: int = 0) -> dict:
    key_list = jax.random.split(jax.random.key(seed), 22)
    return {
        "short_input": centred(key_list[0], (NSHORT, SHORT_LEN, D), 1.0, 6.0, ((0, 32),)),
        "long_input": centred(key_list[1], (NLONG, LONG_LEN, D), 1.0, 6.0, ((0, 8), (1, 4))),
        "short_cotangent": centred(key_list[2], (NSHORT, SHORT_LEN, D), 1.0, 6.0, ((0, 32),)),
        "long_cotangent": centred(key_list[3], (NLONG, LONG_LEN, D), 1.0, 6.0, ((0, 8), (1, 4))),
        "short_lengths": draw_short_lengths(jax.random.fold_in(key_list[21], 71), 0),
        "long_lengths": draw_long_lengths(jax.random.fold_in(key_list[21], 71), 0),
        "query_weight": centred(key_list[6], (D, D), D ** -0.5, 0.1875, ((0, 32),), jnp.float32),
        "key_weight": centred(key_list[7], (D, D), D ** -0.5, 0.1875, ((0, 32),), jnp.float32),
        "value_weight": centred(key_list[8], (D, D), D ** -0.5, 0.1875, ((0, 32),), jnp.float32),
        "output_weight": centred(key_list[9], (D, D), (D // 16) ** -0.5, 0.75, ((0, 32),), jnp.float32),
        "upward_weight": centred(key_list[10], (D, FF), D ** -0.5, 0.1875, ((0, 32),), jnp.float32),
        "downward_weight": centred(key_list[11], (FF, D), FF ** -0.5, 0.09375, ((0, 32),), jnp.float32),
        "query_bias": centred(key_list[12], (D,), 0.5, 3.0, (), jnp.float32),
        "value_bias": centred(key_list[13], (D,), 0.5, 3.0, (), jnp.float32),
        "output_bias": centred(key_list[14], (D,), 0.5, 3.0, (), jnp.float32),
        "upward_bias": centred(key_list[15], (FF,), 0.5, 3.0, (), jnp.float32),
        "downward_bias": centred(key_list[16], (D,), 0.5, 3.0, (), jnp.float32),
        "first_gain": jnp.clip(1.0 + 0.15 * jax.random.normal(key_list[17], (D,), jnp.float32), 0.25, 1.75),
        "first_shift": centred(key_list[18], (D,), 0.5, 3.0, (), jnp.float32),
        "second_gain": jnp.clip(1.0 + 0.15 * jax.random.normal(key_list[19], (D,), jnp.float32), 0.25, 1.75),
        "second_shift": centred(key_list[20], (D,), 0.5, 3.0, (), jnp.float32),
    }


epsilon = 1e-12
masked = -1e+30

@jax.custom_vjp
def low(v):
    return lax.optimization_barrier(v.astype(jnp.bfloat16)).astype(jnp.float32)

@jax.custom_vjp
def low_back(v):
    return v

def low_keep(v):
    return (low(v), None)

def low_pass(kept, grad):
    return (grad,)

def back_keep(v):
    return (v, None)

def back_low(kept, grad):
    return (low(grad),)
low.defvjp(low_keep, low_pass)
low_back.defvjp(back_keep, back_low)

def matmul(left, right):
    return jnp.matmul(left, right, precision=lax.Precision.HIGHEST)

def norm_apply(value, gain, shift):
    center = value - lax.optimization_barrier(jnp.mean(value, axis=-1, keepdims=True))
    spread = lax.optimization_barrier(jnp.mean(center * center, axis=-1, keepdims=True))
    return center * lax.rsqrt(spread + epsilon) * gain + shift

def block_forward(inputs, lengths, weights, params):
    query_weight, key_weight, value_weight, output_weight, upward_weight, downward_weight = weights
    query_bias, value_bias, output_bias, upward_bias, downward_bias, first_gain, first_shift, second_gain, second_shift = params
    number, seqlen, breadth = inputs.shape
    queries = low(low_back(matmul(inputs, query_weight)) + query_bias)
    key_rows = low(matmul(inputs, key_weight))
    values = low(matmul(inputs, value_weight) + value_bias)
    query_heads = queries.reshape(number, seqlen, HEADS, HEAD)
    key_heads = key_rows.reshape(number, seqlen, HEADS, HEAD)
    value_heads = values.reshape(number, seqlen, HEADS, HEAD)
    scores = low_back(jnp.einsum('nqhd,nkhd->nhqk', query_heads, key_heads, precision=lax.Precision.HIGHEST) * HEAD ** (-0.5))
    usable = jnp.arange(seqlen)[None, :] < lengths[:, None]
    scores = jnp.where(usable[:, None, None, :], scores, masked)
    attention = low(jax.nn.softmax(scores, axis=-1))
    blended = jnp.einsum('nhqk,nkhd->nqhd', attention, value_heads, precision=lax.Precision.HIGHEST)
    blended = low(low_back(blended.reshape(number, seqlen, breadth)))
    residual = inputs + low_back(matmul(blended, output_weight)) + output_bias
    normed = norm_apply(residual, first_gain, first_shift)
    pre_up = low_back(matmul(low(normed), upward_weight)) + upward_bias
    active = low(jax.nn.gelu(pre_up, approximate=True))
    ffn_sum = normed + low_back(matmul(active, downward_weight)) + downward_bias
    return norm_apply(ffn_sum, second_gain, second_shift)

def run_groups(inputs, lengths, weights, params, group_size):
    number = inputs.shape[0]
    shaped = inputs.reshape(number // group_size, group_size, inputs.shape[1], inputs.shape[2])
    length_rows = lengths.reshape(number // group_size, group_size)
    one_step = jax.checkpoint(lambda pair: block_forward(pair[0], pair[1], weights, params))
    results = lax.map(one_step, (shaped, length_rows))
    return results.reshape(inputs.shape)

def reference(short_input, long_input, short_cotangent, long_cotangent, short_lengths, long_lengths, query_weight, key_weight, value_weight, output_weight, upward_weight, downward_weight, query_bias, value_bias, output_bias, upward_bias, downward_bias, first_gain, first_shift, second_gain, second_shift):
    weights = tuple((w.astype(jnp.bfloat16).astype(jnp.float32) for w in (query_weight, key_weight, value_weight, output_weight, upward_weight, downward_weight)))
    short_group = math.gcd(NSHORT, max(1, 4096 // SHORT_LEN))
    long_group = math.gcd(NLONG, max(1, 4096 // LONG_LEN))

    def entire(short_x, long_x, q_bias, v_bias, o_bias, u_bias, d_bias, f_shift, s_shift):
        params = (q_bias, v_bias, o_bias, u_bias, d_bias, first_gain, f_shift, second_gain, s_shift)
        return (run_groups(short_x, short_lengths, weights, params, short_group), run_groups(long_x, long_lengths, weights, params, long_group))
    primal = (short_input.astype(jnp.float32), long_input.astype(jnp.float32), query_bias, value_bias, output_bias, upward_bias, downward_bias, first_shift, second_shift)
    (short_out, long_out), pullback = jax.vjp(entire, *primal)
    gradients = pullback((short_cotangent.astype(jnp.float32), long_cotangent.astype(jnp.float32)))
    return (short_out.astype(jnp.bfloat16), long_out.astype(jnp.bfloat16), gradients[0].astype(jnp.bfloat16), gradients[1].astype(jnp.bfloat16), gradients[2], gradients[3], gradients[4], gradients[5], gradients[6], gradients[7], gradients[8])
```

```python
import functools

import jax
import jax.numpy as jnp
from jax import lax
from jax.experimental import pallas as pl
from jax.experimental.pallas import tpu as pltpu
from jax.sharding import PartitionSpec as P

HEADS = 16
HEAD = 64


epsilon = 1e-12
masked = -1e30


def forward_product(left, right):
    return jnp.dot(left, right, preferred_element_type=jnp.float32)


def backward_product(left, right):
    return lax.dot_general(
        left, right, (((left.ndim - 1,), (1,)), ((), ())), preferred_element_type=jnp.float32
    )


def exact_backward(left, right):
    return lax.dot_general(
        left,
        right,
        (((left.ndim - 1,), (1,)), ((), ())),
        precision=lax.Precision.HIGHEST,
        preferred_element_type=jnp.float32,
    )


def norm_apply(value, gain, shift):
    center = value - jnp.mean(value, axis=-1, keepdims=True)
    spread = jnp.mean(center * center, axis=-1, keepdims=True)
    return center * lax.rsqrt(spread + epsilon) * gain + shift


def token_total(value):
    return jnp.sum(value, axis=(0, 1))


def keep_local(first_part, second_part):
    return (first_part, second_part)


def spread_long(key_rows, values):
    return (
        lax.all_gather(key_rows, "seq", axis=1, tiled=True),
        lax.all_gather(values, "seq", axis=1, tiled=True),
    )


def settle_each(value):
    return lax.psum(value, ("dp", "seq"))


def finish_local(key_terms, value_terms, key_exact, value_exact, settle):
    value_delta = settle(token_total(value_terms))
    through = exact_backward(key_terms, key_exact) + exact_backward(value_terms, value_exact)
    return (through, value_delta)


def finish_summed(key_terms, value_terms, key_exact, value_exact, settle):
    key_grad, value_grad = (
        lax.psum_scatter(
            key_terms.astype(jnp.bfloat16), "seq", scatter_dimension=1, tiled=True
        ).astype(jnp.float32),
        lax.psum_scatter(
            value_terms.astype(jnp.bfloat16), "seq", scatter_dimension=1, tiled=True
        ).astype(jnp.float32),
    )
    value_delta = settle(token_total(value_grad))
    through = exact_backward(key_grad, key_exact) + exact_backward(value_grad, value_exact)
    return (through, value_delta)


def recompute(inputs, usable, weights, params, spread):
    query_weight, key_weight, value_weight, output_weight, upward_weight, downward_weight = weights
    (
        query_bias,
        value_bias,
        output_bias,
        upward_bias,
        downward_bias,
        first_gain,
        first_shift,
        second_gain,
        second_shift,
    ) = params
    number, seqlen, breadth = inputs.shape
    queries = (forward_product(inputs, query_weight) + query_bias).astype(jnp.bfloat16)
    key_rows = forward_product(inputs, key_weight).astype(jnp.bfloat16)
    values = (forward_product(inputs, value_weight) + value_bias).astype(jnp.bfloat16)
    key_all, value_all = spread(key_rows, values)
    query_heads = queries.reshape(number, seqlen, HEADS, HEAD)
    key_heads = key_all.reshape(number, key_all.shape[1], HEADS, HEAD)
    value_heads = value_all.reshape(number, value_all.shape[1], HEADS, HEAD)
    scores = jnp.einsum(
        "nqhd,nkhd->nhqk", query_heads, key_heads, preferred_element_type=jnp.float32
    ) * HEAD ** (-0.5)
    scores = jnp.where(usable[:, None, None, :], scores, masked)
    attention = jax.nn.softmax(scores, axis=-1)
    attention_low = attention.astype(jnp.bfloat16)
    blended = jnp.einsum(
        "nhqk,nkhd->nqhd", attention_low, value_heads, preferred_element_type=jnp.float32
    )
    blended = blended.reshape(number, seqlen, breadth).astype(jnp.bfloat16)
    residual = inputs.astype(jnp.float32) + forward_product(blended, output_weight) + output_bias
    normed = norm_apply(residual, first_gain, first_shift)
    pre_up = forward_product(normed.astype(jnp.bfloat16), upward_weight) + upward_bias
    active = jax.nn.gelu(pre_up, approximate=True).astype(jnp.bfloat16)
    ffn_sum = normed + forward_product(active, downward_weight) + downward_bias
    output = norm_apply(ffn_sum, second_gain, second_shift)
    return (
        query_heads,
        key_heads,
        value_heads,
        attention,
        attention_low,
        residual,
        pre_up,
        ffn_sum,
        output,
    )


def backprop(inputs, cotangent, usable, weights, params, spread, finish, settle):
    (
        query_heads,
        key_heads,
        value_heads,
        attention,
        attention_low,
        residual,
        pre_up,
        ffn_sum,
        output,
    ) = recompute(inputs, usable, weights, params, spread)
    query_weight, key_weight, value_weight, output_weight, upward_weight, downward_weight = weights
    (
        query_bias,
        value_bias,
        output_bias,
        upward_bias,
        downward_bias,
        first_gain,
        first_shift,
        second_gain,
        second_shift,
    ) = params
    number, seqlen, breadth = inputs.shape
    upstream = cotangent.astype(jnp.float32)
    second_pull = jax.vjp(lambda value: norm_apply(value, second_gain, second_shift), ffn_sum)[1]
    ffn_grad = second_pull(upstream)[0]
    second_delta = settle(token_total(upstream))
    downward_delta = settle(token_total(ffn_grad))
    active_grad = backward_product(ffn_grad.astype(jnp.bfloat16), downward_weight)
    gelu_pull = jax.vjp(lambda value: jax.nn.gelu(value, approximate=True), pre_up)[1]
    pre_grad = gelu_pull(active_grad)[0]
    upward_delta = settle(token_total(pre_grad))
    normed_grad = ffn_grad + backward_product(pre_grad.astype(jnp.bfloat16), upward_weight)
    first_delta = settle(token_total(normed_grad))
    first_pull = jax.vjp(lambda value: norm_apply(value, first_gain, first_shift), residual)[1]
    residual_grad = first_pull(normed_grad)[0]
    output_delta = settle(token_total(residual_grad))
    blended_grad = backward_product(residual_grad.astype(jnp.bfloat16), output_weight).astype(
        jnp.bfloat16
    )
    blended_grad = blended_grad.reshape(number, seqlen, HEADS, HEAD)
    prob_grad = jnp.einsum(
        "nqhd,nkhd->nhqk", blended_grad, value_heads, preferred_element_type=jnp.float32
    )
    score_grad = attention * (prob_grad - jnp.sum(prob_grad * attention, axis=-1, keepdims=True))
    score_grad = score_grad.astype(jnp.bfloat16)
    query_grad = jnp.einsum(
        "nhqk,nkhd->nqhd", score_grad, key_heads, preferred_element_type=jnp.float32
    )
    query_grad = query_grad.reshape(number, seqlen, breadth) * HEAD ** (-0.5)
    key_terms = jnp.einsum(
        "nhqk,nqhd->nkhd", score_grad, query_heads, preferred_element_type=jnp.float32
    )
    key_terms = key_terms.reshape(number, key_heads.shape[1], breadth) * HEAD ** (-0.5)
    value_terms = jnp.einsum(
        "nhqk,nqhd->nkhd", attention_low, blended_grad, preferred_element_type=jnp.float32
    )
    value_terms = value_terms.reshape(number, value_heads.shape[1], breadth)
    key_exact = key_weight.astype(jnp.float32)
    value_exact = value_weight.astype(jnp.float32)
    through, value_delta = finish(key_terms, value_terms, key_exact, value_exact, settle)
    query_delta = settle(token_total(query_grad))
    input_grad = (
        residual_grad + backward_product(query_grad.astype(jnp.bfloat16), query_weight) + through
    )
    deltas = (
        query_delta,
        value_delta,
        output_delta,
        upward_delta,
        downward_delta,
        first_delta,
        second_delta,
    )
    return (input_grad.astype(jnp.bfloat16), deltas)


MESH = pl.DeviceIdType.MESH


def gather_kernel(depth, wide_ref, tall_ref, wide_out, tall_out, wide_buf, tall_buf, send_sem, recv_sem, own_sem, out_sem):
    dp = lax.axis_index("dp")
    seq = lax.axis_index("seq")
    z, x = dp // 2, dp % 2
    y, c = seq // 2, seq % 2
    x_peer = (z * 2 + (1 - x), seq)
    y_peer = (dp, (1 - y) * 2 + c)
    core_peer = (dp, y * 2 + (1 - c))
    z_peers = [(lax.rem(z + k, depth) * 2 + x, seq) for k in range(1, depth)]
    half = depth // 2
    wide_units = wide_ref.shape[0]
    units = wide_units + tall_ref.shape[0]
    hops = depth - 1

    own = []
    for u in range(units):
        src = wide_ref.at[u] if u < wide_units else tall_ref.at[u - wide_units]
        buf = wide_buf.at[u] if u < wide_units else tall_buf.at[u - wide_units]
        cp = pltpu.make_async_copy(src, buf.at[z, x, y, c], own_sem.at[u])
        cp.start()
        own.append(cp)

    barrier = pltpu.get_barrier_semaphore()
    peers = z_peers + [x_peer, y_peer, core_peer]
    for peer in peers:
        pl.semaphore_signal(barrier, inc=1, device_id=peer, device_id_type=MESH)
    pl.semaphore_wait(barrier, len(peers))

    def unit(u):
        if u < wide_units:
            return wide_ref.at[u], wide_buf.at[u], wide_out.at[u]
        return tall_ref.at[u - wide_units], tall_buf.at[u - wide_units], tall_out.at[u - wide_units]

    def remote(u, slot, src, dst, peer):
        return pltpu.make_async_remote_copy(
            src_ref=src, dst_ref=dst, send_sem=send_sem.at[u, slot], recv_sem=recv_sem.at[u, slot],
            device_id=peer, device_id_type=MESH)

    sends = {}

    def send(u, slot, part, peer):
        _, buf, _ = unit(u)
        cp = remote(u, slot, buf.at[part], buf.at[part], peer)
        cp.start()
        sends[u, slot] = cp

    lo, hi, every = pl.ds(0, half), pl.ds(half, depth - half), pl.ds(0, depth)
    both = pl.ds(0, 2)
    B0, B1, C0, C1, D0 = hops, hops + 1, hops + 2, hops + 3, hops + 4
    for u in range(units):
        src, buf, _ = unit(u)
        for k in range(hops):
            cp = remote(u, k, src, buf.at[z, x, y, c], z_peers[k])
            cp.start()
            sends[u, k] = cp

    def step_a(u):
        for k in range(hops):
            sends[u, k].wait_recv()
        own[u].wait()
        send(u, B0, (lo, x, y, c), x_peer)
        send(u, B1, (hi, x, y, c), y_peer)
        send(u, D0, (every, x, y, c), core_peer)

    def step_b(u):
        sends[u, B0].wait_recv()
        send(u, C0, (lo, both, y, c), y_peer)
        sends[u, B1].wait_recv()
        send(u, C1, (hi, x, both, c), x_peer)
        send(u, D0 + 1, (lo, 1 - x, y, c), core_peer)
        send(u, D0 + 2, (hi, x, 1 - y, c), core_peer)

    def step_c(u):
        sends[u, C0].wait_recv()
        send(u, D0 + 3, (lo, both, 1 - y, c), core_peer)
        sends[u, C1].wait_recv()
        send(u, D0 + 4, (hi, 1 - x, both, c), core_peer)

    def step_d(u):
        for k in range(5):
            sends[u, D0 + k].wait_recv()
        _, buf, out = unit(u)
        pltpu.make_async_copy(buf, out, out_sem.at[u]).start()

    for i in range(units + 3):
        if i < units:
            step_a(i)
        if 0 <= i - 1 < units:
            step_b(i - 1)
        if 0 <= i - 2 < units:
            step_c(i - 2)
        if 0 <= i - 3 < units:
            step_d(i - 3)
    for u in range(units):
        _, buf, out = unit(u)
        pltpu.make_async_copy(buf, out, out_sem.at[u]).wait()
        for slot in range(hops + 9):
            sends[u, slot].wait_send()


def gather_weights(wide, tall):
    dp = lax.axis_size("dp")
    depth = dp // 2
    lead = (depth, 2, 2, 2)
    wide_shape = (wide.shape[0], *lead, *wide.shape[1:])
    tall_shape = (tall.shape[0], *lead, *tall.shape[1:])
    units = wide.shape[0] + tall.shape[0]
    slots = depth + 8
    anywhere = pl.BlockSpec(memory_space=pl.ANY)
    return pl.pallas_call(
        functools.partial(gather_kernel, depth),
        out_shape=(jax.ShapeDtypeStruct(wide_shape, wide.dtype), jax.ShapeDtypeStruct(tall_shape, tall.dtype)),
        in_specs=[anywhere] * 2,
        out_specs=(anywhere,) * 2,
        scratch_shapes=[
            pltpu.VMEM(wide_shape, wide.dtype),
            pltpu.VMEM(tall_shape, tall.dtype),
            pltpu.SemaphoreType.DMA((units, slots)),
            pltpu.SemaphoreType.DMA((units, slots)),
            pltpu.SemaphoreType.DMA((units,)),
            pltpu.SemaphoreType.DMA((units,)),
        ],
        compiler_params=pltpu.CompilerParams(
            collective_id=0, has_side_effects=True, vmem_limit_bytes=60 * 2**20),
        name="gather_weights",
    )(wide, tall)


def gather_all(lows):
    query_low, key_low, value_low, output_low, upward_low, downward_low = lows
    rows, width = query_low.shape
    devices = lax.axis_size("dp") * lax.axis_size("seq")
    if rows % 16 or lax.axis_size("seq") != 4 or lax.axis_size("dp") % 4:
        return tuple(lax.all_gather(low, ("dp", "seq"), axis=0, tiled=True) for low in lows)
    strips = upward_low.shape[1] // width
    slim = width // 4
    wide = jnp.stack(
        [query_low, key_low, value_low, output_low]
        + [upward_low[:, i * width : (i + 1) * width] for i in range(strips)]
    )
    tall = jnp.stack([downward_low[:, i * slim : (i + 1) * slim] for i in range(4)])
    wide_all, tall_all = gather_weights(wide, tall)
    wide_all = wide_all.reshape(wide.shape[0], devices * rows, width)
    tall_all = tall_all.reshape(4, devices * downward_low.shape[0], slim)
    upward_all = jnp.concatenate([wide_all[4 + i] for i in range(strips)], axis=1)
    downward_all = jnp.concatenate([tall_all[i] for i in range(4)], axis=1)
    return (wide_all[0], wide_all[1], wide_all[2], wide_all[3], upward_all, downward_all)


def on_device(
    short_input,
    long_input,
    short_cotangent,
    long_cotangent,
    short_lengths,
    long_lengths,
    query_weight,
    key_weight,
    value_weight,
    output_weight,
    upward_weight,
    downward_weight,
    query_bias,
    value_bias,
    output_bias,
    upward_bias,
    downward_bias,
    first_gain,
    first_shift,
    second_gain,
    second_shift,
):
    params = (
        query_bias,
        value_bias,
        output_bias,
        upward_bias,
        downward_bias,
        first_gain,
        first_shift,
        second_gain,
        second_shift,
    )
    short_usable = jnp.arange(short_input.shape[1])[None, :] < short_lengths[:, None]
    long_span = long_input.shape[1] * lax.axis_size("seq")
    long_usable = jnp.arange(long_span)[None, :] < long_lengths[:, None]
    query_low = query_weight.astype(jnp.bfloat16)
    key_low = key_weight.astype(jnp.bfloat16)
    value_low = value_weight.astype(jnp.bfloat16)
    output_low = output_weight.astype(jnp.bfloat16)
    upward_low = upward_weight.astype(jnp.bfloat16)
    downward_low = downward_weight.astype(jnp.bfloat16)
    lows = (query_low, key_low, value_low, output_low, upward_low, downward_low)
    gathered = gather_all(lows)
    short_output = recompute(short_input, short_usable, gathered, params, keep_local)[-1]
    long_output = recompute(long_input, long_usable, gathered, params, spread_long)[-1]
    regathered = gathered
    short_grad, short_deltas = backprop(
        short_input,
        short_cotangent,
        short_usable,
        regathered,
        params,
        keep_local,
        finish_local,
        settle_each,
    )
    long_grad, long_deltas = backprop(
        long_input,
        long_cotangent,
        long_usable,
        regathered,
        params,
        spread_long,
        finish_summed,
        settle_each,
    )
    summed = tuple(
        (first_part + second_part for first_part, second_part in zip(short_deltas, long_deltas))
    )
    return (
        short_output.astype(jnp.bfloat16),
        long_output.astype(jnp.bfloat16),
        short_grad,
        long_grad,
        summed[0],
        summed[1],
        summed[2],
        summed[3],
        summed[4],
        summed[5],
        summed[6],
    )


def solution(mesh):
    placed = (
        P(("dp", "seq"), None, None),
        P("dp", "seq", None),
        P(("dp", "seq"), None, None),
        P("dp", "seq", None),
        P(("dp", "seq")),
        P("dp"),
        P(("dp", "seq"), None),
        P(("dp", "seq"), None),
        P(("dp", "seq"), None),
        P(("dp", "seq"), None),
        P(("dp", "seq"), None),
        P(("dp", "seq"), None),
        P(),
        P(),
        P(),
        P(),
        P(),
        P(),
        P(),
        P(),
        P(),
    )
    return jax.shard_map(
        on_device,
        mesh=mesh,
        in_specs=placed,
        out_specs=(
            P(("dp", "seq"), None, None),
            P("dp", "seq", None),
            P(("dp", "seq"), None, None),
            P("dp", "seq", None),
            P(),
            P(),
            P(),
            P(),
            P(),
            P(),
            P(),
        ),
        check_vma=False,
    )
```

```python
import functools

import jax
import jax.numpy as jnp
from jax import lax
from jax.experimental import pallas as pl
from jax.experimental.pallas import tpu as pltpu
from jax.sharding import PartitionSpec as P

MESH = pl.DeviceIdType.MESH
F32 = jnp.float32
BF16 = jnp.bfloat16
EPSILON = 1e-12
MASKED = -1e30
SCALE = 0.125
PAIR = 128
BLOCK = 128
CHUNK = 256
TILE = 256
K_UNIT, V_UNIT, Q_UNIT, O_UNIT, UP_UNIT = 0, 1, 2, 3, 4
Q_BIAS, V_BIAS, O_BIAS, D_BIAS, GAIN1, SHIFT1, GAIN2, SHIFT2, U_BIAS = 0, 1, 2, 3, 4, 5, 6, 7, 8
Q_SUM, V_SUM, O_SUM, D_SUM, F_SUM, S_SUM, U_SUM = 0, 1, 2, 3, 4, 5, 6
SUMS = 16


def dot_nn(a, b):
    return jnp.dot(a, b, preferred_element_type=F32)


def dot_nt(a, b):
    return lax.dot_general(a, b, (((1,), (1,)), ((), ())), preferred_element_type=F32)


def dot_tn(a, b):
    return lax.dot_general(a, b, (((0,), (0,)), ((), ())), preferred_element_type=F32)


def flipped(index, bit):
    return index + bit * (1 - 2 * ((index // bit) % 2))


def gelu(u):
    return 0.5 * u * (1.0 + jnp.tanh(0.7978845608028654 * (u + 0.044715 * (u * u * u))))


def gelu_slope(u):
    square = u * u
    t = jnp.tanh(0.7978845608028654 * (u + 0.044715 * (u * square)))
    return 0.5 * (1.0 + t) + 0.5 * u * (1.0 - t * t) * (0.7978845608028654 * (1.0 + 3 * 0.044715 * square))


def step_kernel(
    remote, dp_size, seq_size, nshort,
    wsh, xs, xl, dys, dyl, short_len, long_len, par,
    so, lo, sg, lg, sums,
    w, x, q, k, v, kv_sib, dkv_in, g, r, a16, u16, f, dy, acc, acc_in,
    send_sem, recv_sem, misc_send, misc_recv, own_sem, load_sem, store_sem,
):
    dp = lax.axis_index("dp")
    seq = lax.axis_index("seq")
    y, c = seq // 2, seq % 2
    y_peer = (dp, flipped(seq, 2))
    core_peer = (dp, flipped(seq, 1))
    total, width = x.shape
    short_rows = nshort * BLOCK
    units = w.shape[0]
    depth = w.shape[1]
    hidden_chunks = (units - 4) // 2
    partners = []
    bit = 1
    while bit < seq_size:
        partners.append((dp, flipped(seq, bit)))
        bit *= 2
    bit = 1
    while bit < dp_size:
        partners.append((flipped(dp, bit), seq))
        bit *= 2

    loads = [pltpu.make_async_copy(xs, x.at[pl.ds(0, short_rows)], load_sem.at[0]),
             pltpu.make_async_copy(xl.at[y], x.at[pl.ds(short_rows + BLOCK * y, BLOCK)], load_sem.at[1])]
    late = [pltpu.make_async_copy(dys, dy.at[pl.ds(0, short_rows)], load_sem.at[2]),
            pltpu.make_async_copy(dyl.at[y], dy.at[pl.ds(short_rows + BLOCK * y, BLOCK)], load_sem.at[3])]
    for cp in loads:
        cp.start()

    if remote:
        z, ax = dp // 2, dp % 2
        hops = depth - 1
        z_peers = [((z + n) % depth * 2 + ax, seq) for n in range(1, depth)]
        x_peer = (flipped(dp, 1), seq)
        peers = z_peers + [x_peer, y_peer, core_peer]
        own = [pltpu.make_async_copy(wsh.at[u], w.at[u, z, ax, y, c], own_sem.at[u]) for u in range(units)]
    else:
        peers = partners
        own = [pltpu.make_async_copy(wsh.at[u], w.at[u], own_sem.at[u]) for u in range(units)]
    for cp in own:
        cp.start()

    barrier = pltpu.get_barrier_semaphore()
    for peer in peers:
        pl.semaphore_signal(barrier, inc=1, device_id=peer, device_id_type=MESH)
    pl.semaphore_wait(barrier, len(peers))

    def misc(slot, src, dst, peer):
        return pltpu.make_async_remote_copy(
            src_ref=src, dst_ref=dst, send_sem=misc_send.at[slot], recv_sem=misc_recv.at[slot],
            device_id=peer, device_id_type=MESH)

    swap_x = misc(0, xl.at[1 - y], x.at[pl.ds(short_rows + BLOCK * y, BLOCK)], y_peer)
    swap_dy = misc(1, dyl.at[1 - y], dy.at[pl.ds(short_rows + BLOCK * y, BLOCK)], y_peer)
    swap_x.start()

    sends = {}
    if remote:
        half = depth // 2
        lower, upper, every, both = pl.ds(0, half), pl.ds(half, depth - half), pl.ds(0, depth), pl.ds(0, 2)
        B0, B1, C0, C1, D0 = hops, hops + 1, hops + 2, hops + 3, hops + 4

        def send(u, slot, src, part, peer):
            cp = pltpu.make_async_remote_copy(
                src_ref=src, dst_ref=w.at[(u, *part)], send_sem=send_sem.at[u, slot], recv_sem=recv_sem.at[u, slot],
                device_id=peer, device_id_type=MESH)
            cp.start()
            sends[u, slot] = cp

        def pass_on(u, slot, part, peer):
            send(u, slot, w.at[(u, *part)], part, peer)

        for u in range(units):
            for n in range(hops):
                send(u, n, wsh.at[u], (z, ax, y, c), z_peers[n])

        def step_a(u):
            for n in range(hops):
                sends[u, n].wait_recv()
            own[u].wait()
            pass_on(u, B0, (lower, ax, y, c), x_peer)
            pass_on(u, B1, (upper, ax, y, c), y_peer)
            pass_on(u, D0, (every, ax, y, c), core_peer)

        def step_b(u):
            sends[u, B0].wait_recv()
            pass_on(u, C0, (lower, both, y, c), y_peer)
            sends[u, B1].wait_recv()
            pass_on(u, C1, (upper, ax, both, c), x_peer)
            pass_on(u, D0 + 1, (lower, 1 - ax, y, c), core_peer)
            pass_on(u, D0 + 2, (upper, ax, 1 - y, c), core_peer)

        def step_c(u):
            sends[u, C0].wait_recv()
            pass_on(u, D0 + 3, (lower, both, 1 - y, c), core_peer)
            sends[u, C1].wait_recv()
            pass_on(u, D0 + 4, (upper, 1 - ax, both, c), core_peer)

        def step_d(u):
            for n in range(5):
                sends[u, D0 + n].wait_recv()

        def arrive(i):
            if i + 3 < units:
                step_a(i + 3)
            if i + 2 < units:
                step_b(i + 2)
            if i + 1 < units:
                step_c(i + 1)
            if i == units - 2:
                swap_dy.start()
            step_d(i)

        def warm_up():
            step_a(0)
            step_a(1)
            step_b(0)
            step_a(2)
            step_b(1)
            step_c(0)
    else:
        def arrive(i):
            if i == units - 2:
                swap_dy.start()
            own[i].wait()

        def warm_up():
            pass

    def columns(u, at):
        return w[u, :, :, :, :, :, at].reshape(width, CHUNK)

    def row_block(u, i):
        return w[u, i].reshape(CHUNK, width)

    def chunk(i):
        return pl.ds(pl.multiple_of(i * CHUNK, CHUNK), CHUNK)

    def tile(i):
        return pl.ds(pl.multiple_of(i * TILE, TILE), TILE)

    def project(u, dst, bias, scale):
        @pl.loop(0, width // CHUNK)
        def _(i):
            at = chunk(i)
            value = dot_nn(x[...], columns(u, at))
            if bias is not None:
                value = value + par[bias : bias + 1, at]
            if scale is not None:
                value = value * scale
            dst[:, at] = value.astype(BF16)

    lane = lax.broadcasted_iota(jnp.int32, (BLOCK, PAIR), 1)
    low_half = lane < PAIR // 2
    row_lane = lax.broadcasted_iota(jnp.int32, (1, PAIR), 1)
    first_head = jnp.where(row_lane < PAIR // 2, 1.0, 0.0).astype(BF16)
    second_head = jnp.where(row_lane < PAIR // 2, 0.0, 1.0).astype(BF16)

    def heads(value):
        return jnp.concatenate([value * first_head, value * second_head], axis=0)

    def merged(value):
        return jnp.where(low_half, value[:BLOCK], value[BLOCK:])

    def softmax(scores, usable):
        scores = jnp.where(usable, scores, MASKED)
        weight = jnp.exp(scores - jnp.max(scores, axis=1, keepdims=True))
        return weight * (1.0 / jnp.sum(weight, axis=1, keepdims=True))

    pairs = width // PAIR
    key_lane = lax.broadcasted_iota(jnp.int32, (2 * BLOCK, BLOCK), 1)
    own_rows = pl.ds(short_rows, 2 * BLOCK)

    def pair_at(h):
        return slice(h * PAIR, (h + 1) * PAIR)

    def short_forward(s):
        rows = pl.ds(pl.multiple_of(s * BLOCK, BLOCK), BLOCK)
        usable = key_lane < short_len[s]
        for h in range(pairs):
            at = pair_at(h)
            p = softmax(dot_nt(heads(q[rows, at]), k[rows, at]), usable)
            g[rows, at] = merged(dot_nn(p.astype(BF16), v[rows, at])).astype(BF16)

    def long_usable():
        lanes = lax.broadcasted_iota(jnp.int32, (2 * BLOCK, 4 * BLOCK), 1)
        block = lanes // BLOCK
        inside = lanes - block * BLOCK
        mine = (2 * block + c) * BLOCK + inside
        other = (2 * (block - 2) + 1 - c) * BLOCK + inside
        return jnp.where(block < 2, mine, other) < long_len[y]

    def long_pair(h):
        return pl.ds(pl.multiple_of(h * PAIR, PAIR), PAIR)

    def long_softmax(qm, at, usable):
        scores = jnp.concatenate([dot_nt(qm, k[own_rows, at]), dot_nt(qm, kv_sib[0, :, at])], axis=1)
        return softmax(scores, usable)

    def long_forward(h):
        at = long_pair(h)
        usable = long_usable()
        for n in range(2):
            rows = pl.ds(short_rows + n * BLOCK, BLOCK)
            p = long_softmax(heads(q[rows, at]), at, usable).astype(BF16)
            o2 = dot_nn(p[:, : 2 * BLOCK], v[own_rows, at]) + dot_nn(p[:, 2 * BLOCK :], kv_sib[1, :, at])
            g[rows, at] = merged(o2).astype(BF16)

    def norm_parts(value):
        center = value - jnp.mean(value, axis=1, keepdims=True)
        scale = lax.rsqrt(jnp.mean(center * center, axis=1, keepdims=True) + EPSILON)
        return center * scale, scale

    def norm_back(grad, gain, normed, scale):
        grad = grad * gain
        return scale * (
            grad - jnp.mean(grad, axis=1, keepdims=True) - normed * jnp.mean(grad * normed, axis=1, keepdims=True))

    def row_sum(value):
        return jnp.sum(value, axis=0, keepdims=True)

    def add_sum(row, at, value):
        acc[0, row : row + 1, at] += row_sum(value)

    acc[...] = jnp.zeros_like(acc)
    for cp in loads:
        cp.wait()
    warm_up()
    arrive(K_UNIT)
    swap_x.wait_recv()
    project(K_UNIT, k, None, None)
    arrive(V_UNIT)
    project(V_UNIT, v, V_BIAS, None)
    swap_k = misc(2, k.at[own_rows], kv_sib.at[0], core_peer)
    swap_v = misc(3, v.at[own_rows], kv_sib.at[1], core_peer)
    arrive(Q_UNIT)
    swap_k.start()
    swap_v.start()
    project(Q_UNIT, q, Q_BIAS, SCALE)

    @pl.loop(0, nshort)
    def _(s):
        short_forward(s)

    swap_k.wait_recv()
    swap_v.wait_recv()

    @pl.loop(0, pairs)
    def _(h):
        long_forward(h)

    swap_k.wait_send()
    swap_v.wait_send()
    arrive(O_UNIT)

    @pl.loop(0, width // CHUNK)
    def _(i):
        at = chunk(i)
        r[:, at] = x[:, at].astype(F32) + dot_nn(g[...], columns(O_UNIT, at)) + par[O_BIAS : O_BIAS + 1, at]

    @pl.loop(0, total // TILE)
    def _(i):
        rows = tile(i)
        normed, _ = norm_parts(r[rows, :])
        value = normed * par[GAIN1 : GAIN1 + 1, :] + par[SHIFT1 : SHIFT1 + 1, :]
        a16[rows, :] = value.astype(BF16)
        f[rows, :] = value + par[D_BIAS : D_BIAS + 1, :]

    for j in range(hidden_chunks):
        up, down = UP_UNIT + 2 * j, UP_UNIT + 2 * j + 1
        arrive(up)

        @pl.loop(0, width // CHUNK)
        def _(i):
            at = chunk(i)
            value = dot_nn(a16[...], columns(up, at)) + par[U_BIAS + j : U_BIAS + j + 1, at]
            u16[j, :, at] = value.astype(BF16)
            g[:, at] = gelu(value).astype(BF16)

        if j == hidden_chunks - 2:
            for cp in late:
                cp.start()
        arrive(down)

        @pl.loop(0, width // CHUNK)
        def _(i):
            at = chunk(i)
            f[:, at] += dot_nn(g[...], columns(down, at))

    for cp in late:
        cp.wait()
    swap_dy.wait_recv()

    @pl.loop(0, total // TILE)
    def _(i):
        rows = tile(i)
        normed, scale = norm_parts(f[rows, :])
        upstream = dy[rows, :].astype(F32)
        dy[rows, :] = (normed * par[GAIN2 : GAIN2 + 1, :] + par[SHIFT2 : SHIFT2 + 1, :]).astype(BF16)
        grad = norm_back(upstream, par[GAIN2 : GAIN2 + 1, :], normed, scale)
        f[rows, :] = grad
        a16[rows, :] = grad.astype(BF16)
        add_sum(S_SUM, slice(None), upstream)
        add_sum(D_SUM, slice(None), grad)

    @pl.loop(0, hidden_chunks * (width // CHUNK))
    def _(n):
        j = n // (width // CHUNK)
        i = n % (width // CHUNK)
        at = chunk(i)
        value = dot_nt(a16[...], row_block(UP_UNIT + 1 + 2 * j, i)) * gelu_slope(u16[j, :, at].astype(F32))
        u16[j, :, at] = value.astype(BF16)
        acc[0, pl.ds(U_SUM + j, 1), at] += row_sum(value)

    out_copies = [
        pltpu.make_async_copy(dy.at[pl.ds(0, short_rows)], so, store_sem.at[0]),
        pltpu.make_async_copy(dy.at[pl.ds(short_rows + BLOCK * y, BLOCK)], lo.at[y], store_sem.at[1]),
    ]
    for cp in out_copies:
        cp.start()
    swap_out = misc(4, dy.at[pl.ds(short_rows + BLOCK * (1 - y), BLOCK)], lo.at[y], y_peer)
    swap_out.start()

    @pl.loop(0, width // CHUNK)
    def _(i):
        at = chunk(i)
        value = f[:, at]
        for j in range(hidden_chunks):
            value = value + dot_nt(u16[j], row_block(UP_UNIT + 2 * j, i))
        f[:, at] = value

    @pl.loop(0, total // TILE)
    def _(i):
        rows = tile(i)
        normed, scale = norm_parts(r[rows, :])
        upstream = f[rows, :]
        grad = norm_back(upstream, par[GAIN1 : GAIN1 + 1, :], normed, scale)
        r[rows, :] = grad
        a16[rows, :] = grad.astype(BF16)
        add_sum(F_SUM, slice(None), upstream)
        add_sum(O_SUM, slice(None), grad)

    @pl.loop(0, width // CHUNK)
    def _(i):
        at = chunk(i)
        g[:, at] = dot_nt(a16[...], row_block(O_UNIT, i)).astype(BF16)

    @pl.loop(0, pairs)
    def _(h):
        at = long_pair(h)
        usable = long_usable()
        key_own = key_other = value_own = value_other = 0.0
        query_sum = 0.0
        for n in range(2):
            rows = pl.ds(short_rows + n * BLOCK, BLOCK)
            qm = heads(q[rows, at])
            om = heads(g[rows, at])
            p = long_softmax(qm, at, usable)
            back = jnp.concatenate([dot_nt(om, v[own_rows, at]), dot_nt(om, kv_sib[1, :, at])], axis=1)
            ds = (p * (back - jnp.sum(back * p, axis=1, keepdims=True))).astype(BF16)
            low = p.astype(BF16)
            dq = merged(dot_nn(ds[:, : 2 * BLOCK], k[own_rows, at]) + dot_nn(ds[:, 2 * BLOCK :], kv_sib[0, :, at]))
            dq = dq * SCALE
            q[rows, at] = dq.astype(BF16)
            query_sum = query_sum + row_sum(dq)
            key_own = key_own + dot_tn(ds[:, : 2 * BLOCK], qm)
            key_other = key_other + dot_tn(ds[:, 2 * BLOCK :], qm)
            value_own = value_own + dot_tn(low[:, : 2 * BLOCK], om)
            value_other = value_other + dot_tn(low[:, 2 * BLOCK :], om)
        k[own_rows, at] = key_own.astype(BF16)
        v[own_rows, at] = value_own.astype(BF16)
        kv_sib[0, :, at] = key_other.astype(BF16)
        kv_sib[1, :, at] = value_other.astype(BF16)
        acc[0, Q_SUM : Q_SUM + 1, at] += query_sum
        acc[0, V_SUM : V_SUM + 1, at] += row_sum(value_own) + row_sum(value_other)

    def short_backward(s):
        rows = pl.ds(pl.multiple_of(s * BLOCK, BLOCK), BLOCK)
        usable = key_lane < short_len[s]
        for h in range(pairs):
            at = pair_at(h)
            qm = heads(q[rows, at])
            om = heads(g[rows, at])
            p = softmax(dot_nt(qm, k[rows, at]), usable)
            back = dot_nt(om, v[rows, at])
            ds = (p * (back - jnp.sum(back * p, axis=1, keepdims=True))).astype(BF16)
            dq = merged(dot_nn(ds, k[rows, at])) * SCALE
            dk = dot_tn(ds, qm)
            dv = dot_tn(p.astype(BF16), om)
            q[rows, at] = dq.astype(BF16)
            k[rows, at] = dk.astype(BF16)
            v[rows, at] = dv.astype(BF16)
            add_sum(Q_SUM, at, dq)
            add_sum(V_SUM, at, dv)

    @pl.loop(0, 1)
    def _(s):
        short_backward(s)

    swap_dkv = misc(5, kv_sib, dkv_in, core_peer)
    swap_dkv.start()

    @pl.loop(1, nshort)
    def _(s):
        short_backward(s)

    swap_dkv.wait_recv()
    k[own_rows, :] = (k[own_rows, :].astype(F32) + dkv_in[0].astype(F32)).astype(BF16)
    v[own_rows, :] = (v[own_rows, :].astype(F32) + dkv_in[1].astype(F32)).astype(BF16)

    def exchange(n):
        return misc(8 + n, acc.at[n], acc_in.at[n], partners[n])

    @pl.loop(0, width // CHUNK)
    def _(i):
        at = chunk(i)
        value = r[:, at]
        for ref, u in ((q, Q_UNIT), (k, K_UNIT), (v, V_UNIT)):
            value = value + dot_nt(ref[...], row_block(u, i))
        x[:, at] = value.astype(BF16)

    for n in range(len(partners)):
        cp = exchange(n)
        cp.start()
        cp.wait_recv()
        cp.wait_send()
        acc[n + 1] = acc[n] + acc_in[n]
    sums[...] = acc[len(partners)]

    grad_copies = [
        pltpu.make_async_copy(x.at[pl.ds(0, short_rows)], sg, store_sem.at[2]),
        pltpu.make_async_copy(x.at[pl.ds(short_rows + BLOCK * y, BLOCK)], lg.at[y], store_sem.at[3]),
    ]
    for cp in grad_copies:
        cp.start()
    swap_grad = misc(6, x.at[pl.ds(short_rows + BLOCK * (1 - y), BLOCK)], lg.at[y], y_peer)
    swap_grad.start()
    swap_out.wait_recv()
    swap_grad.wait_recv()
    for cp in out_copies + grad_copies:
        cp.wait()
    for cp in (swap_x, swap_dy, swap_out, swap_dkv, swap_grad):
        cp.wait_send()
    for key in sends:
        sends[key].wait_send()


def whole_step(wsh, xs, xl, dys, dyl, short_len, long_len, par, remote):
    dp_size, seq_size = lax.axis_size("dp"), lax.axis_size("seq")
    width = xs.shape[1]
    nshort = xs.shape[0] // BLOCK
    total = xs.shape[0] + xl.shape[0] * BLOCK
    units = wsh.shape[0]
    lead = (width // CHUNK, 2, 2, 2, CHUNK // 8, width)
    hidden_chunks = (units - 4) // 2
    slots = lead[0] + 8
    steps = (dp_size * seq_size).bit_length() - 1
    anywhere = pl.BlockSpec(memory_space=pl.ANY)
    smem = pl.BlockSpec(memory_space=pltpu.SMEM)
    vmem = pl.BlockSpec(memory_space=pltpu.VMEM)
    act = pltpu.VMEM((total, width), BF16)
    wide = pltpu.VMEM((total, width), F32)
    side = pltpu.VMEM((2, 2 * BLOCK, width), BF16)
    dma = pltpu.SemaphoreType.DMA
    return pl.pallas_call(
        functools.partial(step_kernel, remote, dp_size, seq_size, nshort),
        out_shape=(
            jax.ShapeDtypeStruct(xs.shape, BF16),
            jax.ShapeDtypeStruct(xl.shape, BF16),
            jax.ShapeDtypeStruct(xs.shape, BF16),
            jax.ShapeDtypeStruct(xl.shape, BF16),
            jax.ShapeDtypeStruct((SUMS, width), F32),
        ),
        in_specs=[anywhere] * 5 + [smem] * 2 + [vmem],
        out_specs=(anywhere,) * 4 + (vmem,),
        scratch_shapes=[
            pltpu.VMEM((units, *lead), BF16),
            act, act, act, act, side, side, act, wide, act,
            pltpu.VMEM((hidden_chunks, total, width), BF16),
            wide, act,
            pltpu.VMEM((steps + 1, SUMS, width), F32),
            pltpu.VMEM((steps, SUMS, width), F32),
            dma((units, slots)), dma((units, slots)), dma((8 + steps,)), dma((8 + steps,)),
            dma((units,)), dma((4,)), dma((4,)),
        ],
        compiler_params=pltpu.CompilerParams(
            collective_id=0, has_side_effects=True, vmem_limit_bytes=67043328),
        name="whole_step",
    )(wsh, xs, xl, dys, dyl, short_len, long_len, par)


def on_device(
    short_input, long_input, short_cotangent, long_cotangent, short_lengths, long_lengths,
    query_weight, key_weight, value_weight, output_weight, upward_weight, downward_weight,
    query_bias, value_bias, output_bias, upward_bias, downward_bias,
    first_gain, first_shift, second_gain, second_shift,
):
    rows, width = query_weight.shape
    devices = lax.axis_size("dp") * lax.axis_size("seq")
    hidden_chunks = upward_weight.shape[1] // width
    shape = short_input.shape

    def permuted(value):
        lead = value.shape[:-1]
        value = value.reshape(*lead, devices, hidden_chunks, rows)
        return jnp.moveaxis(value, -2, 0).reshape(hidden_chunks, *lead, width)

    upward = permuted(upward_weight)
    downward = downward_weight.reshape(hidden_chunks, rows, width)
    parts = [key_weight, value_weight, query_weight, output_weight]
    for j in range(hidden_chunks):
        parts += [upward[j], downward[j]]
    wsh = jnp.stack([part.astype(BF16) for part in parts])
    remote = rows == 32 and lax.axis_size("seq") == 4
    if not remote:
        wsh = lax.all_gather(wsh, ("dp", "seq"), axis=1, tiled=True)
        wsh = wsh.reshape(len(parts), width // CHUNK, 2, 2, 2, CHUNK // 8, width)
    par = jnp.concatenate([
        jnp.stack([query_bias, value_bias, output_bias, downward_bias,
                   first_gain, first_shift, second_gain, second_shift]),
        permuted(upward_bias)])
    so, lo, sg, lg, sums = whole_step(
        wsh, short_input.reshape(-1, width), long_input, short_cotangent.reshape(-1, width), long_cotangent,
        short_lengths, long_lengths, par, remote)
    upward_delta = sums[U_SUM : U_SUM + hidden_chunks].reshape(hidden_chunks, devices, rows)
    upward_delta = jnp.moveaxis(upward_delta, 0, 1).reshape(-1)
    return (
        so.reshape(shape), lo, sg.reshape(shape), lg,
        sums[Q_SUM], sums[V_SUM], sums[O_SUM], upward_delta, sums[D_SUM], sums[F_SUM], sums[S_SUM],
    )


def solution(mesh):
    split = ("dp", "seq")
    placed = (
        P(split, None, None), P("dp", "seq", None), P(split, None, None), P("dp", "seq", None),
        P(split), P("dp"),
        *(P(split, None) for _ in range(6)), *(P() for _ in range(9)),
    )
    return jax.shard_map(
        on_device,
        mesh=mesh,
        in_specs=placed,
        out_specs=(
            P(split, None, None), P("dp", "seq", None), P(split, None, None), P("dp", "seq", None),
            *(P() for _ in range(7)),
        ),
        check_vma=False,
    )
```

```python
import functools

import jax
import jax.numpy as jnp
from jax import lax
from jax.experimental import pallas as pl
from jax.experimental.pallas import tpu as pltpu
from jax.sharding import PartitionSpec as P

MESH = pl.DeviceIdType.MESH


def phase(name, start, stop):
    return pl.loop(start, stop)


F32 = jnp.float32
BF16 = jnp.bfloat16
EPSILON = 1e-12
MASKED = -1e30
SCALE = 0.125
PAIR = 128
BLOCK = 128
CHUNK = 256
TILE = 256
K_UNIT, V_UNIT, Q_UNIT, O_UNIT, UP_UNIT = 0, 1, 2, 3, 4
Q_BIAS, V_BIAS, O_BIAS, D_BIAS, GAIN1, SHIFT1, GAIN2, SHIFT2, U_BIAS = 0, 1, 2, 3, 4, 5, 6, 7, 8
Q_SUM, V_SUM = 0, 1
O_SUM, D_SUM, F_SUM, S_SUM, U_SUM = 0, 1, 2, 3, 4


def dot_nn(a, b):
    return jnp.dot(a, b, preferred_element_type=F32)


def dot_nt(a, b):
    return lax.dot_general(a, b, (((1,), (1,)), ((), ())), preferred_element_type=F32)


def dot_tn(a, b):
    return lax.dot_general(a, b, (((0,), (0,)), ((), ())), preferred_element_type=F32)


def flipped(index, bit):
    return index + bit * (1 - 2 * ((index // bit) % 2))


def gelu_parts(u):
    square = u * u
    t = jnp.tanh(0.7978845608028654 * (u + 0.044715 * (u * square)))
    half = 0.5 * (1.0 + t)
    slope = half + 0.5 * u * (1.0 - t * t) * (0.7978845608028654 * (1.0 + 3 * 0.044715 * square))
    return u * half, slope


def step_kernel(
    remote, dp_size, seq_size, nshort,
    wsh, xs, xl, dys, dyl, short_len, long_len, par,
    so, lo, sg, lg, sums, tail_sums, parked,
    w, x, q, k, v, kv_sib, dkv_in, g, r, a16, hid, f, dy, acc, acc_in, tail, tail_in,
    send_sem, recv_sem, misc_send, misc_recv, own_sem, load_sem, store_sem,
):
    dp = lax.axis_index("dp")
    seq = lax.axis_index("seq")
    y, c = seq // 2, seq % 2
    y_peer = (dp, flipped(seq, 2))
    core_peer = (dp, flipped(seq, 1))
    total, width = x.shape
    short_rows = nshort * BLOCK
    units = w.shape[0]
    depth = w.shape[1]
    hidden_chunks = (units - 4) // 2
    partners = []
    bit = 1
    while bit < seq_size:
        partners.append((dp, flipped(seq, bit)))
        bit *= 2
    bit = 1
    while bit < dp_size:
        partners.append((flipped(dp, bit), seq))
        bit *= 2

    loads = [pltpu.make_async_copy(xs, x.at[pl.ds(0, short_rows)], load_sem.at[0]),
             pltpu.make_async_copy(xl.at[y], x.at[pl.ds(short_rows + BLOCK * y, BLOCK)], load_sem.at[1])]
    late = [pltpu.make_async_copy(dys, dy.at[pl.ds(0, short_rows)], load_sem.at[2]),
            pltpu.make_async_copy(dyl.at[y], dy.at[pl.ds(short_rows + BLOCK * y, BLOCK)], load_sem.at[3])]
    for cp in loads:
        cp.start()

    if remote:
        z, ax = dp // 2, dp % 2
        hops = depth - 1
        z_peers = [((z + n) % depth * 2 + ax, seq) for n in range(1, depth)]
        x_peer = (flipped(dp, 1), seq)
        peers = z_peers + [x_peer, y_peer, core_peer]
        own = [pltpu.make_async_copy(wsh.at[u], w.at[u, z, ax, y, c], own_sem.at[u]) for u in range(units)]
    else:
        peers = partners
        own = [pltpu.make_async_copy(wsh.at[u], w.at[u], own_sem.at[u]) for u in range(units)]
    for cp in own:
        cp.start()

    barrier = pltpu.get_barrier_semaphore()
    for peer in peers:
        pl.semaphore_signal(barrier, inc=1, device_id=peer, device_id_type=MESH)
    pl.semaphore_wait(barrier, len(peers))

    def misc(slot, src, dst, peer):
        return pltpu.make_async_remote_copy(
            src_ref=src, dst_ref=dst, send_sem=misc_send.at[slot], recv_sem=misc_recv.at[slot],
            device_id=peer, device_id_type=MESH)

    swap_x = misc(0, xl.at[1 - y], x.at[pl.ds(short_rows + BLOCK * y, BLOCK)], y_peer)
    swap_dy = misc(1, dyl.at[1 - y], dy.at[pl.ds(short_rows + BLOCK * y, BLOCK)], y_peer)
    swap_x.start()

    sends = {}
    if remote:
        half = depth // 2
        lower, upper, every, both = pl.ds(0, half), pl.ds(half, depth - half), pl.ds(0, depth), pl.ds(0, 2)
        B0, B1, C0, C1, D0 = hops, hops + 1, hops + 2, hops + 3, hops + 4

        def send(u, slot, src, part, peer):
            cp = pltpu.make_async_remote_copy(
                src_ref=src, dst_ref=w.at[(u, *part)], send_sem=send_sem.at[u, slot], recv_sem=recv_sem.at[u, slot],
                device_id=peer, device_id_type=MESH)
            cp.start()
            sends[u, slot] = cp

        def pass_on(u, slot, part, peer):
            send(u, slot, w.at[(u, *part)], part, peer)

        for u in range(units):
            for n in range(hops):
                send(u, n, wsh.at[u], (z, ax, y, c), z_peers[n])

        def step_a(u):
            for n in range(hops):
                sends[u, n].wait_recv()
            own[u].wait()
            pass_on(u, B0, (lower, ax, y, c), x_peer)
            pass_on(u, B1, (upper, ax, y, c), y_peer)
            pass_on(u, D0, (every, ax, y, c), core_peer)

        def step_b(u):
            sends[u, B0].wait_recv()
            pass_on(u, C0, (lower, both, y, c), y_peer)
            sends[u, B1].wait_recv()
            pass_on(u, C1, (upper, ax, both, c), x_peer)
            pass_on(u, D0 + 1, (lower, 1 - ax, y, c), core_peer)
            pass_on(u, D0 + 2, (upper, ax, 1 - y, c), core_peer)

        def step_c(u):
            sends[u, C0].wait_recv()
            pass_on(u, D0 + 3, (lower, both, 1 - y, c), core_peer)
            sends[u, C1].wait_recv()
            pass_on(u, D0 + 4, (upper, 1 - ax, both, c), core_peer)

        def step_d(u):
            for n in range(5):
                sends[u, D0 + n].wait_recv()

        def arrive(i):
            if i + 3 < units:
                step_a(i + 3)
            if i + 2 < units:
                step_b(i + 2)
            if i + 1 < units:
                step_c(i + 1)
            if i == units - 2:
                swap_dy.start()
            step_d(i)

        def warm_up():
            step_a(0)
            step_a(1)
            step_b(0)
            step_a(2)
            step_b(1)
            step_c(0)
    else:
        def arrive(i):
            if i == units - 2:
                swap_dy.start()
            own[i].wait()

        def warm_up():
            pass

    def columns(u, at):
        return w[u, :, :, :, :, :, at].reshape(width, CHUNK)

    def row_block(u, i):
        return w[u, i].reshape(CHUNK, width)

    def chunk(i):
        return pl.ds(pl.multiple_of(i * CHUNK, CHUNK), CHUNK)

    def tile(i):
        return pl.ds(pl.multiple_of(i * TILE, TILE), TILE)

    def project(u, dst, bias, scale):
        @phase("proj", 0, width // CHUNK)
        def _(i):
            at = chunk(i)
            value = dot_nn(x[...], columns(u, at))
            if bias is not None:
                value = value + par[bias : bias + 1, at]
            if scale is not None:
                value = value * scale
            dst[:, at] = value.astype(BF16)

    lane = lax.broadcasted_iota(jnp.int32, (BLOCK, PAIR), 1)
    low_half = lane < PAIR // 2
    row_lane = lax.broadcasted_iota(jnp.int32, (1, PAIR), 1)
    first_head = jnp.where(row_lane < PAIR // 2, 1.0, 0.0).astype(BF16)
    second_head = jnp.where(row_lane < PAIR // 2, 0.0, 1.0).astype(BF16)

    def heads(value):
        return jnp.concatenate([value * first_head, value * second_head], axis=0)

    def merged(value):
        return jnp.where(low_half, value[:BLOCK], value[BLOCK:])

    def softmax(scores, usable):
        scores = jnp.where(usable, scores, MASKED)
        weight = jnp.exp(scores - jnp.max(scores, axis=0, keepdims=True))
        return weight * (1.0 / jnp.sum(weight, axis=0, keepdims=True))

    pairs = width // PAIR
    per_row = width // (2 * BLOCK)
    own_rows = pl.ds(short_rows, 2 * BLOCK)

    def pair_at(h):
        return slice(h * PAIR, (h + 1) * PAIR)

    def short_kept(s, h):
        start = (s % 4) * (pairs // per_row) + h // per_row
        col = h % per_row * 2 * BLOCK
        return s // 4, pl.ds(pl.multiple_of(start * BLOCK, BLOCK), BLOCK), slice(col, col + 2 * BLOCK)

    def long_kept(n, h):
        rows = pl.ds(pl.multiple_of(h // per_row * 4 * BLOCK, 4 * BLOCK), 4 * BLOCK)
        return 2 + n, rows, pl.ds(pl.multiple_of(h % per_row * 2 * BLOCK, 2 * BLOCK), 2 * BLOCK)

    def short_forward(s):
        rows = pl.ds(pl.multiple_of(s * BLOCK, BLOCK), BLOCK)
        usable = lax.broadcasted_iota(jnp.int32, (BLOCK, 2 * BLOCK), 0) < short_len[s]
        for h in range(pairs):
            at = pair_at(h)
            p = softmax(dot_nt(k[rows, at], heads(q[rows, at])), usable).astype(BF16)
            hid[short_kept(s, h)] = p
            g[rows, at] = merged(dot_tn(p, v[rows, at])).astype(BF16)

    def long_usable():
        key = lax.broadcasted_iota(jnp.int32, (4 * BLOCK, 2 * BLOCK), 0)
        block = key // BLOCK
        mine = key + (block + c) * BLOCK
        other = key + (block - 3 - c) * BLOCK
        return jnp.where(block < 2, mine, other) < long_len[y]

    def long_pair(h):
        return pl.ds(pl.multiple_of(h * PAIR, PAIR), PAIR)

    def long_forward(h):
        at = long_pair(h)
        usable = long_usable()
        for n in range(2):
            rows = pl.ds(short_rows + n * BLOCK, BLOCK)
            qm = heads(q[rows, at])
            scores = jnp.concatenate([dot_nt(k[own_rows, at], qm), dot_nt(kv_sib[0, :, at], qm)], axis=0)
            p = softmax(scores, usable).astype(BF16)
            hid[long_kept(n, h)] = p
            o2 = dot_tn(p[: 2 * BLOCK], v[own_rows, at]) + dot_tn(p[2 * BLOCK :], kv_sib[1, :, at])
            g[rows, at] = merged(o2).astype(BF16)

    def norm_parts(value):
        center = value - jnp.mean(value, axis=1, keepdims=True)
        scale = lax.rsqrt(jnp.mean(center * center, axis=1, keepdims=True) + EPSILON)
        return center * scale, scale

    def norm_back(grad, gain, normed, scale):
        grad = grad * gain
        return scale * (
            grad - jnp.mean(grad, axis=1, keepdims=True) - normed * jnp.mean(grad * normed, axis=1, keepdims=True))

    def row_sum(value):
        return jnp.sum(value, axis=0, keepdims=True)

    def add_sum(row, at, value):
        acc[0, row : row + 1, at] += row_sum(value)

    acc[0] = jnp.zeros_like(acc[0])
    tail[0] = jnp.zeros_like(tail[0])
    for cp in loads:
        cp.wait()
    warm_up()
    arrive(K_UNIT)
    swap_x.wait_recv()
    project(K_UNIT, k, None, None)
    arrive(V_UNIT)
    project(V_UNIT, v, V_BIAS, None)
    swap_k = misc(2, k.at[own_rows], kv_sib.at[0], core_peer)
    swap_v = misc(3, v.at[own_rows], kv_sib.at[1], core_peer)
    arrive(Q_UNIT)
    swap_k.start()
    swap_v.start()
    project(Q_UNIT, q, Q_BIAS, SCALE)

    @phase("sf", 0, nshort)
    def _(s):
        short_forward(s)

    swap_k.wait_recv()
    swap_v.wait_recv()

    @phase("lf", 0, pairs)
    def _(h):
        long_forward(h)

    swap_k.wait_send()
    swap_v.wait_send()
    park = pltpu.make_async_copy(hid, parked, store_sem.at[4])
    park.start()
    arrive(O_UNIT)

    @phase("wo", 0, width // CHUNK)
    def _(i):
        at = chunk(i)
        r[:, at] = x[:, at].astype(F32) + dot_nn(g[...], columns(O_UNIT, at)) + par[O_BIAS : O_BIAS + 1, at]

    @phase("ln1", 0, total // TILE)
    def _(i):
        rows = tile(i)
        normed, _ = norm_parts(r[rows, :])
        value = normed * par[GAIN1 : GAIN1 + 1, :] + par[SHIFT1 : SHIFT1 + 1, :]
        a16[rows, :] = value.astype(BF16)
        f[rows, :] = value + par[D_BIAS : D_BIAS + 1, :]

    for j in range(hidden_chunks):
        up, down = UP_UNIT + 2 * j, UP_UNIT + 2 * j + 1
        arrive(up)
        if j == 0:
            park.wait()

        @phase("up", 0, width // CHUNK)
        def _(i):
            at = chunk(i)
            value = dot_nn(a16[...], columns(up, at)) + par[U_BIAS + j : U_BIAS + j + 1, at]
            active, slope = gelu_parts(value)
            hid[j, :, at] = slope.astype(BF16)
            g[:, at] = active.astype(BF16)

        if j == hidden_chunks - 2:
            for cp in late:
                cp.start()
        arrive(down)

        @phase("down", 0, width // CHUNK)
        def _(i):
            at = chunk(i)
            f[:, at] += dot_nn(g[...], columns(down, at))

    for cp in late:
        cp.wait()
    swap_dy.wait_recv()

    @phase("ln2", 0, total // TILE)
    def _(i):
        rows = tile(i)
        normed, scale = norm_parts(f[rows, :])
        upstream = dy[rows, :].astype(F32)
        dy[rows, :] = (normed * par[GAIN2 : GAIN2 + 1, :] + par[SHIFT2 : SHIFT2 + 1, :]).astype(BF16)
        grad = norm_back(upstream, par[GAIN2 : GAIN2 + 1, :], normed, scale)
        f[rows, :] = grad
        a16[rows, :] = grad.astype(BF16)
        add_sum(S_SUM, slice(None), upstream)
        add_sum(D_SUM, slice(None), grad)

    out_copies = [
        pltpu.make_async_copy(dy.at[pl.ds(0, short_rows)], so, store_sem.at[0]),
        pltpu.make_async_copy(dy.at[pl.ds(short_rows + BLOCK * y, BLOCK)], lo.at[y], store_sem.at[1]),
    ]
    for cp in out_copies:
        cp.start()
    swap_out = misc(4, dy.at[pl.ds(short_rows + BLOCK * (1 - y), BLOCK)], lo.at[y], y_peer)
    swap_out.start()

    @phase("dg", 0, hidden_chunks * (width // CHUNK))
    def _(n):
        j = n // (width // CHUNK)
        i = n % (width // CHUNK)
        at = chunk(i)
        value = dot_nt(a16[...], row_block(UP_UNIT + 1 + 2 * j, i)) * hid[j, :, at].astype(F32)
        hid[j, :, at] = value.astype(BF16)
        acc[0, pl.ds(U_SUM + j, 1), at] += row_sum(value)

    @phase("da", 0, width // CHUNK)
    def _(i):
        at = chunk(i)
        value = f[:, at]
        for j in range(hidden_chunks):
            value = value + dot_nt(hid[j], row_block(UP_UNIT + 2 * j, i))
        f[:, at] = value

    unpark = pltpu.make_async_copy(parked, hid, store_sem.at[5])
    unpark.start()

    @phase("ln1b", 0, total // TILE)
    def _(i):
        rows = tile(i)
        normed, scale = norm_parts(r[rows, :])
        upstream = f[rows, :]
        grad = norm_back(upstream, par[GAIN1 : GAIN1 + 1, :], normed, scale)
        r[rows, :] = grad
        a16[rows, :] = grad.astype(BF16)
        add_sum(F_SUM, slice(None), upstream)
        add_sum(O_SUM, slice(None), grad)

    def early(n):
        return misc(8 + n, acc.at[n], acc_in.at[n], partners[n])

    def finish_early(n):
        early(n).wait_recv()
        early(n).wait_send()
        acc[n + 1] = acc[n] + acc_in[n]

    def next_early(n):
        if n > 0:
            finish_early(n - 1)
        early(n).start()

    next_early(0)

    @phase("do", 0, width // CHUNK)
    def _(i):
        at = chunk(i)
        g[:, at] = dot_nt(a16[...], row_block(O_UNIT, i)).astype(BF16)

    next_early(1)
    unpark.wait()

    @phase("lb", 0, pairs)
    def _(h):
        at = long_pair(h)
        keys, values = k[own_rows, at], v[own_rows, at]
        keys_far, values_far = kv_sib[0, :, at], kv_sib[1, :, at]
        key_grad = value_grad = query_sum = 0.0
        for n in range(2):
            rows = pl.ds(short_rows + n * BLOCK, BLOCK)
            qm = heads(q[rows, at])
            om = heads(g[rows, at])
            low = hid[long_kept(n, h)]
            p = low.astype(F32)
            back = jnp.concatenate([dot_nt(values, om), dot_nt(values_far, om)], axis=0)
            ds = (p * (back - jnp.sum(back * p, axis=0, keepdims=True))).astype(BF16)
            dq = merged(dot_tn(ds[: 2 * BLOCK], keys) + dot_tn(ds[2 * BLOCK :], keys_far)) * SCALE
            q[rows, at] = dq.astype(BF16)
            query_sum = query_sum + row_sum(dq)
            key_grad = key_grad + dot_nn(ds, qm)
            value_grad = value_grad + dot_nn(low, om)
        k[own_rows, at] = key_grad[: 2 * BLOCK].astype(BF16)
        v[own_rows, at] = value_grad[: 2 * BLOCK].astype(BF16)
        kv_sib[0, :, at] = key_grad[2 * BLOCK :].astype(BF16)
        kv_sib[1, :, at] = value_grad[2 * BLOCK :].astype(BF16)
        tail[0, Q_SUM : Q_SUM + 1, at] += query_sum
        tail[0, V_SUM : V_SUM + 1, at] += row_sum(value_grad)

    def short_backward(s):
        rows = pl.ds(pl.multiple_of(s * BLOCK, BLOCK), BLOCK)
        for h in range(pairs):
            at = pair_at(h)
            qm = heads(q[rows, at])
            om = heads(g[rows, at])
            keys = k[rows, at]
            low = hid[short_kept(s, h)]
            p = low.astype(F32)
            back = dot_nt(v[rows, at], om)
            ds = (p * (back - jnp.sum(back * p, axis=0, keepdims=True))).astype(BF16)
            dq = merged(dot_tn(ds, keys)) * SCALE
            dk = dot_nn(ds, qm)
            dv = dot_nn(low, om)
            q[rows, at] = dq.astype(BF16)
            k[rows, at] = dk.astype(BF16)
            v[rows, at] = dv.astype(BF16)
            tail[0, Q_SUM : Q_SUM + 1, at] += row_sum(dq)
            tail[0, V_SUM : V_SUM + 1, at] += row_sum(dv)

    next_early(2)

    @phase("sb1", 0, 1)
    def _(s):
        short_backward(s)

    swap_dkv = misc(5, kv_sib, dkv_in, core_peer)
    swap_dkv.start()
    next_early(3)

    @phase("sb2", 1, nshort)
    def _(s):
        short_backward(s)

    steps = len(partners)

    def late_sum(n):
        return misc(8 + steps + n, tail.at[n], tail_in.at[n], partners[n])

    def finish_late(n):
        late_sum(n).wait_recv()
        late_sum(n).wait_send()
        tail[n + 1] = tail[n] + tail_in[n]

    def next_late(n):
        if n > 0:
            finish_late(n - 1)
        late_sum(n).start()

    next_late(0)
    for n in range(4, steps):
        next_early(n)
    swap_dkv.wait_recv()
    k[own_rows, :] = (k[own_rows, :].astype(F32) + dkv_in[0].astype(F32)).astype(BF16)
    v[own_rows, :] = (v[own_rows, :].astype(F32) + dkv_in[1].astype(F32)).astype(BF16)

    def input_grad(rows, i):
        at = chunk(i)
        value = r[rows, at]
        for ref, u in ((q, Q_UNIT), (k, K_UNIT), (v, V_UNIT)):
            value = value + dot_nt(ref[rows, :], row_block(u, i))
        x[rows, at] = value.astype(BF16)

    @phase("gxl", 0, width // CHUNK)
    def _(i):
        input_grad(own_rows, i)

    swap_grad = misc(6, x.at[pl.ds(short_rows + BLOCK * (1 - y), BLOCK)], lg.at[y], y_peer)
    swap_grad.start()
    finish_early(steps - 1)
    next_late(1)
    for i in range(width // CHUNK):

        @phase("gxs", i, i + 1)
        def _(n):
            input_grad(pl.ds(0, short_rows), n)

        if i + 2 < steps:
            next_late(i + 2)
    for n in range(width // CHUNK + 2, steps):
        next_late(n)
    finish_late(steps - 1)
    sums[...] = acc[steps]
    tail_sums[...] = tail[steps]

    grad_copies = [
        pltpu.make_async_copy(x.at[pl.ds(0, short_rows)], sg, store_sem.at[2]),
        pltpu.make_async_copy(x.at[pl.ds(short_rows + BLOCK * y, BLOCK)], lg.at[y], store_sem.at[3]),
    ]
    for cp in grad_copies:
        cp.start()
    swap_out.wait_recv()
    swap_grad.wait_recv()
    for cp in out_copies + grad_copies:
        cp.wait()
    for cp in (swap_x, swap_dy, swap_out, swap_dkv, swap_grad):
        cp.wait_send()
    for key in sends:
        sends[key].wait_send()


def whole_step(wsh, xs, xl, dys, dyl, short_len, long_len, par, remote):
    dp_size, seq_size = lax.axis_size("dp"), lax.axis_size("seq")
    width = xs.shape[1]
    nshort = xs.shape[0] // BLOCK
    total = xs.shape[0] + xl.shape[0] * BLOCK
    units = wsh.shape[0]
    lead = (width // CHUNK, 2, 2, 2, CHUNK // 8, width)
    hidden_chunks = (units - 4) // 2
    slots = lead[0] + 8
    steps = (dp_size * seq_size).bit_length() - 1
    anywhere = pl.BlockSpec(memory_space=pl.ANY)
    smem = pl.BlockSpec(memory_space=pltpu.SMEM)
    vmem = pl.BlockSpec(memory_space=pltpu.VMEM)
    act = pltpu.VMEM((total, width), BF16)
    wide = pltpu.VMEM((total, width), F32)
    side = pltpu.VMEM((2, 2 * BLOCK, width), BF16)
    dma = pltpu.SemaphoreType.DMA
    return pl.pallas_call(
        functools.partial(step_kernel, remote, dp_size, seq_size, nshort),
        out_shape=(
            jax.ShapeDtypeStruct(xs.shape, BF16),
            jax.ShapeDtypeStruct(xl.shape, BF16),
            jax.ShapeDtypeStruct(xs.shape, BF16),
            jax.ShapeDtypeStruct(xl.shape, BF16),
            jax.ShapeDtypeStruct((4 + hidden_chunks, width), F32),
            jax.ShapeDtypeStruct((2, width), F32),
            jax.ShapeDtypeStruct((hidden_chunks, total, width), BF16),
        ),
        in_specs=[anywhere] * 5 + [smem] * 2 + [vmem],
        out_specs=(anywhere,) * 4 + (vmem,) * 2 + (anywhere,),
        scratch_shapes=[
            pltpu.VMEM((units, *lead), BF16),
            act, act, act, act, side, side, act, wide, act,
            pltpu.VMEM((hidden_chunks, total, width), BF16),
            wide, act,
            pltpu.VMEM((steps + 1, 4 + hidden_chunks, width), F32),
            pltpu.VMEM((steps, 4 + hidden_chunks, width), F32),
            pltpu.VMEM((steps + 1, 2, width), F32),
            pltpu.VMEM((steps, 2, width), F32),
            dma((units, slots)), dma((units, slots)), dma((8 + 2 * steps,)), dma((8 + 2 * steps,)),
            dma((units,)), dma((4,)), dma((6,)),
        ],
        compiler_params=pltpu.CompilerParams(
            collective_id=0, has_side_effects=True, vmem_limit_bytes=67043328),
        name="whole_step",
    )(wsh, xs, xl, dys, dyl, short_len, long_len, par)


def on_device(
    short_input, long_input, short_cotangent, long_cotangent, short_lengths, long_lengths,
    query_weight, key_weight, value_weight, output_weight, upward_weight, downward_weight,
    query_bias, value_bias, output_bias, upward_bias, downward_bias,
    first_gain, first_shift, second_gain, second_shift,
):
    rows, width = query_weight.shape
    devices = lax.axis_size("dp") * lax.axis_size("seq")
    hidden_chunks = upward_weight.shape[1] // width
    shape = short_input.shape

    def permuted(value):
        lead = value.shape[:-1]
        value = value.reshape(*lead, devices, hidden_chunks, rows)
        return jnp.moveaxis(value, -2, 0).reshape(hidden_chunks, *lead, width)

    upward = permuted(upward_weight)
    downward = downward_weight.reshape(hidden_chunks, rows, width)
    parts = [key_weight, value_weight, query_weight, output_weight]
    for j in range(hidden_chunks):
        parts += [upward[j], downward[j]]
    wsh = jnp.stack([part.astype(BF16) for part in parts])
    remote = rows == 32 and lax.axis_size("seq") == 4
    if not remote:
        wsh = lax.all_gather(wsh, ("dp", "seq"), axis=1, tiled=True)
        wsh = wsh.reshape(len(parts), width // CHUNK, 2, 2, 2, CHUNK // 8, width)
    par = jnp.concatenate([
        jnp.stack([query_bias, value_bias, output_bias, downward_bias,
                   first_gain, first_shift, second_gain, second_shift]),
        permuted(upward_bias)])
    so, lo, sg, lg, sums, tail_sums, _ = whole_step(
        wsh, short_input.reshape(-1, width), long_input, short_cotangent.reshape(-1, width), long_cotangent,
        short_lengths, long_lengths, par, remote)
    upward_delta = sums[U_SUM : U_SUM + hidden_chunks].reshape(hidden_chunks, devices, rows)
    upward_delta = jnp.moveaxis(upward_delta, 0, 1).reshape(-1)
    return (
        so.reshape(shape), lo, sg.reshape(shape), lg,
        tail_sums[Q_SUM], tail_sums[V_SUM], sums[O_SUM], upward_delta, sums[D_SUM], sums[F_SUM], sums[S_SUM],
    )


def solution(mesh):
    split = ("dp", "seq")
    placed = (
        P(split, None, None), P("dp", "seq", None), P(split, None, None), P("dp", "seq", None),
        P(split), P("dp"),
        *(P(split, None) for _ in range(6)), *(P() for _ in range(9)),
    )
    return jax.shard_map(
        on_device,
        mesh=mesh,
        in_specs=placed,
        out_specs=(
            P(split, None, None), P("dp", "seq", None), P(split, None, None), P("dp", "seq", None),
            *(P() for _ in range(7)),
        ),
        check_vma=False,
    )
```

```python
import functools

import jax
import jax.numpy as jnp
from jax import lax
from jax.experimental import pallas as pl
from jax.experimental.pallas import tpu as pltpu
from jax.sharding import PartitionSpec as P

MESH = pl.DeviceIdType.MESH


def phase(name, start, stop):
    return pl.loop(start, stop)


F32 = jnp.float32
BF16 = jnp.bfloat16
EPSILON = 1e-12
MASKED = -1e30
SCALE = 0.125
PAIR = 128
BLOCK = 128
CHUNK = 256
TILE = 256
K_UNIT, V_UNIT, Q_UNIT, O_UNIT, UP_UNIT = 0, 1, 2, 3, 4
Q_BIAS, V_BIAS, O_BIAS, D_BIAS, GAIN1, SHIFT1, GAIN2, SHIFT2, U_BIAS = 0, 1, 2, 3, 4, 5, 6, 7, 8
Q_SUM, V_SUM = 0, 1
O_SUM, D_SUM, F_SUM, S_SUM, U_SUM = 0, 1, 2, 3, 4


def dot_nn(a, b):
    return jnp.dot(a, b, preferred_element_type=F32)


def dot_nt(a, b):
    return lax.dot_general(a, b, (((1,), (1,)), ((), ())), preferred_element_type=F32)


def dot_tn(a, b):
    return lax.dot_general(a, b, (((0,), (0,)), ((), ())), preferred_element_type=F32)


def flipped(index, bit):
    return index + bit * (1 - 2 * ((index // bit) % 2))


def gelu_parts(u):
    square = u * u
    t = jnp.tanh(0.7978845608028654 * (u + 0.044715 * (u * square)))
    half = 0.5 * (1.0 + t)
    slope = half + 0.5 * u * (1.0 - t * t) * (0.7978845608028654 * (1.0 + 3 * 0.044715 * square))
    return u * half, slope


def every_fourth(pieces, j, lanes, stride):
    found = []
    for piece in pieces:
        for start in range(j * lanes, piece.shape[1], stride * lanes):
            found.append(piece[:, start : start + lanes])
    return found


def step_kernel(
    remote, dp_size, seq_size, nshort,
    *refs,
):
    given = 6 if remote else 1
    shards, refs = refs[:given], refs[given:]
    small, refs = refs[:9], refs[9:]
    (xs, xl, dys, dyl, short_len, long_len,
     so, lo, sg, lg, sums, up_sums, parked,
     par, wide_par,
     w, x, q, k, v, kv_sib, dkv_in, g, r, a16, hid, f, dy, acc, acc_in, tail, tail_in,
     send_sem, recv_sem, misc_send, misc_recv, own_sem, small_sem, load_sem, store_sem) = refs
    dp = lax.axis_index("dp")
    seq = lax.axis_index("seq")
    y, c = seq // 2, seq % 2
    y_peer = (dp, flipped(seq, 2))
    core_peer = (dp, flipped(seq, 1))
    total, width = x.shape
    short_rows = nshort * BLOCK
    units = w.shape[0]
    depth = w.shape[1]
    hidden_chunks = (units - 4) // 2
    partners = []
    bit = 1
    while bit < seq_size:
        partners.append((dp, flipped(seq, bit)))
        bit *= 2
    bit = 1
    while bit < dp_size:
        partners.append((flipped(dp, bit), seq))
        bit *= 2

    loads = [pltpu.make_async_copy(xs, x.at[pl.ds(0, short_rows)], load_sem.at[0]),
             pltpu.make_async_copy(xl.at[y], x.at[pl.ds(short_rows + BLOCK * y, BLOCK)], load_sem.at[1])]
    late = [pltpu.make_async_copy(dys, dy.at[pl.ds(0, short_rows)], load_sem.at[2]),
            pltpu.make_async_copy(dyl.at[y], dy.at[pl.ds(short_rows + BLOCK * y, BLOCK)], load_sem.at[3])]
    for cp in loads:
        cp.start()

    if remote:
        z, ax = dp // 2, dp % 2
        hops = depth - 1
        z_peers = [((z + n) % depth * 2 + ax, seq) for n in range(1, depth)]
        x_peer = (flipped(dp, 1), seq)
        peers = z_peers + [x_peer, y_peer, core_peer]
        piece = w.shape[5]
        key_shard, value_shard, query_shard, output_shard, up_shard, down_shard = shards
        sources = [key_shard, value_shard, query_shard, output_shard]
        sources += [up_shard.at[:, pl.ds(n * width, width)] for n in range(hidden_chunks)]
        sources += [down_shard.at[pl.ds(n * piece, piece)] for n in range(hidden_chunks)]
        own = [pltpu.make_async_copy(source, f.at[pl.ds(n * piece, piece)], own_sem.at[n])
               for n, source in enumerate(sources)]
    else:
        peers = partners
        own = [pltpu.make_async_copy(shards[0].at[u], w.at[u], own_sem.at[u]) for u in range(units)]
    for cp in own:
        cp.start()
    small_loads = [pltpu.make_async_copy(ref, par.at[n] if n < U_BIAS else wide_par, small_sem.at[n])
                   for n, ref in enumerate(small)]
    for cp in small_loads:
        cp.start()

    barrier = pltpu.get_barrier_semaphore()
    for peer in peers:
        pl.semaphore_signal(barrier, inc=1, device_id=peer, device_id_type=MESH)

    if remote:
        lanes = width // (8 * depth)
        for cp in own:
            cp.wait()
        for u in range(4):
            w[u, z, ax, y, c] = f[u * piece : (u + 1) * piece, :].astype(BF16)
        up_rows = [f[(4 + n) * piece : (5 + n) * piece, :].astype(BF16) for n in range(hidden_chunks)]
        for j in range(hidden_chunks):
            first = (4 + hidden_chunks + j) * piece
            w[UP_UNIT + 2 * j, z, ax, y, c] = jnp.concatenate(every_fourth(up_rows, j, lanes, hidden_chunks), axis=1)
            w[UP_UNIT + 2 * j + 1, z, ax, y, c] = f[first : first + piece, :].astype(BF16)
    pl.semaphore_wait(barrier, len(peers))

    def misc(slot, src, dst, peer):
        return pltpu.make_async_remote_copy(
            src_ref=src, dst_ref=dst, send_sem=misc_send.at[slot], recv_sem=misc_recv.at[slot],
            device_id=peer, device_id_type=MESH)

    swap_x = misc(0, xl.at[1 - y], x.at[pl.ds(short_rows + BLOCK * y, BLOCK)], y_peer)
    swap_dy = misc(1, dyl.at[1 - y], dy.at[pl.ds(short_rows + BLOCK * y, BLOCK)], y_peer)
    swap_x.start()

    sends = {}
    if remote:
        half = depth // 2
        lower, upper, every, both = pl.ds(0, half), pl.ds(half, depth - half), pl.ds(0, depth), pl.ds(0, 2)
        B0, B1, C0, C1, D0 = hops, hops + 1, hops + 2, hops + 3, hops + 4

        def send(u, slot, src, part, peer):
            cp = pltpu.make_async_remote_copy(
                src_ref=src, dst_ref=w.at[(u, *part)], send_sem=send_sem.at[u, slot], recv_sem=recv_sem.at[u, slot],
                device_id=peer, device_id_type=MESH)
            cp.start()
            sends[u, slot] = cp

        def pass_on(u, slot, part, peer):
            send(u, slot, w.at[(u, *part)], part, peer)

        for u in range(units):
            for n in range(hops):
                pass_on(u, n, (z, ax, y, c), z_peers[n])

        def step_a(u):
            for n in range(hops):
                sends[u, n].wait_recv()
            pass_on(u, B0, (lower, ax, y, c), x_peer)
            pass_on(u, B1, (upper, ax, y, c), y_peer)
            pass_on(u, D0, (every, ax, y, c), core_peer)

        def step_b(u):
            sends[u, B0].wait_recv()
            pass_on(u, C0, (lower, both, y, c), y_peer)
            sends[u, B1].wait_recv()
            pass_on(u, C1, (upper, ax, both, c), x_peer)
            pass_on(u, D0 + 1, (lower, 1 - ax, y, c), core_peer)
            pass_on(u, D0 + 2, (upper, ax, 1 - y, c), core_peer)

        def step_c(u):
            sends[u, C0].wait_recv()
            pass_on(u, D0 + 3, (lower, both, 1 - y, c), core_peer)
            sends[u, C1].wait_recv()
            pass_on(u, D0 + 4, (upper, 1 - ax, both, c), core_peer)

        def step_d(u):
            for n in range(5):
                sends[u, D0 + n].wait_recv()

        def arrive(i):
            if i + 3 < units:
                step_a(i + 3)
            if i + 2 < units:
                step_b(i + 2)
            if i + 1 < units:
                step_c(i + 1)
            if i == units - 2:
                swap_dy.start()
            step_d(i)

        def warm_up():
            step_a(0)
            step_a(1)
            step_b(0)
            step_a(2)
            step_b(1)
            step_c(0)
    else:
        def arrive(i):
            if i == units - 2:
                swap_dy.start()
            own[i].wait()

        def warm_up():
            pass

    def columns(u, at):
        return w[u, :, :, :, :, :, at].reshape(width, CHUNK)

    def row_block(u, i):
        return w[u, i].reshape(CHUNK, width)

    def chunk(i):
        return pl.ds(pl.multiple_of(i * CHUNK, CHUNK), CHUNK)

    def tile(i):
        return pl.ds(pl.multiple_of(i * TILE, TILE), TILE)

    def project(u, dst, bias, scale):
        @phase("proj", 0, width // CHUNK)
        def _(i):
            at = chunk(i)
            value = dot_nn(x[...], columns(u, at))
            if bias is not None:
                value = value + par[bias, :, at]
            if scale is not None:
                value = value * scale
            dst[:, at] = value.astype(BF16)

    lane = lax.broadcasted_iota(jnp.int32, (BLOCK, PAIR), 1)
    low_half = lane < PAIR // 2
    row_lane = lax.broadcasted_iota(jnp.int32, (1, PAIR), 1)
    first_head = jnp.where(row_lane < PAIR // 2, 1.0, 0.0).astype(BF16)
    second_head = jnp.where(row_lane < PAIR // 2, 0.0, 1.0).astype(BF16)

    def heads(value):
        return jnp.concatenate([value * first_head, value * second_head], axis=0)

    def merged(value):
        return jnp.where(low_half, value[:BLOCK], value[BLOCK:])

    def softmax(scores, usable):
        scores = jnp.where(usable, scores, MASKED)
        weight = jnp.exp(scores - jnp.max(scores, axis=0, keepdims=True))
        return weight * (1.0 / jnp.sum(weight, axis=0, keepdims=True))

    pairs = width // PAIR
    per_row = width // (2 * BLOCK)
    own_rows = pl.ds(short_rows, 2 * BLOCK)

    def pair_at(h):
        return slice(h * PAIR, (h + 1) * PAIR)

    def short_kept(s, h):
        start = (s % 4) * (pairs // per_row) + h // per_row
        col = h % per_row * 2 * BLOCK
        return s // 4, pl.ds(pl.multiple_of(start * BLOCK, BLOCK), BLOCK), slice(col, col + 2 * BLOCK)

    def long_kept(n, h):
        rows = pl.ds(pl.multiple_of(h // per_row * 4 * BLOCK, 4 * BLOCK), 4 * BLOCK)
        return 2 + n, rows, pl.ds(pl.multiple_of(h % per_row * 2 * BLOCK, 2 * BLOCK), 2 * BLOCK)

    def short_forward(s):
        rows = pl.ds(pl.multiple_of(s * BLOCK, BLOCK), BLOCK)
        usable = lax.broadcasted_iota(jnp.int32, (BLOCK, 2 * BLOCK), 0) < short_len[s]
        for h in range(pairs):
            at = pair_at(h)
            p = softmax(dot_nt(k[rows, at], heads(q[rows, at])), usable).astype(BF16)
            hid[short_kept(s, h)] = p
            g[rows, at] = merged(dot_tn(p, v[rows, at])).astype(BF16)

    def long_usable():
        key = lax.broadcasted_iota(jnp.int32, (4 * BLOCK, 2 * BLOCK), 0)
        block = key // BLOCK
        mine = key + (block + c) * BLOCK
        other = key + (block - 3 - c) * BLOCK
        return jnp.where(block < 2, mine, other) < long_len[y]

    def long_pair(h):
        return pl.ds(pl.multiple_of(h * PAIR, PAIR), PAIR)

    def long_forward(h):
        at = long_pair(h)
        usable = long_usable()
        for n in range(2):
            rows = pl.ds(short_rows + n * BLOCK, BLOCK)
            qm = heads(q[rows, at])
            scores = jnp.concatenate([dot_nt(k[own_rows, at], qm), dot_nt(kv_sib[0, :, at], qm)], axis=0)
            p = softmax(scores, usable).astype(BF16)
            hid[long_kept(n, h)] = p
            o2 = dot_tn(p[: 2 * BLOCK], v[own_rows, at]) + dot_tn(p[2 * BLOCK :], kv_sib[1, :, at])
            g[rows, at] = merged(o2).astype(BF16)

    def norm_parts(value):
        center = value - jnp.mean(value, axis=1, keepdims=True)
        scale = lax.rsqrt(jnp.mean(center * center, axis=1, keepdims=True) + EPSILON)
        return center * scale, scale

    def norm_back(grad, gain, normed, scale):
        grad = grad * gain
        return scale * (
            grad - jnp.mean(grad, axis=1, keepdims=True) - normed * jnp.mean(grad * normed, axis=1, keepdims=True))

    def row_sum(value):
        return jnp.sum(value, axis=0, keepdims=True)

    def add_sum(row, at, value):
        acc[0, row : row + 1, at] += row_sum(value)

    acc[0] = jnp.zeros_like(acc[0])
    tail[0] = jnp.zeros_like(tail[0])
    for cp in small_loads:
        cp.wait()
    for j in range(hidden_chunks):
        if remote:
            par[U_BIAS + j] = jnp.concatenate(every_fourth([wide_par[...]], j, lanes, hidden_chunks), axis=1)
        else:
            par[U_BIAS + j] = wide_par[:, j * width : (j + 1) * width]
    for cp in loads:
        cp.wait()
    warm_up()
    arrive(K_UNIT)
    swap_x.wait_recv()
    project(K_UNIT, k, None, None)
    arrive(V_UNIT)
    project(V_UNIT, v, V_BIAS, None)
    swap_k = misc(2, k.at[own_rows], kv_sib.at[0], core_peer)
    swap_v = misc(3, v.at[own_rows], kv_sib.at[1], core_peer)
    arrive(Q_UNIT)
    swap_k.start()
    swap_v.start()
    project(Q_UNIT, q, Q_BIAS, SCALE)

    @phase("sf", 0, nshort // 2)
    def _(s):
        short_forward(s)

    arrive(O_UNIT)

    @phase("sf2", nshort // 2, nshort)
    def _(s):
        short_forward(s)

    arrive(UP_UNIT)
    swap_k.wait_recv()
    swap_v.wait_recv()

    @phase("lf", 0, pairs)
    def _(h):
        long_forward(h)

    swap_k.wait_send()
    swap_v.wait_send()
    park = pltpu.make_async_copy(hid, parked, store_sem.at[4])
    park.start()
    arrive(UP_UNIT + 1)

    @phase("wo", 0, width // CHUNK)
    def _(i):
        at = chunk(i)
        r[:, at] = x[:, at].astype(F32) + dot_nn(g[...], columns(O_UNIT, at)) + par[O_BIAS, :, at]

    @phase("ln1", 0, total // TILE)
    def _(i):
        rows = tile(i)
        normed, _ = norm_parts(r[rows, :])
        value = normed * par[GAIN1] + par[SHIFT1]
        a16[rows, :] = value.astype(BF16)
        f[rows, :] = value + par[D_BIAS]

    park.wait()
    for j in range(hidden_chunks):
        up, down = UP_UNIT + 2 * j, UP_UNIT + 2 * j + 1
        if j == 0:
            arrive(down + 1)
        elif j > 1:
            arrive(up)

        @phase("up", 0, width // CHUNK)
        def _(i):
            at = chunk(i)
            value = dot_nn(a16[...], columns(up, at)) + par[U_BIAS + j, :, at]
            active, slope = gelu_parts(value)
            hid[j, :, at] = slope.astype(BF16)
            g[:, at] = active.astype(BF16)

        if j == hidden_chunks - 2:
            for cp in late:
                cp.start()
        if j > 0:
            arrive(down)

        @phase("down", 0, width // CHUNK)
        def _(i):
            at = chunk(i)
            f[:, at] += dot_nn(g[...], columns(down, at))

    for cp in late:
        cp.wait()
    swap_dy.wait_recv()

    @phase("ln2", 0, total // TILE)
    def _(i):
        rows = tile(i)
        normed, scale = norm_parts(f[rows, :])
        upstream = dy[rows, :].astype(F32)
        dy[rows, :] = (normed * par[GAIN2] + par[SHIFT2]).astype(BF16)
        grad = norm_back(upstream, par[GAIN2], normed, scale)
        f[rows, :] = grad
        a16[rows, :] = grad.astype(BF16)
        add_sum(S_SUM, slice(None), upstream)
        add_sum(D_SUM, slice(None), grad)

    out_copies = [
        pltpu.make_async_copy(dy.at[pl.ds(0, short_rows)], so, store_sem.at[0]),
        pltpu.make_async_copy(dy.at[pl.ds(short_rows + BLOCK * y, BLOCK)], lo.at[y], store_sem.at[1]),
    ]
    for cp in out_copies:
        cp.start()
    swap_out = misc(4, dy.at[pl.ds(short_rows + BLOCK * (1 - y), BLOCK)], lo.at[y], y_peer)
    swap_out.start()

    @phase("dg", 0, hidden_chunks * (width // CHUNK))
    def _(n):
        j = n // (width // CHUNK)
        i = n % (width // CHUNK)
        at = chunk(i)
        value = dot_nt(a16[...], row_block(UP_UNIT + 1 + 2 * j, i)) * hid[j, :, at].astype(F32)
        hid[j, :, at] = value.astype(BF16)
        acc[0, pl.ds(U_SUM + j, 1), at] += row_sum(value)

    @phase("da", 0, width // CHUNK)
    def _(i):
        at = chunk(i)
        value = f[:, at]
        for j in range(hidden_chunks):
            value = value + dot_nt(hid[j], row_block(UP_UNIT + 2 * j, i))
        f[:, at] = value

    unpark = pltpu.make_async_copy(parked, hid, store_sem.at[5])
    unpark.start()

    @phase("ln1b", 0, total // TILE)
    def _(i):
        rows = tile(i)
        normed, scale = norm_parts(r[rows, :])
        upstream = f[rows, :]
        grad = norm_back(upstream, par[GAIN1], normed, scale)
        r[rows, :] = grad
        a16[rows, :] = grad.astype(BF16)
        add_sum(F_SUM, slice(None), upstream)
        add_sum(O_SUM, slice(None), grad)

    def early(n):
        return misc(8 + n, acc.at[n], acc_in.at[n], partners[n])

    def finish_early(n):
        early(n).wait_recv()
        early(n).wait_send()
        acc[n + 1] = acc[n] + acc_in[n]

    def next_early(n):
        if n > 0:
            finish_early(n - 1)
        early(n).start()

    next_early(0)

    @phase("do", 0, width // CHUNK)
    def _(i):
        at = chunk(i)
        g[:, at] = dot_nt(a16[...], row_block(O_UNIT, i)).astype(BF16)

    next_early(1)
    unpark.wait()

    @phase("lb", 0, pairs)
    def _(h):
        at = long_pair(h)
        keys, values = k[own_rows, at], v[own_rows, at]
        keys_far, values_far = kv_sib[0, :, at], kv_sib[1, :, at]
        key_grad = value_grad = query_sum = 0.0
        for n in range(2):
            rows = pl.ds(short_rows + n * BLOCK, BLOCK)
            qm = heads(q[rows, at])
            om = heads(g[rows, at])
            low = hid[long_kept(n, h)]
            p = low.astype(F32)
            back = jnp.concatenate([dot_nt(values, om), dot_nt(values_far, om)], axis=0)
            ds = (p * (back - jnp.sum(back * p, axis=0, keepdims=True))).astype(BF16)
            dq = merged(dot_tn(ds[: 2 * BLOCK], keys) + dot_tn(ds[2 * BLOCK :], keys_far)) * SCALE
            q[rows, at] = dq.astype(BF16)
            query_sum = query_sum + row_sum(dq)
            key_grad = key_grad + dot_nn(ds, qm)
            value_grad = value_grad + dot_nn(low, om)
        k[own_rows, at] = key_grad[: 2 * BLOCK].astype(BF16)
        v[own_rows, at] = value_grad[: 2 * BLOCK].astype(BF16)
        kv_sib[0, :, at] = key_grad[2 * BLOCK :].astype(BF16)
        kv_sib[1, :, at] = value_grad[2 * BLOCK :].astype(BF16)
        tail[0, Q_SUM : Q_SUM + 1, at] += query_sum
        tail[0, V_SUM : V_SUM + 1, at] += row_sum(value_grad)

    def short_backward(s):
        rows = pl.ds(pl.multiple_of(s * BLOCK, BLOCK), BLOCK)
        for h in range(pairs):
            at = pair_at(h)
            qm = heads(q[rows, at])
            om = heads(g[rows, at])
            keys = k[rows, at]
            low = hid[short_kept(s, h)]
            p = low.astype(F32)
            back = dot_nt(v[rows, at], om)
            ds = (p * (back - jnp.sum(back * p, axis=0, keepdims=True))).astype(BF16)
            dq = merged(dot_tn(ds, keys)) * SCALE
            dk = dot_nn(ds, qm)
            dv = dot_nn(low, om)
            q[rows, at] = dq.astype(BF16)
            k[rows, at] = dk.astype(BF16)
            v[rows, at] = dv.astype(BF16)
            tail[0, Q_SUM : Q_SUM + 1, at] += row_sum(dq)
            tail[0, V_SUM : V_SUM + 1, at] += row_sum(dv)

    next_early(2)

    @phase("sb1", 0, 1)
    def _(s):
        short_backward(s)

    swap_dkv = misc(5, kv_sib, dkv_in, core_peer)
    swap_dkv.start()
    next_early(3)

    @phase("sb2", 1, nshort)
    def _(s):
        short_backward(s)

    steps = len(partners)

    def late_sum(n):
        return misc(8 + steps + n, tail.at[n], tail_in.at[n], partners[n])

    def finish_late(n):
        late_sum(n).wait_recv()
        late_sum(n).wait_send()
        tail[n + 1] = tail[n] + tail_in[n]

    def next_late(n):
        if n > 0:
            finish_late(n - 1)
        late_sum(n).start()

    next_late(0)
    for n in range(4, steps):
        next_early(n)
    swap_dkv.wait_recv()
    k[own_rows, :] = (k[own_rows, :].astype(F32) + dkv_in[0].astype(F32)).astype(BF16)
    v[own_rows, :] = (v[own_rows, :].astype(F32) + dkv_in[1].astype(F32)).astype(BF16)

    def input_grad(rows, i):
        at = chunk(i)
        value = r[rows, at]
        for ref, u in ((q, Q_UNIT), (k, K_UNIT), (v, V_UNIT)):
            value = value + dot_nt(ref[rows, :], row_block(u, i))
        x[rows, at] = value.astype(BF16)

    @phase("gxl", 0, width // CHUNK)
    def _(i):
        input_grad(own_rows, i)

    swap_grad = misc(6, x.at[pl.ds(short_rows + BLOCK * (1 - y), BLOCK)], lg.at[y], y_peer)
    swap_grad.start()
    finish_early(steps - 1)
    next_late(1)
    for i in range(width // CHUNK):

        @phase("gxs", i, i + 1)
        def _(n):
            input_grad(pl.ds(0, short_rows), n)

        if i + 2 < steps:
            next_late(i + 2)
    for n in range(width // CHUNK + 2, steps):
        next_late(n)
    finish_late(steps - 1)
    sums[0:2, :] = tail[steps]
    sums[2:6, :] = acc[steps, 0:4, :]
    hidden_sums = [acc[steps, U_SUM + j : U_SUM + j + 1, :] for j in range(hidden_chunks)]
    if remote:
        order = [hidden_sums[j][:, n * lanes : (n + 1) * lanes]
                 for n in range(width // lanes) for j in range(hidden_chunks)]
        up_sums[...] = jnp.concatenate(order, axis=1)
    else:
        up_sums[...] = jnp.concatenate(hidden_sums, axis=1)

    grad_copies = [
        pltpu.make_async_copy(x.at[pl.ds(0, short_rows)], sg, store_sem.at[2]),
        pltpu.make_async_copy(x.at[pl.ds(short_rows + BLOCK * y, BLOCK)], lg.at[y], store_sem.at[3]),
    ]
    for cp in grad_copies:
        cp.start()
    swap_out.wait_recv()
    swap_grad.wait_recv()
    for cp in out_copies + grad_copies:
        cp.wait()
    for cp in (swap_x, swap_dy, swap_out, swap_dkv, swap_grad):
        cp.wait_send()
    for key in sends:
        sends[key].wait_send()


def whole_step(shards, small, xs, xl, dys, dyl, short_len, long_len, remote):
    dp_size, seq_size = lax.axis_size("dp"), lax.axis_size("seq")
    width = xs.shape[1]
    nshort = xs.shape[0] // BLOCK
    total = xs.shape[0] + xl.shape[0] * BLOCK
    hidden_chunks = small[-1].shape[1] // width
    units = 4 + 2 * hidden_chunks
    lead = (width // CHUNK, 2, 2, 2, CHUNK // 8, width)
    slots = lead[0] + 8
    steps = (dp_size * seq_size).bit_length() - 1
    anywhere = pl.BlockSpec(memory_space=pl.ANY)
    smem = pl.BlockSpec(memory_space=pltpu.SMEM)
    vmem = pl.BlockSpec(memory_space=pltpu.VMEM)
    act = pltpu.VMEM((total, width), BF16)
    wide = pltpu.VMEM((total, width), F32)
    side = pltpu.VMEM((2, 2 * BLOCK, width), BF16)
    dma = pltpu.SemaphoreType.DMA
    return pl.pallas_call(
        functools.partial(step_kernel, remote, dp_size, seq_size, nshort),
        out_shape=(
            jax.ShapeDtypeStruct(xs.shape, BF16),
            jax.ShapeDtypeStruct(xl.shape, BF16),
            jax.ShapeDtypeStruct(xs.shape, BF16),
            jax.ShapeDtypeStruct(xl.shape, BF16),
            jax.ShapeDtypeStruct((8, width), F32),
            jax.ShapeDtypeStruct((1, hidden_chunks * width), F32),
            jax.ShapeDtypeStruct((hidden_chunks, total, width), BF16),
        ),
        in_specs=[anywhere] * (len(shards) + len(small) + 4) + [smem] * 2,
        out_specs=(anywhere,) * 4 + (vmem,) * 2 + (anywhere,),
        scratch_shapes=[
            pltpu.VMEM((U_BIAS + hidden_chunks, 1, width), F32),
            pltpu.VMEM((1, hidden_chunks * width), F32),
            pltpu.VMEM((units, *lead), BF16),
            act, act, act, act, side, side, act, wide, act,
            pltpu.VMEM((hidden_chunks, total, width), BF16),
            wide, act,
            pltpu.VMEM((steps + 1, 4 + hidden_chunks, width), F32),
            pltpu.VMEM((steps, 4 + hidden_chunks, width), F32),
            pltpu.VMEM((steps + 1, 2, width), F32),
            pltpu.VMEM((steps, 2, width), F32),
            dma((units, slots)), dma((units, slots)), dma((8 + 2 * steps,)), dma((8 + 2 * steps,)),
            dma((units,)), dma((len(small),)), dma((4,)), dma((6,)),
        ],
        compiler_params=pltpu.CompilerParams(
            collective_id=0, has_side_effects=True, vmem_limit_bytes=67043328),
        name="whole_step",
    )(*shards, *small, xs, xl, dys, dyl, short_len, long_len)


def on_device(
    short_input, long_input, short_cotangent, long_cotangent, short_lengths, long_lengths,
    query_weight, key_weight, value_weight, output_weight, upward_weight, downward_weight,
    query_bias, value_bias, output_bias, upward_bias, downward_bias,
    first_gain, first_shift, second_gain, second_shift,
):
    rows, width = query_weight.shape
    devices = lax.axis_size("dp") * lax.axis_size("seq")
    hidden_chunks = upward_weight.shape[1] // width
    shape = short_input.shape

    def permuted(value):
        lead = value.shape[:-1]
        value = value.reshape(*lead, devices, hidden_chunks, rows)
        return jnp.moveaxis(value, -2, 0).reshape(hidden_chunks, *lead, width)

    remote = rows == 32 and lax.axis_size("seq") == 4
    small = [query_bias, value_bias, output_bias, downward_bias, first_gain, first_shift, second_gain, second_shift]
    if remote:
        shards = [key_weight, value_weight, query_weight, output_weight, upward_weight, downward_weight]
        small.append(upward_bias)
    else:
        upward = permuted(upward_weight)
        downward = downward_weight.reshape(hidden_chunks, rows, width)
        parts = [key_weight, value_weight, query_weight, output_weight]
        for j in range(hidden_chunks):
            parts += [upward[j], downward[j]]
        whole = lax.all_gather(jnp.stack([part.astype(BF16) for part in parts]), ("dp", "seq"), axis=1, tiled=True)
        shards = [whole.reshape(len(parts), width // CHUNK, 2, 2, 2, CHUNK // 8, width)]
        small.append(permuted(upward_bias))
    so, lo, sg, lg, sums, up_sums, _ = whole_step(
        shards, [value.reshape(1, -1) for value in small],
        short_input.reshape(-1, width), long_input, short_cotangent.reshape(-1, width), long_cotangent,
        short_lengths, long_lengths, remote)
    if remote:
        upward_delta = up_sums.reshape(-1)
    else:
        upward_delta = jnp.moveaxis(up_sums.reshape(hidden_chunks, devices, rows), 0, 1).reshape(-1)
    query_delta, value_delta, output_delta, downward_delta, first_delta, second_delta = (sums[n] for n in range(6))
    return (
        so.reshape(shape), lo, sg.reshape(shape), lg,
        query_delta, value_delta, output_delta, upward_delta, downward_delta, first_delta, second_delta,
    )


def solution(mesh):
    split = ("dp", "seq")
    placed = (
        P(split, None, None), P("dp", "seq", None), P(split, None, None), P("dp", "seq", None),
        P(split), P("dp"),
        *(P(split, None) for _ in range(6)), *(P() for _ in range(9)),
    )
    return jax.shard_map(
        on_device,
        mesh=mesh,
        in_specs=placed,
        out_specs=(
            P(split, None, None), P("dp", "seq", None), P(split, None, None), P("dp", "seq", None),
            *(P() for _ in range(7)),
        ),
        check_vma=False,
    )
```

```python
import functools

import jax
import jax.numpy as jnp
from jax import lax
from jax.experimental import pallas as pl
from jax.experimental.pallas import tpu as pltpu
from jax.sharding import PartitionSpec as P

MESH = pl.DeviceIdType.MESH


def phase(name, start, stop):
    return pl.loop(start, stop)


F32 = jnp.float32
BF16 = jnp.bfloat16
EPSILON = 1e-12
MASKED = -1e30
SCALE = 0.125
PAIR = 128
BLOCK = 128
CHUNK = 256
TILE = 256
K_UNIT, V_UNIT, Q_UNIT, O_UNIT, UP_UNIT = 0, 1, 2, 3, 4
Q_BIAS, V_BIAS, O_BIAS, D_BIAS, GAIN1, SHIFT1, GAIN2, SHIFT2, U_BIAS = 0, 1, 2, 3, 4, 5, 6, 7, 8
Q_SUM, V_SUM = 0, 1
O_SUM, D_SUM, F_SUM, S_SUM, U_SUM = 0, 1, 2, 3, 4


def dot_nn(a, b):
    return jnp.dot(a, b, preferred_element_type=F32)


def dot_nt(a, b):
    return lax.dot_general(a, b, (((1,), (1,)), ((), ())), preferred_element_type=F32)


def dot_tn(a, b):
    return lax.dot_general(a, b, (((0,), (0,)), ((), ())), preferred_element_type=F32)


def flipped(index, bit):
    return index + bit * (1 - 2 * ((index // bit) % 2))


def gelu_parts(u):
    square = u * u
    t = jnp.tanh(0.7978845608028654 * (u + 0.044715 * (u * square)))
    half = 0.5 * (1.0 + t)
    slope = half + 0.5 * u * (1.0 - t * t) * (0.7978845608028654 * (1.0 + 3 * 0.044715 * square))
    return u * half, slope


def every_fourth(pieces, j, lanes, stride):
    found = []
    for piece in pieces:
        for start in range(j * lanes, piece.shape[1], stride * lanes):
            found.append(piece[:, start : start + lanes])
    return found


def step_kernel(
    remote, dp_size, seq_size, nshort,
    *refs,
):
    given = 6 if remote else 1
    shards, refs = refs[:given], refs[given:]
    small, refs = refs[:9], refs[9:]
    (xs, xl, dys, dyl, short_len, long_len,
     so, lo, sg, lg, sums, up_sums, parked,
     par, wide_par,
     w, x, q, k, v, kv_sib, dkv_in, g, r, a16, hid, f, dy, acc, acc_in, tail, tail_in,
     send_sem, recv_sem, misc_send, misc_recv, own_sem, small_sem, load_sem, store_sem) = refs
    dp = lax.axis_index("dp")
    seq = lax.axis_index("seq")
    y, c = seq // 2, seq % 2
    y_peer = (dp, flipped(seq, 2))
    core_peer = (dp, flipped(seq, 1))
    total, width = x.shape
    short_rows = nshort * BLOCK
    units = w.shape[0]
    depth = w.shape[1]
    hidden_chunks = (units - 4) // 2
    partners = []
    bit = 1
    while bit < seq_size:
        partners.append((dp, flipped(seq, bit)))
        bit *= 2
    bit = 1
    while bit < dp_size:
        partners.append((flipped(dp, bit), seq))
        bit *= 2

    loads = [pltpu.make_async_copy(xs, x.at[pl.ds(0, short_rows)], load_sem.at[0]),
             pltpu.make_async_copy(xl.at[y], x.at[pl.ds(short_rows + BLOCK * y, BLOCK)], load_sem.at[1])]
    late = [pltpu.make_async_copy(dys, dy.at[pl.ds(0, short_rows)], load_sem.at[2]),
            pltpu.make_async_copy(dyl.at[y], dy.at[pl.ds(short_rows + BLOCK * y, BLOCK)], load_sem.at[3])]
    for cp in loads:
        cp.start()

    if remote:
        z, ax = dp // 2, dp % 2
        hops = depth - 1
        z_peers = [((z + n) % depth * 2 + ax, seq) for n in range(1, depth)]
        x_peer = (flipped(dp, 1), seq)
        peers = z_peers + [x_peer, y_peer, core_peer]
        piece = w.shape[5]
        key_shard, value_shard, query_shard, output_shard, up_shard, down_shard = shards
        sources = [key_shard, value_shard, query_shard, output_shard]
        sources += [up_shard.at[:, pl.ds(n * width, width)] for n in range(hidden_chunks)]
        sources += [down_shard.at[pl.ds(n * piece, piece)] for n in range(hidden_chunks)]
        own = [pltpu.make_async_copy(source, f.at[pl.ds(n * piece, piece)], own_sem.at[n])
               for n, source in enumerate(sources)]
    else:
        peers = partners
        own = [pltpu.make_async_copy(shards[0].at[u], w.at[u], own_sem.at[u]) for u in range(units)]
    for cp in own:
        cp.start()
    small_loads = [pltpu.make_async_copy(ref, par.at[n] if n < U_BIAS else wide_par, small_sem.at[n])
                   for n, ref in enumerate(small)]
    for cp in small_loads:
        cp.start()

    barrier = pltpu.get_barrier_semaphore()
    for peer in peers:
        pl.semaphore_signal(barrier, inc=1, device_id=peer, device_id_type=MESH)

    if remote:
        lanes = width // (8 * depth)
        for cp in own:
            cp.wait()
        for u in range(4):
            w[u, z, ax, y, c] = f[u * piece : (u + 1) * piece, :].astype(BF16)
        up_rows = [f[(4 + n) * piece : (5 + n) * piece, :].astype(BF16) for n in range(hidden_chunks)]
        for j in range(hidden_chunks):
            first = (4 + hidden_chunks + j) * piece
            w[UP_UNIT + 2 * j, z, ax, y, c] = jnp.concatenate(every_fourth(up_rows, j, lanes, hidden_chunks), axis=1)
            w[UP_UNIT + 2 * j + 1, z, ax, y, c] = f[first : first + piece, :].astype(BF16)
    pl.semaphore_wait(barrier, len(peers))

    def misc(slot, src, dst, peer):
        return pltpu.make_async_remote_copy(
            src_ref=src, dst_ref=dst, send_sem=misc_send.at[slot], recv_sem=misc_recv.at[slot],
            device_id=peer, device_id_type=MESH)

    swap_x = misc(0, xl.at[1 - y], x.at[pl.ds(short_rows + BLOCK * y, BLOCK)], y_peer)
    swap_dy = misc(1, dyl.at[1 - y], dy.at[pl.ds(short_rows + BLOCK * y, BLOCK)], y_peer)
    swap_x.start()

    sends, inner_sends = {}, []
    if remote:
        half = depth // 2
        lower, upper, every, both = pl.ds(0, half), pl.ds(half, half), pl.ds(0, depth), pl.ds(0, 2)
        pair, far_pair = pl.ds(z // 2 * 2, 2), pl.ds(2 - z // 2 * 2, 2)
        top, bottom = pl.ds(0, piece // 2), pl.ds(piece // 2, piece // 2)
        is_inner = (z + 1) // 2 == 1
        z_next = (flipped(z, 1) * 2 + ax, seq)
        z_across = ((depth - 1 - z) * 2 + ax, seq)
        stages = 6

        def plan(u, slot, part, peer):
            cp = pltpu.make_async_remote_copy(
                src_ref=w.at[(u, *part)], dst_ref=w.at[(u, *part)],
                send_sem=send_sem.at[u, slot], recv_sem=recv_sem.at[u, slot], device_id=peer, device_id_type=MESH)
            sends[u, slot] = cp
            return cp

        def pass_on(u, slot, part, peer):
            plan(u, slot, part, peer).start()

        def from_inner(u, parts):
            copies = [plan(u, slot, part, peer) for slot, part, peer in parts]
            for cp, (slot, _, _) in zip(copies, parts):
                inner_sends.append((u, slot))

            @pl.when(is_inner)
            def _():
                for cp in copies:
                    cp.start()

        def wait_where(here, u, slots):
            @pl.when(here)
            def _():
                for slot in slots:
                    sends[u, slot].wait_recv()

        def wait_for(u, slots):
            for slot in slots:
                sends[u, slot].wait_recv()

        def z_first(u, stage):
            if stage == 0:
                pass_on(u, 0, (z, ax, y, c), z_next)
            elif stage == 1:
                wait_for(u, (0,))
                from_inner(u, [(1, (pair, ax, y, c), z_across)])
            elif stage == 2:
                wait_where(is_inner, u, (1,))
                from_inner(u, [(2, (far_pair, ax, y, c), z_next)])
            elif stage == 3:
                wait_where(jnp.logical_not(is_inner), u, (2,))
                pass_on(u, 3, (lower, ax, y, c), x_peer)
                pass_on(u, 4, (upper, ax, y, c), y_peer)
                pass_on(u, 7, (every, ax, y, c), core_peer)
            elif stage == 4:
                wait_for(u, (3, 4))
                pass_on(u, 5, (lower, both, y, c), y_peer)
                pass_on(u, 6, (upper, ax, both, c), x_peer)
                pass_on(u, 8, (lower, 1 - ax, y, c), core_peer)
                pass_on(u, 9, (upper, ax, 1 - y, c), core_peer)
            elif stage == 5:
                wait_for(u, (5, 6))
                pass_on(u, 10, (lower, both, 1 - y, c), core_peer)
                pass_on(u, 11, (upper, 1 - ax, both, c), core_peer)
            else:
                wait_for(u, range(7, 12))

        def z_second(u, stage):
            if stage == 0:
                pass_on(u, 0, (z, ax, y, c, top), x_peer)
                pass_on(u, 1, (z, ax, y, c, bottom), y_peer)
            elif stage == 1:
                wait_for(u, (0, 1))
                pass_on(u, 2, (z, both, y, c, top), z_next)
                pass_on(u, 3, (z, ax, both, c, bottom), z_next)
            elif stage == 2:
                wait_for(u, (2, 3))
                from_inner(u, [(4, (pair, both, y, c, top), z_across), (5, (pair, ax, both, c, bottom), z_across)])
            elif stage == 3:
                wait_where(is_inner, u, (4, 5))
                from_inner(u, [(6, (far_pair, both, y, c, top), z_next), (7, (far_pair, ax, both, c, bottom), z_next)])
            elif stage == 4:
                wait_where(jnp.logical_not(is_inner), u, (6, 7))
                pass_on(u, 8, (every, both, y, c, top), y_peer)
                pass_on(u, 9, (every, ax, both, c, bottom), x_peer)
                pass_on(u, 10, (every, both, y, c, top), core_peer)
                pass_on(u, 11, (every, ax, both, c, bottom), core_peer)
            elif stage == 5:
                wait_for(u, (8, 9))
                pass_on(u, 12, (every, both, 1 - y, c, top), core_peer)
                pass_on(u, 13, (every, 1 - ax, both, c, bottom), core_peer)
            else:
                wait_for(u, range(10, 14))

        def arrive(i):
            for stage in range(stages + 1):
                u = i + stages - stage
                if 0 <= u < units:
                    (z_first if u % 3 == 0 else z_second)(u, stage)
            if i == units - 2:
                swap_dy.start()

        def warm_up():
            for i in range(-stages, 0):
                arrive(i)
    else:
        def arrive(i):
            if i == units - 2:
                swap_dy.start()
            own[i].wait()

        def warm_up():
            pass

    def columns(u, at):
        return w[u, :, :, :, :, :, at].reshape(width, CHUNK)

    def row_block(u, i):
        return w[u, i].reshape(CHUNK, width)

    def chunk(i):
        return pl.ds(pl.multiple_of(i * CHUNK, CHUNK), CHUNK)

    def tile(i):
        return pl.ds(pl.multiple_of(i * TILE, TILE), TILE)

    def project(u, dst, bias, scale):
        @phase("proj", 0, width // CHUNK)
        def _(i):
            at = chunk(i)
            value = dot_nn(x[...], columns(u, at))
            if bias is not None:
                value = value + par[bias, :, at]
            if scale is not None:
                value = value * scale
            dst[:, at] = value.astype(BF16)

    lane = lax.broadcasted_iota(jnp.int32, (BLOCK, PAIR), 1)
    low_half = lane < PAIR // 2
    row_lane = lax.broadcasted_iota(jnp.int32, (1, PAIR), 1)
    first_head = jnp.where(row_lane < PAIR // 2, 1.0, 0.0).astype(BF16)
    second_head = jnp.where(row_lane < PAIR // 2, 0.0, 1.0).astype(BF16)

    def heads(value):
        return jnp.concatenate([value * first_head, value * second_head], axis=0)

    def merged(value):
        return jnp.where(low_half, value[:BLOCK], value[BLOCK:])

    def softmax(scores, usable):
        scores = jnp.where(usable, scores, MASKED)
        weight = jnp.exp(scores - jnp.max(scores, axis=0, keepdims=True))
        return weight * (1.0 / jnp.sum(weight, axis=0, keepdims=True))

    pairs = width // PAIR
    per_row = width // (2 * BLOCK)
    own_rows = pl.ds(short_rows, 2 * BLOCK)

    def pair_at(h):
        return slice(h * PAIR, (h + 1) * PAIR)

    def short_kept(s, h):
        start = (s % 4) * (pairs // per_row) + h // per_row
        col = h % per_row * 2 * BLOCK
        return s // 4, pl.ds(pl.multiple_of(start * BLOCK, BLOCK), BLOCK), slice(col, col + 2 * BLOCK)

    def long_kept(n, h):
        rows = pl.ds(pl.multiple_of(h // per_row * 4 * BLOCK, 4 * BLOCK), 4 * BLOCK)
        return 2 + n, rows, pl.ds(pl.multiple_of(h % per_row * 2 * BLOCK, 2 * BLOCK), 2 * BLOCK)

    def short_forward(s):
        rows = pl.ds(pl.multiple_of(s * BLOCK, BLOCK), BLOCK)
        usable = lax.broadcasted_iota(jnp.int32, (BLOCK, 2 * BLOCK), 0) < short_len[s]
        for h in range(pairs):
            at = pair_at(h)
            p = softmax(dot_nt(k[rows, at], heads(q[rows, at])), usable).astype(BF16)
            hid[short_kept(s, h)] = p
            g[rows, at] = merged(dot_tn(p, v[rows, at])).astype(BF16)

    def long_usable():
        key = lax.broadcasted_iota(jnp.int32, (4 * BLOCK, 2 * BLOCK), 0)
        block = key // BLOCK
        mine = key + (block + c) * BLOCK
        other = key + (block - 3 - c) * BLOCK
        return jnp.where(block < 2, mine, other) < long_len[y]

    def long_pair(h):
        return pl.ds(pl.multiple_of(h * PAIR, PAIR), PAIR)

    def long_forward(h):
        at = long_pair(h)
        usable = long_usable()
        for n in range(2):
            rows = pl.ds(short_rows + n * BLOCK, BLOCK)
            qm = heads(q[rows, at])
            scores = jnp.concatenate([dot_nt(k[own_rows, at], qm), dot_nt(kv_sib[0, :, at], qm)], axis=0)
            p = softmax(scores, usable).astype(BF16)
            hid[long_kept(n, h)] = p
            o2 = dot_tn(p[: 2 * BLOCK], v[own_rows, at]) + dot_tn(p[2 * BLOCK :], kv_sib[1, :, at])
            g[rows, at] = merged(o2).astype(BF16)

    def norm_parts(value):
        center = value - jnp.mean(value, axis=1, keepdims=True)
        scale = lax.rsqrt(jnp.mean(center * center, axis=1, keepdims=True) + EPSILON)
        return center * scale, scale

    def norm_back(grad, gain, normed, scale):
        grad = grad * gain
        return scale * (
            grad - jnp.mean(grad, axis=1, keepdims=True) - normed * jnp.mean(grad * normed, axis=1, keepdims=True))

    def row_sum(value):
        return jnp.sum(value, axis=0, keepdims=True)

    def add_sum(row, at, value):
        acc[0, row : row + 1, at] += row_sum(value)

    acc[0] = jnp.zeros_like(acc[0])
    tail[0] = jnp.zeros_like(tail[0])
    for cp in small_loads:
        cp.wait()
    for j in range(hidden_chunks):
        if remote:
            par[U_BIAS + j] = jnp.concatenate(every_fourth([wide_par[...]], j, lanes, hidden_chunks), axis=1)
        else:
            par[U_BIAS + j] = wide_par[:, j * width : (j + 1) * width]
    for cp in loads:
        cp.wait()
    warm_up()
    arrive(K_UNIT)
    swap_x.wait_recv()
    project(K_UNIT, k, None, None)
    arrive(V_UNIT)
    project(V_UNIT, v, V_BIAS, None)
    swap_k = misc(2, k.at[own_rows], kv_sib.at[0], core_peer)
    swap_v = misc(3, v.at[own_rows], kv_sib.at[1], core_peer)
    arrive(Q_UNIT)
    swap_k.start()
    swap_v.start()
    project(Q_UNIT, q, Q_BIAS, SCALE)

    @phase("sf", 0, nshort // 2)
    def _(s):
        short_forward(s)

    arrive(O_UNIT)

    @phase("sf2", nshort // 2, nshort)
    def _(s):
        short_forward(s)

    arrive(UP_UNIT)
    swap_k.wait_recv()
    swap_v.wait_recv()

    @phase("lf", 0, pairs)
    def _(h):
        long_forward(h)

    swap_k.wait_send()
    swap_v.wait_send()
    park = pltpu.make_async_copy(hid, parked, store_sem.at[4])
    park.start()
    arrive(UP_UNIT + 1)

    @phase("wo", 0, width // CHUNK)
    def _(i):
        at = chunk(i)
        r[:, at] = x[:, at].astype(F32) + dot_nn(g[...], columns(O_UNIT, at)) + par[O_BIAS, :, at]

    @phase("ln1", 0, total // TILE)
    def _(i):
        rows = tile(i)
        normed, _ = norm_parts(r[rows, :])
        value = normed * par[GAIN1] + par[SHIFT1]
        a16[rows, :] = value.astype(BF16)
        f[rows, :] = value + par[D_BIAS]

    park.wait()
    for j in range(hidden_chunks):
        up, down = UP_UNIT + 2 * j, UP_UNIT + 2 * j + 1
        if j == 0:
            arrive(down + 1)
        elif j > 1:
            arrive(up)

        @phase("up", 0, width // CHUNK)
        def _(i):
            at = chunk(i)
            value = dot_nn(a16[...], columns(up, at)) + par[U_BIAS + j, :, at]
            active, slope = gelu_parts(value)
            hid[j, :, at] = slope.astype(BF16)
            g[:, at] = active.astype(BF16)

        if j == hidden_chunks - 2:
            for cp in late:
                cp.start()
        if j > 0:
            arrive(down)

        @phase("down", 0, width // CHUNK)
        def _(i):
            at = chunk(i)
            f[:, at] += dot_nn(g[...], columns(down, at))

    for cp in late:
        cp.wait()
    swap_dy.wait_recv()

    @phase("ln2", 0, total // TILE)
    def _(i):
        rows = tile(i)
        normed, scale = norm_parts(f[rows, :])
        upstream = dy[rows, :].astype(F32)
        dy[rows, :] = (normed * par[GAIN2] + par[SHIFT2]).astype(BF16)
        grad = norm_back(upstream, par[GAIN2], normed, scale)
        f[rows, :] = grad
        a16[rows, :] = grad.astype(BF16)
        add_sum(S_SUM, slice(None), upstream)
        add_sum(D_SUM, slice(None), grad)

    out_copies = [
        pltpu.make_async_copy(dy.at[pl.ds(0, short_rows)], so, store_sem.at[0]),
        pltpu.make_async_copy(dy.at[pl.ds(short_rows + BLOCK * y, BLOCK)], lo.at[y], store_sem.at[1]),
    ]
    for cp in out_copies:
        cp.start()
    swap_out = misc(4, dy.at[pl.ds(short_rows + BLOCK * (1 - y), BLOCK)], lo.at[y], y_peer)
    swap_out.start()

    @phase("dg", 0, hidden_chunks * (width // CHUNK))
    def _(n):
        j = n // (width // CHUNK)
        i = n % (width // CHUNK)
        at = chunk(i)
        value = dot_nt(a16[...], row_block(UP_UNIT + 1 + 2 * j, i)) * hid[j, :, at].astype(F32)
        hid[j, :, at] = value.astype(BF16)
        acc[0, pl.ds(U_SUM + j, 1), at] += row_sum(value)

    @phase("da", 0, width // CHUNK)
    def _(i):
        at = chunk(i)
        value = f[:, at]
        for j in range(hidden_chunks):
            value = value + dot_nt(hid[j], row_block(UP_UNIT + 2 * j, i))
        f[:, at] = value

    unpark = pltpu.make_async_copy(parked, hid, store_sem.at[5])
    unpark.start()

    @phase("ln1b", 0, total // TILE)
    def _(i):
        rows = tile(i)
        normed, scale = norm_parts(r[rows, :])
        upstream = f[rows, :]
        grad = norm_back(upstream, par[GAIN1], normed, scale)
        r[rows, :] = grad
        a16[rows, :] = grad.astype(BF16)
        add_sum(F_SUM, slice(None), upstream)
        add_sum(O_SUM, slice(None), grad)

    def early(n):
        return misc(8 + n, acc.at[n], acc_in.at[n], partners[n])

    def finish_early(n):
        early(n).wait_recv()
        early(n).wait_send()
        acc[n + 1] = acc[n] + acc_in[n]

    def next_early(n):
        if n > 0:
            finish_early(n - 1)
        early(n).start()

    next_early(0)

    @phase("do", 0, width // CHUNK)
    def _(i):
        at = chunk(i)
        g[:, at] = dot_nt(a16[...], row_block(O_UNIT, i)).astype(BF16)

    next_early(1)
    unpark.wait()

    @phase("lb", 0, pairs)
    def _(h):
        at = long_pair(h)
        keys, values = k[own_rows, at], v[own_rows, at]
        keys_far, values_far = kv_sib[0, :, at], kv_sib[1, :, at]
        key_grad = value_grad = query_sum = 0.0
        for n in range(2):
            rows = pl.ds(short_rows + n * BLOCK, BLOCK)
            qm = heads(q[rows, at])
            om = heads(g[rows, at])
            low = hid[long_kept(n, h)]
            p = low.astype(F32)
            back = jnp.concatenate([dot_nt(values, om), dot_nt(values_far, om)], axis=0)
            ds = (p * (back - jnp.sum(back * p, axis=0, keepdims=True))).astype(BF16)
            dq = merged(dot_tn(ds[: 2 * BLOCK], keys) + dot_tn(ds[2 * BLOCK :], keys_far)) * SCALE
            q[rows, at] = dq.astype(BF16)
            query_sum = query_sum + row_sum(dq)
            key_grad = key_grad + dot_nn(ds, qm)
            value_grad = value_grad + dot_nn(low, om)
        k[own_rows, at] = key_grad[: 2 * BLOCK].astype(BF16)
        v[own_rows, at] = value_grad[: 2 * BLOCK].astype(BF16)
        kv_sib[0, :, at] = key_grad[2 * BLOCK :].astype(BF16)
        kv_sib[1, :, at] = value_grad[2 * BLOCK :].astype(BF16)
        tail[0, Q_SUM : Q_SUM + 1, at] += query_sum
        tail[0, V_SUM : V_SUM + 1, at] += row_sum(value_grad)

    def short_backward(s):
        rows = pl.ds(pl.multiple_of(s * BLOCK, BLOCK), BLOCK)
        for h in range(pairs):
            at = pair_at(h)
            qm = heads(q[rows, at])
            om = heads(g[rows, at])
            keys = k[rows, at]
            low = hid[short_kept(s, h)]
            p = low.astype(F32)
            back = dot_nt(v[rows, at], om)
            ds = (p * (back - jnp.sum(back * p, axis=0, keepdims=True))).astype(BF16)
            dq = merged(dot_tn(ds, keys)) * SCALE
            dk = dot_nn(ds, qm)
            dv = dot_nn(low, om)
            q[rows, at] = dq.astype(BF16)
            k[rows, at] = dk.astype(BF16)
            v[rows, at] = dv.astype(BF16)
            tail[0, Q_SUM : Q_SUM + 1, at] += row_sum(dq)
            tail[0, V_SUM : V_SUM + 1, at] += row_sum(dv)

    next_early(2)

    @phase("sb1", 0, 1)
    def _(s):
        short_backward(s)

    swap_dkv = misc(5, kv_sib, dkv_in, core_peer)
    swap_dkv.start()
    next_early(3)

    @phase("sb2", 1, nshort)
    def _(s):
        short_backward(s)

    steps = len(partners)

    def late_sum(n):
        return misc(8 + steps + n, tail.at[n], tail_in.at[n], partners[n])

    def finish_late(n):
        late_sum(n).wait_recv()
        late_sum(n).wait_send()
        tail[n + 1] = tail[n] + tail_in[n]

    def next_late(n):
        if n > 0:
            finish_late(n - 1)
        late_sum(n).start()

    next_late(0)
    for n in range(4, steps):
        next_early(n)
    swap_dkv.wait_recv()
    k[own_rows, :] = (k[own_rows, :].astype(F32) + dkv_in[0].astype(F32)).astype(BF16)
    v[own_rows, :] = (v[own_rows, :].astype(F32) + dkv_in[1].astype(F32)).astype(BF16)

    def input_grad(rows, i):
        at = chunk(i)
        value = r[rows, at]
        for ref, u in ((q, Q_UNIT), (k, K_UNIT), (v, V_UNIT)):
            value = value + dot_nt(ref[rows, :], row_block(u, i))
        x[rows, at] = value.astype(BF16)

    @phase("gxl", 0, width // CHUNK)
    def _(i):
        input_grad(own_rows, i)

    swap_grad = misc(6, x.at[pl.ds(short_rows + BLOCK * (1 - y), BLOCK)], lg.at[y], y_peer)
    swap_grad.start()
    finish_early(steps - 1)
    next_late(1)
    for i in range(width // CHUNK):

        @phase("gxs", i, i + 1)
        def _(n):
            input_grad(pl.ds(0, short_rows), n)

        if i + 2 < steps:
            next_late(i + 2)
    for n in range(width // CHUNK + 2, steps):
        next_late(n)
    finish_late(steps - 1)
    sums[0:2, :] = tail[steps]
    sums[2:6, :] = acc[steps, 0:4, :]
    hidden_sums = [acc[steps, U_SUM + j : U_SUM + j + 1, :] for j in range(hidden_chunks)]
    if remote:
        order = [hidden_sums[j][:, n * lanes : (n + 1) * lanes]
                 for n in range(width // lanes) for j in range(hidden_chunks)]
        up_sums[...] = jnp.concatenate(order, axis=1)
    else:
        up_sums[...] = jnp.concatenate(hidden_sums, axis=1)

    grad_copies = [
        pltpu.make_async_copy(x.at[pl.ds(0, short_rows)], sg, store_sem.at[2]),
        pltpu.make_async_copy(x.at[pl.ds(short_rows + BLOCK * y, BLOCK)], lg.at[y], store_sem.at[3]),
    ]
    for cp in grad_copies:
        cp.start()
    swap_out.wait_recv()
    swap_grad.wait_recv()
    for cp in out_copies + grad_copies:
        cp.wait()
    for cp in (swap_x, swap_dy, swap_out, swap_dkv, swap_grad):
        cp.wait_send()
    for key in sends:
        if key not in inner_sends:
            sends[key].wait_send()
    if inner_sends:
        @pl.when(is_inner)
        def _():
            for key in inner_sends:
                sends[key].wait_send()


def whole_step(shards, small, xs, xl, dys, dyl, short_len, long_len, remote):
    dp_size, seq_size = lax.axis_size("dp"), lax.axis_size("seq")
    width = xs.shape[1]
    nshort = xs.shape[0] // BLOCK
    total = xs.shape[0] + xl.shape[0] * BLOCK
    hidden_chunks = small[-1].shape[1] // width
    units = 4 + 2 * hidden_chunks
    lead = (width // CHUNK, 2, 2, 2, CHUNK // 8, width)
    slots = 14
    steps = (dp_size * seq_size).bit_length() - 1
    anywhere = pl.BlockSpec(memory_space=pl.ANY)
    smem = pl.BlockSpec(memory_space=pltpu.SMEM)
    vmem = pl.BlockSpec(memory_space=pltpu.VMEM)
    act = pltpu.VMEM((total, width), BF16)
    wide = pltpu.VMEM((total, width), F32)
    side = pltpu.VMEM((2, 2 * BLOCK, width), BF16)
    dma = pltpu.SemaphoreType.DMA
    return pl.pallas_call(
        functools.partial(step_kernel, remote, dp_size, seq_size, nshort),
        out_shape=(
            jax.ShapeDtypeStruct(xs.shape, BF16),
            jax.ShapeDtypeStruct(xl.shape, BF16),
            jax.ShapeDtypeStruct(xs.shape, BF16),
            jax.ShapeDtypeStruct(xl.shape, BF16),
            jax.ShapeDtypeStruct((8, width), F32),
            jax.ShapeDtypeStruct((1, hidden_chunks * width), F32),
            jax.ShapeDtypeStruct((hidden_chunks, total, width), BF16),
        ),
        in_specs=[anywhere] * (len(shards) + len(small) + 4) + [smem] * 2,
        out_specs=(anywhere,) * 4 + (vmem,) * 2 + (anywhere,),
        scratch_shapes=[
            pltpu.VMEM((U_BIAS + hidden_chunks, 1, width), F32),
            pltpu.VMEM((1, hidden_chunks * width), F32),
            pltpu.VMEM((units, *lead), BF16),
            act, act, act, act, side, side, act, wide, act,
            pltpu.VMEM((hidden_chunks, total, width), BF16),
            wide, act,
            pltpu.VMEM((steps + 1, 4 + hidden_chunks, width), F32),
            pltpu.VMEM((steps, 4 + hidden_chunks, width), F32),
            pltpu.VMEM((steps + 1, 2, width), F32),
            pltpu.VMEM((steps, 2, width), F32),
            dma((units, slots)), dma((units, slots)), dma((8 + 2 * steps,)), dma((8 + 2 * steps,)),
            dma((units,)), dma((len(small),)), dma((4,)), dma((6,)),
        ],
        compiler_params=pltpu.CompilerParams(
            collective_id=0, has_side_effects=True, vmem_limit_bytes=67043328),
        name="whole_step",
    )(*shards, *small, xs, xl, dys, dyl, short_len, long_len)


def on_device(
    short_input, long_input, short_cotangent, long_cotangent, short_lengths, long_lengths,
    query_weight, key_weight, value_weight, output_weight, upward_weight, downward_weight,
    query_bias, value_bias, output_bias, upward_bias, downward_bias,
    first_gain, first_shift, second_gain, second_shift,
):
    rows, width = query_weight.shape
    devices = lax.axis_size("dp") * lax.axis_size("seq")
    hidden_chunks = upward_weight.shape[1] // width
    shape = short_input.shape

    def permuted(value):
        lead = value.shape[:-1]
        value = value.reshape(*lead, devices, hidden_chunks, rows)
        return jnp.moveaxis(value, -2, 0).reshape(hidden_chunks, *lead, width)

    remote = rows == 32 and lax.axis_size("seq") == 4
    small = [query_bias, value_bias, output_bias, downward_bias, first_gain, first_shift, second_gain, second_shift]
    if remote:
        shards = [key_weight, value_weight, query_weight, output_weight, upward_weight, downward_weight]
        small.append(upward_bias)
    else:
        upward = permuted(upward_weight)
        downward = downward_weight.reshape(hidden_chunks, rows, width)
        parts = [key_weight, value_weight, query_weight, output_weight]
        for j in range(hidden_chunks):
            parts += [upward[j], downward[j]]
        whole = lax.all_gather(jnp.stack([part.astype(BF16) for part in parts]), ("dp", "seq"), axis=1, tiled=True)
        shards = [whole.reshape(len(parts), width // CHUNK, 2, 2, 2, CHUNK // 8, width)]
        small.append(permuted(upward_bias))
    so, lo, sg, lg, sums, up_sums, _ = whole_step(
        shards, [value.reshape(1, -1) for value in small],
        short_input.reshape(-1, width), long_input, short_cotangent.reshape(-1, width), long_cotangent,
        short_lengths, long_lengths, remote)
    if remote:
        upward_delta = up_sums.reshape(-1)
    else:
        upward_delta = jnp.moveaxis(up_sums.reshape(hidden_chunks, devices, rows), 0, 1).reshape(-1)
    query_delta, value_delta, output_delta, downward_delta, first_delta, second_delta = (sums[n] for n in range(6))
    return (
        so.reshape(shape), lo, sg.reshape(shape), lg,
        query_delta, value_delta, output_delta, upward_delta, downward_delta, first_delta, second_delta,
    )


def solution(mesh):
    split = ("dp", "seq")
    placed = (
        P(split, None, None), P("dp", "seq", None), P(split, None, None), P("dp", "seq", None),
        P(split), P("dp"),
        *(P(split, None) for _ in range(6)), *(P() for _ in range(9)),
    )
    return jax.shard_map(
        on_device,
        mesh=mesh,
        in_specs=placed,
        out_specs=(
            P(split, None, None), P("dp", "seq", None), P(split, None, None), P("dp", "seq", None),
            *(P() for _ in range(7)),
        ),
        check_vma=False,
    )
```

```python
import functools

import jax
import jax.numpy as jnp
from jax import lax
from jax.experimental import pallas as pl
from jax.experimental.pallas import tpu as pltpu
from jax.sharding import PartitionSpec as P

MESH = pl.DeviceIdType.MESH


def phase(name, start, stop):
    return pl.loop(start, stop)


F32 = jnp.float32
BF16 = jnp.bfloat16
EPSILON = 1e-12
MASKED = -1e30
SCALE = 0.125
PAIR = 128
BLOCK = 128
CHUNK = 256
TILE = 256
AHEAD = 3
K_UNIT, V_UNIT, Q_UNIT, O_UNIT, UP_UNIT = 0, 1, 2, 3, 4
Q_BIAS, V_BIAS, O_BIAS, D_BIAS, GAIN1, SHIFT1, GAIN2, SHIFT2, U_BIAS = 0, 1, 2, 3, 4, 5, 6, 7, 8
Q_SUM, V_SUM = 0, 1
O_SUM, D_SUM, F_SUM, S_SUM, U_SUM = 0, 1, 2, 3, 4


def dot_nn(a, b):
    return jnp.dot(a, b, preferred_element_type=F32)


def dot_nt(a, b):
    return lax.dot_general(a, b, (((1,), (1,)), ((), ())), preferred_element_type=F32)


def dot_tn(a, b):
    return lax.dot_general(a, b, (((0,), (0,)), ((), ())), preferred_element_type=F32)


def flipped(index, bit):
    return index + bit * (1 - 2 * ((index // bit) % 2))


def gelu_parts(u):
    square = u * u
    t = jnp.tanh(0.7978845608028654 * (u + 0.044715 * (u * square)))
    half = 0.5 * (1.0 + t)
    slope = half + 0.5 * u * (1.0 - t * t) * (0.7978845608028654 * (1.0 + 3 * 0.044715 * square))
    return u * half, slope


def every_fourth(pieces, j, lanes, stride):
    found = []
    for piece in pieces:
        for start in range(j * lanes, piece.shape[1], stride * lanes):
            found.append(piece[:, start : start + lanes])
    return found


def step_kernel(
    remote, dp_size, seq_size, nshort,
    *refs,
):
    given = 6 if remote else 1
    shards, refs = refs[:given], refs[given:]
    small, refs = refs[:9], refs[9:]
    (xs, xl, dys, dyl, short_len, long_len,
     so, lo, sg, lg, sums, up_sums, parked,
     par, wide_par,
     w, x, q, k, v, kv_sib, dkv_in, g, r, a16, hid, f, dy, acc, acc_in, tail, seq_in, dp_in,
     send_sem, recv_sem, misc_send, misc_recv, own_sem, small_sem, load_sem, store_sem) = refs
    dp = lax.axis_index("dp")
    seq = lax.axis_index("seq")
    y, c = seq // 2, seq % 2
    y_peer = (dp, flipped(seq, 2))
    core_peer = (dp, flipped(seq, 1))
    total, width = x.shape
    short_rows = nshort * BLOCK
    units = w.shape[0]
    depth = w.shape[1]
    hidden_chunks = (units - 4) // 2
    partners = []
    bit = 1
    while bit < seq_size:
        partners.append((dp, flipped(seq, bit)))
        bit *= 2
    bit = 1
    while bit < dp_size:
        partners.append((flipped(dp, bit), seq))
        bit *= 2

    loads = [pltpu.make_async_copy(xs, x.at[pl.ds(0, short_rows)], load_sem.at[0]),
             pltpu.make_async_copy(xl.at[y], x.at[pl.ds(short_rows + BLOCK * y, BLOCK)], load_sem.at[1])]
    late = [pltpu.make_async_copy(dys, dy.at[pl.ds(0, short_rows)], load_sem.at[2]),
            pltpu.make_async_copy(dyl.at[y], dy.at[pl.ds(short_rows + BLOCK * y, BLOCK)], load_sem.at[3])]
    for cp in loads:
        cp.start()

    if remote:
        z, ax = dp // 2, dp % 2
        x_peer = (flipped(dp, 1), seq)
        piece = w.shape[5]
        key_shard, value_shard, query_shard, output_shard, up_shard, down_shard = shards
        sources = [key_shard, value_shard, query_shard, output_shard]
        sources += [up_shard.at[:, pl.ds(n * width, width)] for n in range(hidden_chunks)]
        sources += [down_shard.at[pl.ds(n * piece, piece)] for n in range(hidden_chunks)]
        own = [pltpu.make_async_copy(source, f.at[pl.ds(n * piece, piece)], own_sem.at[n])
               for n, source in enumerate(sources)]
    else:
        own = [pltpu.make_async_copy(shards[0].at[u], w.at[u], own_sem.at[u]) for u in range(units)]
    for cp in own:
        cp.start()
    small_loads = [pltpu.make_async_copy(ref, par.at[n] if n < U_BIAS else wide_par, small_sem.at[n])
                   for n, ref in enumerate(small)]
    for cp in small_loads:
        cp.start()

    seq_peers = [(dp, (seq + n) % seq_size) for n in range(1, seq_size)]
    dp_peers = [((dp + n) % dp_size, seq) for n in range(1, dp_size)]
    peers = seq_peers + dp_peers
    barrier = pltpu.get_barrier_semaphore()
    for peer in peers:
        pl.semaphore_signal(barrier, inc=1, device_id=peer, device_id_type=MESH)

    if remote:
        lanes = width // (8 * depth)
        for cp in own:
            cp.wait()
        for u in range(4):
            w[u, z, ax, y, c] = f[u * piece : (u + 1) * piece, :].astype(BF16)
        up_rows = [f[(4 + n) * piece : (5 + n) * piece, :].astype(BF16) for n in range(hidden_chunks)]
        for j in range(hidden_chunks):
            first = (4 + hidden_chunks + j) * piece
            w[UP_UNIT + 2 * j, z, ax, y, c] = jnp.concatenate(every_fourth(up_rows, j, lanes, hidden_chunks), axis=1)
            w[UP_UNIT + 2 * j + 1, z, ax, y, c] = f[first : first + piece, :].astype(BF16)
    pl.semaphore_wait(barrier, len(peers))

    def misc(slot, src, dst, peer):
        return pltpu.make_async_remote_copy(
            src_ref=src, dst_ref=dst, send_sem=misc_send.at[slot], recv_sem=misc_recv.at[slot],
            device_id=peer, device_id_type=MESH)

    swap_x = misc(0, xl.at[1 - y], x.at[pl.ds(short_rows + BLOCK * y, BLOCK)], y_peer)
    swap_dy = misc(1, dyl.at[1 - y], dy.at[pl.ds(short_rows + BLOCK * y, BLOCK)], y_peer)
    swap_x.start()

    sends, inner_sends = {}, []
    if remote:
        half = depth // 2
        lower, upper, every, both = pl.ds(0, half), pl.ds(half, half), pl.ds(0, depth), pl.ds(0, 2)
        pair, far_pair = pl.ds(z // 2 * 2, 2), pl.ds(2 - z // 2 * 2, 2)
        top, bottom = pl.ds(0, piece // 2), pl.ds(piece // 2, piece // 2)
        is_inner = (z + 1) // 2 == 1
        z_next = (flipped(z, 1) * 2 + ax, seq)
        z_across = ((depth - 1 - z) * 2 + ax, seq)
        stages = 6

        def plan(u, slot, part, peer):
            cp = pltpu.make_async_remote_copy(
                src_ref=w.at[(u, *part)], dst_ref=w.at[(u, *part)],
                send_sem=send_sem.at[u, slot], recv_sem=recv_sem.at[u, slot], device_id=peer, device_id_type=MESH)
            sends[u, slot] = cp
            return cp

        def pass_on(u, slot, part, peer):
            plan(u, slot, part, peer).start()

        def from_inner(u, parts):
            copies = [plan(u, slot, part, peer) for slot, part, peer in parts]
            for cp, (slot, _, _) in zip(copies, parts):
                inner_sends.append((u, slot))

            @pl.when(is_inner)
            def _():
                for cp in copies:
                    cp.start()

        def wait_where(here, u, slots):
            @pl.when(here)
            def _():
                for slot in slots:
                    sends[u, slot].wait_recv()

        def wait_for(u, slots):
            for slot in slots:
                sends[u, slot].wait_recv()

        def z_first(u, stage):
            if stage == 0:
                pass_on(u, 0, (z, ax, y, c), z_next)
            elif stage == 1:
                wait_for(u, (0,))
                from_inner(u, [(1, (pair, ax, y, c), z_across)])
            elif stage == 2:
                wait_where(is_inner, u, (1,))
                from_inner(u, [(2, (far_pair, ax, y, c), z_next)])
            elif stage == 3:
                wait_where(jnp.logical_not(is_inner), u, (2,))
                pass_on(u, 3, (lower, ax, y, c), x_peer)
                pass_on(u, 4, (upper, ax, y, c), y_peer)
                pass_on(u, 7, (every, ax, y, c), core_peer)
            elif stage == 4:
                wait_for(u, (3, 4))
                pass_on(u, 5, (lower, both, y, c), y_peer)
                pass_on(u, 6, (upper, ax, both, c), x_peer)
                pass_on(u, 8, (lower, 1 - ax, y, c), core_peer)
                pass_on(u, 9, (upper, ax, 1 - y, c), core_peer)
            elif stage == 5:
                wait_for(u, (5, 6))
                pass_on(u, 10, (lower, both, 1 - y, c), core_peer)
                pass_on(u, 11, (upper, 1 - ax, both, c), core_peer)
            else:
                wait_for(u, range(7, 12))

        def z_second(u, stage):
            if stage == 0:
                pass_on(u, 0, (z, ax, y, c, top), x_peer)
                pass_on(u, 1, (z, ax, y, c, bottom), y_peer)
            elif stage == 1:
                wait_for(u, (0, 1))
                pass_on(u, 2, (z, both, y, c, top), z_next)
                pass_on(u, 3, (z, ax, both, c, bottom), z_next)
            elif stage == 2:
                wait_for(u, (2, 3))
                from_inner(u, [(4, (pair, both, y, c, top), z_across), (5, (pair, ax, both, c, bottom), z_across)])
            elif stage == 3:
                wait_where(is_inner, u, (4, 5))
                from_inner(u, [(6, (far_pair, both, y, c, top), z_next), (7, (far_pair, ax, both, c, bottom), z_next)])
            elif stage == 4:
                wait_where(jnp.logical_not(is_inner), u, (6, 7))
                pass_on(u, 8, (every, both, y, c, top), y_peer)
                pass_on(u, 9, (every, ax, both, c, bottom), x_peer)
                pass_on(u, 10, (every, both, y, c, top), core_peer)
                pass_on(u, 11, (every, ax, both, c, bottom), core_peer)
            elif stage == 5:
                wait_for(u, (8, 9))
                pass_on(u, 12, (every, both, 1 - y, c, top), core_peer)
                pass_on(u, 13, (every, 1 - ax, both, c, bottom), core_peer)
            else:
                wait_for(u, range(10, 14))

        events = [(i + stages - stage, stage) for i in range(-stages, units) for stage in range(stages + 1)]
        events = [(u, stage) for u, stage in events if 0 <= u < units]

        def advance(count):
            for u, stage in events[:count]:
                (z_first if u % 3 == 0 else z_second)(u, stage)
                if (u, stage) == (units - 1, stages - 1):
                    swap_dy.start()
            del events[:count]

        def arrive(i):
            if (i, stages) in events:
                advance(events.index((i, stages)) + 1)
    else:
        def advance(count):
            pass

        def arrive(i):
            if i == units - 2:
                swap_dy.start()
            own[i].wait()

    def columns(u, at):
        return w[u, :, :, :, :, :, at].reshape(width, CHUNK)

    def row_block(u, i):
        return w[u, i].reshape(CHUNK, width)

    def chunk(i):
        return pl.ds(pl.multiple_of(i * CHUNK, CHUNK), CHUNK)

    def tile(i):
        return pl.ds(pl.multiple_of(i * TILE, TILE), TILE)

    def project(u, dst, bias, scale):
        @phase("proj", 0, width // CHUNK)
        def _(i):
            at = chunk(i)
            value = dot_nn(x[...], columns(u, at))
            if bias is not None:
                value = value + par[bias, :, at]
            if scale is not None:
                value = value * scale
            dst[:, at] = value.astype(BF16)

    lane = lax.broadcasted_iota(jnp.int32, (BLOCK, PAIR), 1)
    low_half = lane < PAIR // 2
    row_lane = lax.broadcasted_iota(jnp.int32, (1, PAIR), 1)
    first_head = jnp.where(row_lane < PAIR // 2, 1.0, 0.0).astype(BF16)
    second_head = jnp.where(row_lane < PAIR // 2, 0.0, 1.0).astype(BF16)

    def heads(value):
        return jnp.concatenate([value * first_head, value * second_head], axis=0)

    def merged(value):
        return jnp.where(low_half, value[:BLOCK], value[BLOCK:])

    def softmax(scores, usable):
        scores = jnp.where(usable, scores, MASKED)
        weight = jnp.exp(scores - jnp.max(scores, axis=0, keepdims=True))
        return weight * (1.0 / jnp.sum(weight, axis=0, keepdims=True))

    pairs = width // PAIR
    per_row = width // (2 * BLOCK)
    own_rows = pl.ds(short_rows, 2 * BLOCK)

    def pair_at(h):
        return slice(h * PAIR, (h + 1) * PAIR)

    def short_kept(s, h):
        start = (s % 4) * (pairs // per_row) + h // per_row
        col = h % per_row * 2 * BLOCK
        return s // 4, pl.ds(pl.multiple_of(start * BLOCK, BLOCK), BLOCK), slice(col, col + 2 * BLOCK)

    def long_kept(n, h):
        rows = pl.ds(pl.multiple_of(h // per_row * 4 * BLOCK, 4 * BLOCK), 4 * BLOCK)
        return 2 + n, rows, pl.ds(pl.multiple_of(h % per_row * 2 * BLOCK, 2 * BLOCK), 2 * BLOCK)

    def short_forward(s):
        rows = pl.ds(pl.multiple_of(s * BLOCK, BLOCK), BLOCK)
        usable = lax.broadcasted_iota(jnp.int32, (BLOCK, 2 * BLOCK), 0) < short_len[s]
        for h in range(pairs):
            at = pair_at(h)
            p = softmax(dot_nt(k[rows, at], heads(q[rows, at])), usable).astype(BF16)
            hid[short_kept(s, h)] = p
            g[rows, at] = merged(dot_tn(p, v[rows, at])).astype(BF16)

    def long_usable():
        key = lax.broadcasted_iota(jnp.int32, (4 * BLOCK, 2 * BLOCK), 0)
        block = key // BLOCK
        mine = key + (block + c) * BLOCK
        other = key + (block - 3 - c) * BLOCK
        return jnp.where(block < 2, mine, other) < long_len[y]

    def long_pair(h):
        return pl.ds(pl.multiple_of(h * PAIR, PAIR), PAIR)

    def long_forward(h):
        at = long_pair(h)
        usable = long_usable()
        for n in range(2):
            rows = pl.ds(short_rows + n * BLOCK, BLOCK)
            qm = heads(q[rows, at])
            scores = jnp.concatenate([dot_nt(k[own_rows, at], qm), dot_nt(kv_sib[0, :, at], qm)], axis=0)
            p = softmax(scores, usable).astype(BF16)
            hid[long_kept(n, h)] = p
            o2 = dot_tn(p[: 2 * BLOCK], v[own_rows, at]) + dot_tn(p[2 * BLOCK :], kv_sib[1, :, at])
            g[rows, at] = merged(o2).astype(BF16)

    def norm_parts(value):
        center = value - jnp.mean(value, axis=1, keepdims=True)
        scale = lax.rsqrt(jnp.mean(center * center, axis=1, keepdims=True) + EPSILON)
        return center * scale, scale

    def norm_back(grad, gain, normed, scale):
        grad = grad * gain
        return scale * (
            grad - jnp.mean(grad, axis=1, keepdims=True) - normed * jnp.mean(grad * normed, axis=1, keepdims=True))

    def row_sum(value):
        return jnp.sum(value, axis=0, keepdims=True)

    def add_sum(row, at, value):
        acc[0, row : row + 1, at] += row_sum(value)

    acc[0] = jnp.zeros_like(acc[0])
    tail[...] = jnp.zeros_like(tail)
    for cp in small_loads:
        cp.wait()
    for j in range(hidden_chunks):
        if remote:
            par[U_BIAS + j] = jnp.concatenate(every_fourth([wide_par[...]], j, lanes, hidden_chunks), axis=1)
        else:
            par[U_BIAS + j] = wide_par[:, j * width : (j + 1) * width]
    for cp in loads:
        cp.wait()
    arrive(K_UNIT)
    swap_x.wait_recv()
    project(K_UNIT, k, None, None)
    arrive(V_UNIT)
    project(V_UNIT, v, V_BIAS, None)
    swap_k = misc(2, k.at[own_rows], kv_sib.at[0], core_peer)
    swap_v = misc(3, v.at[own_rows], kv_sib.at[1], core_peer)
    arrive(Q_UNIT)
    swap_k.start()
    swap_v.start()
    project(Q_UNIT, q, Q_BIAS, SCALE)

    for n in range(3):

        @phase("sf", n * nshort // 3, (n + 1) * nshort // 3)
        def _(s):
            short_forward(s)

        if n < 2:
            advance(AHEAD)
        else:
            arrive(O_UNIT)

    swap_k.wait_recv()
    swap_v.wait_recv()
    for n in range(4):

        @phase("lf", n * pairs // 4, (n + 1) * pairs // 4)
        def _(h):
            long_forward(h)

        if n < 3:
            advance(AHEAD)

    swap_k.wait_send()
    swap_v.wait_send()
    park = pltpu.make_async_copy(hid, parked, store_sem.at[4])
    park.start()
    arrive(UP_UNIT)

    @phase("wo", 0, width // CHUNK)
    def _(i):
        at = chunk(i)
        r[:, at] = x[:, at].astype(F32) + dot_nn(g[...], columns(O_UNIT, at)) + par[O_BIAS, :, at]

    advance(AHEAD)

    @phase("ln1", 0, total // TILE)
    def _(i):
        rows = tile(i)
        normed, _ = norm_parts(r[rows, :])
        value = normed * par[GAIN1] + par[SHIFT1]
        a16[rows, :] = value.astype(BF16)
        f[rows, :] = value + par[D_BIAS]

    park.wait()
    for j in range(hidden_chunks):
        up, down = UP_UNIT + 2 * j, UP_UNIT + 2 * j + 1
        if j > 0:
            arrive(up)
        else:
            advance(AHEAD)
        for n in range(2):

            @phase("up", 2 * n, 2 * n + 2)
            def _(i):
                at = chunk(i)
                value = dot_nn(a16[...], columns(up, at)) + par[U_BIAS + j, :, at]
                active, slope = gelu_parts(value)
                hid[j, :, at] = slope.astype(BF16)
                g[:, at] = active.astype(BF16)

            if n == 0:
                advance(AHEAD)

        if j == hidden_chunks - 2:
            for cp in late:
                cp.start()
        arrive(down)

        @phase("down", 0, width // CHUNK)
        def _(i):
            at = chunk(i)
            f[:, at] += dot_nn(g[...], columns(down, at))

    for cp in late:
        cp.wait()
    swap_dy.wait_recv()

    @phase("ln2", 0, total // TILE)
    def _(i):
        rows = tile(i)
        normed, scale = norm_parts(f[rows, :])
        upstream = dy[rows, :].astype(F32)
        dy[rows, :] = (normed * par[GAIN2] + par[SHIFT2]).astype(BF16)
        grad = norm_back(upstream, par[GAIN2], normed, scale)
        f[rows, :] = grad
        a16[rows, :] = grad.astype(BF16)
        add_sum(S_SUM, slice(None), upstream)
        add_sum(D_SUM, slice(None), grad)

    out_copies = [
        pltpu.make_async_copy(dy.at[pl.ds(0, short_rows)], so, store_sem.at[0]),
        pltpu.make_async_copy(dy.at[pl.ds(short_rows + BLOCK * y, BLOCK)], lo.at[y], store_sem.at[1]),
    ]
    for cp in out_copies:
        cp.start()
    swap_out = misc(4, dy.at[pl.ds(short_rows + BLOCK * (1 - y), BLOCK)], lo.at[y], y_peer)
    swap_out.start()

    @phase("dg", 0, hidden_chunks * (width // CHUNK))
    def _(n):
        j = n // (width // CHUNK)
        i = n % (width // CHUNK)
        at = chunk(i)
        value = dot_nt(a16[...], row_block(UP_UNIT + 1 + 2 * j, i)) * hid[j, :, at].astype(F32)
        hid[j, :, at] = value.astype(BF16)
        acc[0, pl.ds(U_SUM + j, 1), at] += row_sum(value)

    @phase("da", 0, width // CHUNK)
    def _(i):
        at = chunk(i)
        value = f[:, at]
        for j in range(hidden_chunks):
            value = value + dot_nt(hid[j], row_block(UP_UNIT + 2 * j, i))
        f[:, at] = value

    unpark = pltpu.make_async_copy(parked, hid, store_sem.at[5])
    unpark.start()

    @phase("ln1b", 0, total // TILE)
    def _(i):
        rows = tile(i)
        normed, scale = norm_parts(r[rows, :])
        upstream = f[rows, :]
        grad = norm_back(upstream, par[GAIN1], normed, scale)
        r[rows, :] = grad
        a16[rows, :] = grad.astype(BF16)
        add_sum(F_SUM, slice(None), upstream)
        add_sum(O_SUM, slice(None), grad)

    def early(n):
        return misc(8 + n, acc.at[n], acc_in.at[n], partners[n])

    def finish_early(n):
        early(n).wait_recv()
        early(n).wait_send()
        acc[n + 1] = acc[n] + acc_in[n]

    def next_early(n):
        if n > 0:
            finish_early(n - 1)
        early(n).start()

    next_early(0)

    @phase("do", 0, width // CHUNK)
    def _(i):
        at = chunk(i)
        g[:, at] = dot_nt(a16[...], row_block(O_UNIT, i)).astype(BF16)

    next_early(1)
    unpark.wait()

    @phase("lb", 0, pairs)
    def _(h):
        at = long_pair(h)
        keys, values = k[own_rows, at], v[own_rows, at]
        keys_far, values_far = kv_sib[0, :, at], kv_sib[1, :, at]
        key_grad = value_grad = query_sum = 0.0
        for n in range(2):
            rows = pl.ds(short_rows + n * BLOCK, BLOCK)
            qm = heads(q[rows, at])
            om = heads(g[rows, at])
            low = hid[long_kept(n, h)]
            p = low.astype(F32)
            back = jnp.concatenate([dot_nt(values, om), dot_nt(values_far, om)], axis=0)
            ds = (p * (back - jnp.sum(back * p, axis=0, keepdims=True))).astype(BF16)
            dq = merged(dot_tn(ds[: 2 * BLOCK], keys) + dot_tn(ds[2 * BLOCK :], keys_far)) * SCALE
            q[rows, at] = dq.astype(BF16)
            query_sum = query_sum + row_sum(dq)
            key_grad = key_grad + dot_nn(ds, qm)
            value_grad = value_grad + dot_nn(low, om)
        k[own_rows, at] = key_grad[: 2 * BLOCK].astype(BF16)
        v[own_rows, at] = value_grad[: 2 * BLOCK].astype(BF16)
        kv_sib[0, :, at] = key_grad[2 * BLOCK :].astype(BF16)
        kv_sib[1, :, at] = value_grad[2 * BLOCK :].astype(BF16)
        tail[Q_SUM : Q_SUM + 1, at] += query_sum
        tail[V_SUM : V_SUM + 1, at] += row_sum(value_grad)

    def short_backward(s):
        rows = pl.ds(pl.multiple_of(s * BLOCK, BLOCK), BLOCK)
        for h in range(pairs):
            at = pair_at(h)
            qm = heads(q[rows, at])
            om = heads(g[rows, at])
            keys = k[rows, at]
            low = hid[short_kept(s, h)]
            p = low.astype(F32)
            back = dot_nt(v[rows, at], om)
            ds = (p * (back - jnp.sum(back * p, axis=0, keepdims=True))).astype(BF16)
            dq = merged(dot_tn(ds, keys)) * SCALE
            dk = dot_nn(ds, qm)
            dv = dot_nn(low, om)
            q[rows, at] = dq.astype(BF16)
            k[rows, at] = dk.astype(BF16)
            v[rows, at] = dv.astype(BF16)
            tail[Q_SUM : Q_SUM + 1, at] += row_sum(dq)
            tail[V_SUM : V_SUM + 1, at] += row_sum(dv)

    next_early(2)

    @phase("sb1", 0, 1)
    def _(s):
        short_backward(s)

    swap_dkv = misc(5, kv_sib, dkv_in, core_peer)
    swap_dkv.start()
    next_early(3)

    @phase("sb2", 1, nshort)
    def _(s):
        short_backward(s)

    steps = len(partners)

    def exchange(slots, me, others, base):
        return [misc(base + n, slots.at[me], slots.at[me], peer) for n, peer in enumerate(others)]

    seq_round = exchange(seq_in, seq, seq_peers, 8 + steps)
    dp_round = exchange(dp_in, dp, dp_peers, 8 + steps + len(seq_peers))
    seq_in[seq] = tail[...]

    for n in range(4, steps):
        next_early(n)
    swap_dkv.wait_recv()
    for cp in seq_round:
        cp.start()
    k[own_rows, :] = (k[own_rows, :].astype(F32) + dkv_in[0].astype(F32)).astype(BF16)
    v[own_rows, :] = (v[own_rows, :].astype(F32) + dkv_in[1].astype(F32)).astype(BF16)

    def input_grad(rows, i):
        at = chunk(i)
        value = r[rows, at]
        for ref, u in ((q, Q_UNIT), (k, K_UNIT), (v, V_UNIT)):
            value = value + dot_nt(ref[rows, :], row_block(u, i))
        x[rows, at] = value.astype(BF16)

    @phase("gxl", 0, width // CHUNK)
    def _(i):
        input_grad(own_rows, i)

    swap_grad = misc(6, x.at[pl.ds(short_rows + BLOCK * (1 - y), BLOCK)], lg.at[y], y_peer)
    swap_grad.start()
    finish_early(steps - 1)
    for cp in seq_round:
        cp.wait_recv()
    dp_in[dp] = sum(seq_in[n] for n in range(1, seq_size)) + seq_in[0]
    for i in range(width // CHUNK):

        @phase("gxs", i, i + 1)
        def _(n):
            input_grad(pl.ds(0, short_rows), n)

        if i == 0:
            for cp in dp_round:
                cp.start()
    for cp in dp_round:
        cp.wait_recv()
    for cp in seq_round + dp_round:
        cp.wait_send()
    sums[0:2, :] = sum(dp_in[n] for n in range(1, dp_size)) + dp_in[0]
    sums[2:6, :] = acc[steps, 0:4, :]
    hidden_sums = [acc[steps, U_SUM + j : U_SUM + j + 1, :] for j in range(hidden_chunks)]
    if remote:
        order = [hidden_sums[j][:, n * lanes : (n + 1) * lanes]
                 for n in range(width // lanes) for j in range(hidden_chunks)]
        up_sums[...] = jnp.concatenate(order, axis=1)
    else:
        up_sums[...] = jnp.concatenate(hidden_sums, axis=1)

    grad_copies = [
        pltpu.make_async_copy(x.at[pl.ds(0, short_rows)], sg, store_sem.at[2]),
        pltpu.make_async_copy(x.at[pl.ds(short_rows + BLOCK * y, BLOCK)], lg.at[y], store_sem.at[3]),
    ]
    for cp in grad_copies:
        cp.start()
    swap_out.wait_recv()
    swap_grad.wait_recv()
    for cp in out_copies + grad_copies:
        cp.wait()
    for cp in (swap_x, swap_dy, swap_out, swap_dkv, swap_grad):
        cp.wait_send()
    for key in sends:
        if key not in inner_sends:
            sends[key].wait_send()
    if inner_sends:
        @pl.when(is_inner)
        def _():
            for key in inner_sends:
                sends[key].wait_send()


def whole_step(shards, small, xs, xl, dys, dyl, short_len, long_len, remote):
    dp_size, seq_size = lax.axis_size("dp"), lax.axis_size("seq")
    width = xs.shape[1]
    nshort = xs.shape[0] // BLOCK
    total = xs.shape[0] + xl.shape[0] * BLOCK
    hidden_chunks = small[-1].shape[1] // width
    units = 4 + 2 * hidden_chunks
    lead = (width // CHUNK, 2, 2, 2, CHUNK // 8, width)
    slots = 14
    steps = (dp_size * seq_size).bit_length() - 1
    exchanges = 8 + steps + seq_size + dp_size
    anywhere = pl.BlockSpec(memory_space=pl.ANY)
    smem = pl.BlockSpec(memory_space=pltpu.SMEM)
    vmem = pl.BlockSpec(memory_space=pltpu.VMEM)
    act = pltpu.VMEM((total, width), BF16)
    wide = pltpu.VMEM((total, width), F32)
    side = pltpu.VMEM((2, 2 * BLOCK, width), BF16)
    dma = pltpu.SemaphoreType.DMA
    return pl.pallas_call(
        functools.partial(step_kernel, remote, dp_size, seq_size, nshort),
        out_shape=(
            jax.ShapeDtypeStruct(xs.shape, BF16),
            jax.ShapeDtypeStruct(xl.shape, BF16),
            jax.ShapeDtypeStruct(xs.shape, BF16),
            jax.ShapeDtypeStruct(xl.shape, BF16),
            jax.ShapeDtypeStruct((8, width), F32),
            jax.ShapeDtypeStruct((1, hidden_chunks * width), F32),
            jax.ShapeDtypeStruct((hidden_chunks, total, width), BF16),
        ),
        in_specs=[anywhere] * (len(shards) + len(small) + 4) + [smem] * 2,
        out_specs=(anywhere,) * 4 + (vmem,) * 2 + (anywhere,),
        scratch_shapes=[
            pltpu.VMEM((U_BIAS + hidden_chunks, 1, width), F32),
            pltpu.VMEM((1, hidden_chunks * width), F32),
            pltpu.VMEM((units, *lead), BF16),
            act, act, act, act, side, side, act, wide, act,
            pltpu.VMEM((hidden_chunks, total, width), BF16),
            wide, act,
            pltpu.VMEM((steps + 1, 4 + hidden_chunks, width), F32),
            pltpu.VMEM((steps, 4 + hidden_chunks, width), F32),
            pltpu.VMEM((2, width), F32),
            pltpu.VMEM((seq_size, 2, width), F32),
            pltpu.VMEM((dp_size, 2, width), F32),
            dma((units, slots)), dma((units, slots)), dma((exchanges,)), dma((exchanges,)),
            dma((units,)), dma((len(small),)), dma((4,)), dma((6,)),
        ],
        compiler_params=pltpu.CompilerParams(
            collective_id=0, has_side_effects=True, vmem_limit_bytes=67043328),
        name="whole_step",
    )(*shards, *small, xs, xl, dys, dyl, short_len, long_len)


def deliver_kernel(so, lo, sg, lg, sums, up_sums, *refs):
    outs, deltas = refs[:4], refs[4:11]
    stages, rows, in_sem, out_sem, row_sem = refs[11:15], refs[15], refs[16], refs[17], refs[18]
    ins = [pltpu.make_async_copy(ref, stage, in_sem.at[n]) for n, (ref, stage) in enumerate(zip((so, lo, sg, lg), stages))]
    gather = pltpu.make_async_copy(sums, rows, row_sem.at[0])
    for cp in ins:
        cp.start()
    gather.start()
    outs = [pltpu.make_async_copy(stage, out, out_sem.at[n]) for n, (stage, out) in enumerate(zip(stages, outs))]
    gather.wait()
    for n in range(6):
        deltas[n][...] = rows[n : n + 1, :]
    deltas[6][...] = up_sums[...]
    for n in range(4):
        ins[n].wait()
        outs[n].start()
    for n in range(4):
        outs[n].wait()


def deliver(so, lo, sg, lg, sums, up_sums):
    anywhere = pl.BlockSpec(memory_space=pl.ANY)
    vmem = pl.BlockSpec(memory_space=pltpu.VMEM)
    width = sums.shape[1]
    big = (so, lo, sg, lg)
    row = jax.ShapeDtypeStruct((1, width), F32)
    dma = pltpu.SemaphoreType.DMA
    return pl.pallas_call(
        deliver_kernel,
        out_shape=tuple(jax.ShapeDtypeStruct(a.shape, a.dtype) for a in big)
        + (row,) * 6 + (jax.ShapeDtypeStruct(up_sums.shape, F32),),
        in_specs=[anywhere] * 5 + [vmem],
        out_specs=(anywhere,) * 4 + (vmem,) * 7,
        scratch_shapes=[pltpu.VMEM(a.shape, a.dtype) for a in big]
        + [pltpu.VMEM(sums.shape, F32), dma((4,)), dma((4,)), dma((1,))],
        name="deliver",
    )(so, lo, sg, lg, sums, up_sums)


def on_device(
    short_input, long_input, short_cotangent, long_cotangent, short_lengths, long_lengths,
    query_weight, key_weight, value_weight, output_weight, upward_weight, downward_weight,
    query_bias, value_bias, output_bias, upward_bias, downward_bias,
    first_gain, first_shift, second_gain, second_shift,
):
    rows, width = query_weight.shape
    devices = lax.axis_size("dp") * lax.axis_size("seq")
    hidden_chunks = upward_weight.shape[1] // width
    shape = short_input.shape

    def permuted(value):
        lead = value.shape[:-1]
        value = value.reshape(*lead, devices, hidden_chunks, rows)
        return jnp.moveaxis(value, -2, 0).reshape(hidden_chunks, *lead, width)

    remote = rows == 32 and lax.axis_size("seq") == 4
    small = [query_bias, value_bias, output_bias, downward_bias, first_gain, first_shift, second_gain, second_shift]
    if remote:
        shards = [key_weight, value_weight, query_weight, output_weight, upward_weight, downward_weight]
        small.append(upward_bias)
    else:
        upward = permuted(upward_weight)
        downward = downward_weight.reshape(hidden_chunks, rows, width)
        parts = [key_weight, value_weight, query_weight, output_weight]
        for j in range(hidden_chunks):
            parts += [upward[j], downward[j]]
        whole = lax.all_gather(jnp.stack([part.astype(BF16) for part in parts]), ("dp", "seq"), axis=1, tiled=True)
        shards = [whole.reshape(len(parts), width // CHUNK, 2, 2, 2, CHUNK // 8, width)]
        small.append(permuted(upward_bias))
    so, lo, sg, lg, sums, up_sums, _ = whole_step(
        shards, [value.reshape(1, -1) for value in small],
        short_input.reshape(-1, width), long_input, short_cotangent.reshape(-1, width), long_cotangent,
        short_lengths, long_lengths, remote)
    so, lo, sg, lg, *deltas = deliver(so, lo, sg, lg, sums, up_sums)
    up_sums = deltas[6]
    if remote:
        upward_delta = up_sums.reshape(-1)
    else:
        upward_delta = jnp.moveaxis(up_sums.reshape(hidden_chunks, devices, rows), 0, 1).reshape(-1)
    query_delta, value_delta, output_delta, downward_delta, first_delta, second_delta = (value.reshape(-1) for value in deltas[:6])
    return (
        so.reshape(shape), lo, sg.reshape(shape), lg,
        query_delta, value_delta, output_delta, upward_delta, downward_delta, first_delta, second_delta,
    )


def solution(mesh):
    split = ("dp", "seq")
    placed = (
        P(split, None, None), P("dp", "seq", None), P(split, None, None), P("dp", "seq", None),
        P(split), P("dp"),
        *(P(split, None) for _ in range(6)), *(P() for _ in range(9)),
    )
    return jax.shard_map(
        on_device,
        mesh=mesh,
        in_specs=placed,
        out_specs=(
            P(split, None, None), P("dp", "seq", None), P(split, None, None), P("dp", "seq", None),
            *(P() for _ in range(7)),
        ),
        check_vma=False,
    )
```

```python
import functools

import jax
import jax.numpy as jnp
from jax import lax
from jax.experimental import pallas as pl
from jax.experimental.pallas import tpu as pltpu
from jax.sharding import PartitionSpec as P

MESH = pl.DeviceIdType.MESH


def phase(name, start, stop):
    return pl.loop(start, stop)


F32 = jnp.float32
BF16 = jnp.bfloat16
EPSILON = 1e-12
MASKED = -1e30
SCALE = 0.125
PAIR = 128
BLOCK = 128
CHUNK = 256
TILE = 256
AHEAD = 3
Z_FIRST_EVERY = 4
LEAN_UNIT = -1
K_UNIT, V_UNIT, Q_UNIT, O_UNIT, UP_UNIT = 0, 1, 2, 3, 4
Q_BIAS, V_BIAS, O_BIAS, D_BIAS, GAIN1, SHIFT1, GAIN2, SHIFT2, U_BIAS = 0, 1, 2, 3, 4, 5, 6, 7, 8
Q_SUM, V_SUM = 0, 1
O_SUM, D_SUM, F_SUM, S_SUM, U_SUM = 0, 1, 2, 3, 4


def dot_nn(a, b):
    return jnp.dot(a, b, preferred_element_type=F32)


def dot_nt(a, b):
    return lax.dot_general(a, b, (((1,), (1,)), ((), ())), preferred_element_type=F32)


def dot_tn(a, b):
    return lax.dot_general(a, b, (((0,), (0,)), ((), ())), preferred_element_type=F32)


def flipped(index, bit):
    return index + bit * (1 - 2 * ((index // bit) % 2))


def gelu_parts(u):
    square = u * u
    t = jnp.tanh(0.7978845608028654 * (u + 0.044715 * (u * square)))
    half = 0.5 * (1.0 + t)
    slope = half + 0.5 * u * (1.0 - t * t) * (0.7978845608028654 * (1.0 + 3 * 0.044715 * square))
    return u * half, slope


def every_fourth(pieces, j, lanes, stride):
    found = []
    for piece in pieces:
        for start in range(j * lanes, piece.shape[1], stride * lanes):
            found.append(piece[:, start : start + lanes])
    return found


def step_kernel(
    remote, dp_size, seq_size, nshort,
    *refs,
):
    given = 6 if remote else 1
    shards, refs = refs[:given], refs[given:]
    small, refs = refs[:9], refs[9:]
    (xs, xl, dys, dyl, short_len, long_len,
     so, lo, sg, lg, sums, up_sums, parked,
     par, wide_par,
     w, x, q, k, v, kv_sib, dkv_in, g, r, a16, hid, f, dy, acc, acc_in, tail, seq_in, dp_in,
     send_sem, recv_sem, misc_send, misc_recv, own_sem, small_sem, load_sem, store_sem) = refs
    dp = lax.axis_index("dp")
    seq = lax.axis_index("seq")
    y, c = seq // 2, seq % 2
    y_peer = (dp, flipped(seq, 2))
    core_peer = (dp, flipped(seq, 1))
    total, width = x.shape
    short_rows = nshort * BLOCK
    units = w.shape[0]
    depth = w.shape[1]
    hidden_chunks = (units - 4) // 2
    partners = []
    bit = 1
    while bit < seq_size:
        partners.append((dp, flipped(seq, bit)))
        bit *= 2
    bit = 1
    while bit < dp_size:
        partners.append((flipped(dp, bit), seq))
        bit *= 2

    loads = [pltpu.make_async_copy(xs, x.at[pl.ds(0, short_rows)], load_sem.at[0]),
             pltpu.make_async_copy(xl.at[y], x.at[pl.ds(short_rows + BLOCK * y, BLOCK)], load_sem.at[1])]
    late = [pltpu.make_async_copy(dys, dy.at[pl.ds(0, short_rows)], load_sem.at[2]),
            pltpu.make_async_copy(dyl.at[y], dy.at[pl.ds(short_rows + BLOCK * y, BLOCK)], load_sem.at[3])]
    for cp in loads:
        cp.start()

    if remote:
        z, ax = dp // 2, dp % 2
        x_peer = (flipped(dp, 1), seq)
        piece = w.shape[5]
        key_shard, value_shard, query_shard, output_shard, up_shard, down_shard = shards
        sources = [key_shard, value_shard, query_shard, output_shard]
        sources += [up_shard.at[:, pl.ds(n * width, width)] for n in range(hidden_chunks)]
        sources += [down_shard.at[pl.ds(n * piece, piece)] for n in range(hidden_chunks)]
        own = [pltpu.make_async_copy(source, f.at[pl.ds(n * piece, piece)], own_sem.at[n])
               for n, source in enumerate(sources)]
    else:
        own = [pltpu.make_async_copy(shards[0].at[u], w.at[u], own_sem.at[u]) for u in range(units)]
    for cp in own:
        cp.start()
    small_loads = [pltpu.make_async_copy(ref, par.at[n] if n < U_BIAS else wide_par, small_sem.at[n])
                   for n, ref in enumerate(small)]
    for cp in small_loads:
        cp.start()

    seq_peers = [(dp, (seq + n) % seq_size) for n in range(1, seq_size)]
    dp_peers = [((dp + n) % dp_size, seq) for n in range(1, dp_size)]
    peers = seq_peers + dp_peers
    barrier = pltpu.get_barrier_semaphore()
    for peer in peers:
        pl.semaphore_signal(barrier, inc=1, device_id=peer, device_id_type=MESH)

    if remote:
        lanes = width // (8 * depth)

        def cast(u, source):
            own[source].wait()
            w[u, z, ax, y, c] = f[source * piece : (source + 1) * piece, :].astype(BF16)

        cast(0, 0)
        cast(1, 1)
    pl.semaphore_wait(barrier, len(peers))

    def misc(slot, src, dst, peer):
        return pltpu.make_async_remote_copy(
            src_ref=src, dst_ref=dst, send_sem=misc_send.at[slot], recv_sem=misc_recv.at[slot],
            device_id=peer, device_id_type=MESH)

    swap_x = misc(0, xl.at[1 - y], x.at[pl.ds(short_rows + BLOCK * y, BLOCK)], y_peer)
    swap_dy = misc(1, dyl.at[1 - y], dy.at[pl.ds(short_rows + BLOCK * y, BLOCK)], y_peer)
    swap_x.start()

    sends, inner_sends = {}, []
    if remote:
        half = depth // 2
        lower, upper, every, both = pl.ds(0, half), pl.ds(half, half), pl.ds(0, depth), pl.ds(0, 2)
        pair, far_pair = pl.ds(z // 2 * 2, 2), pl.ds(2 - z // 2 * 2, 2)
        top, bottom = pl.ds(0, piece // 2), pl.ds(piece // 2, piece // 2)
        is_inner = (z + 1) // 2 == 1
        z_next = (flipped(z, 1) * 2 + ax, seq)
        z_across = ((depth - 1 - z) * 2 + ax, seq)
        stages = 6

        def plan(u, slot, part, peer):
            cp = pltpu.make_async_remote_copy(
                src_ref=w.at[(u, *part)], dst_ref=w.at[(u, *part)],
                send_sem=send_sem.at[u, slot], recv_sem=recv_sem.at[u, slot], device_id=peer, device_id_type=MESH)
            sends[u, slot] = cp
            return cp

        def pass_on(u, slot, part, peer):
            plan(u, slot, part, peer).start()

        def from_inner(u, parts):
            copies = [plan(u, slot, part, peer) for slot, part, peer in parts]
            for cp, (slot, _, _) in zip(copies, parts):
                inner_sends.append((u, slot))

            @pl.when(is_inner)
            def _():
                for cp in copies:
                    cp.start()

        def wait_where(here, u, slots):
            @pl.when(here)
            def _():
                for slot in slots:
                    sends[u, slot].wait_recv()

        def wait_for(u, slots):
            for slot in slots:
                sends[u, slot].wait_recv()

        def z_first(u, stage):
            if stage == 0:
                pass_on(u, 0, (z, ax, y, c), z_next)
            elif stage == 1:
                wait_for(u, (0,))
                from_inner(u, [(1, (pair, ax, y, c), z_across)])
            elif stage == 2:
                wait_where(is_inner, u, (1,))
                from_inner(u, [(2, (far_pair, ax, y, c), z_next)])
            elif stage == 3:
                wait_where(jnp.logical_not(is_inner), u, (2,))
                pass_on(u, 3, (lower, ax, y, c), x_peer)
                pass_on(u, 4, (upper, ax, y, c), y_peer)
                pass_on(u, 7, (every, ax, y, c), core_peer)
            elif stage == 4:
                wait_for(u, (3, 4))
                pass_on(u, 5, (lower, both, y, c), y_peer)
                pass_on(u, 6, (upper, ax, both, c), x_peer)
                pass_on(u, 8, (lower, 1 - ax, y, c), core_peer)
                pass_on(u, 9, (upper, ax, 1 - y, c), core_peer)
            elif stage == 5:
                wait_for(u, (5, 6))
                pass_on(u, 10, (lower, both, 1 - y, c), core_peer)
                pass_on(u, 11, (upper, 1 - ax, both, c), core_peer)
            else:
                wait_for(u, range(7, 12))

        def z_second(u, stage):
            own_y = [(1, bottom if u != LEAN_UNIT else pl.ds(0, piece))]
            ways = own_y if u == LEAN_UNIT else [(0, top)] + own_y

            def slots(first):
                return [first + way for way, _ in ways]

            def spread(way, at, rows):
                return (at, both, y, c, rows) if way == 0 else (at, ax, both, c, rows)

            if stage == 0:
                for way, rows in ways:
                    pass_on(u, way, (z, ax, y, c, rows), (x_peer, y_peer)[way])
            elif stage == 1:
                wait_for(u, slots(0))
                for way, rows in ways:
                    pass_on(u, 2 + way, spread(way, z, rows), z_next)
            elif stage == 2:
                wait_for(u, slots(2))
                from_inner(u, [(4 + way, spread(way, pair, rows), z_across) for way, rows in ways])
            elif stage == 3:
                wait_where(is_inner, u, slots(4))
                from_inner(u, [(6 + way, spread(way, far_pair, rows), z_next) for way, rows in ways])
            elif stage == 4:
                wait_where(jnp.logical_not(is_inner), u, slots(6))
                for way, rows in ways:
                    pass_on(u, 8 + way, spread(way, every, rows), (y_peer, x_peer)[way])
                for way, rows in ways:
                    pass_on(u, 10 + way, spread(way, every, rows), core_peer)
            elif stage == 5:
                wait_for(u, slots(8))
                for way, rows in ways:
                    part = (every, both, 1 - y, c, rows) if way == 0 else (every, 1 - ax, both, c, rows)
                    pass_on(u, 12 + way, part, core_peer)
            else:
                wait_for(u, slots(10) + slots(12))

        events = [(i + stages - stage, stage) for i in range(-stages, units) for stage in range(stages + 1)]
        events = [(u, stage) for u, stage in events if 0 <= u < units]
        events.remove((1, 0))
        events.insert(1, (1, 0))

        def advance(count):
            for u, stage in events[:count]:
                (z_first if u % Z_FIRST_EVERY == 0 else z_second)(u, stage)
                if (u, stage) == (units - 1, stages - 1):
                    swap_dy.start()
            del events[:count]

        def arrive(i):
            if (i, stages) in events:
                advance(events.index((i, stages)) + 1)
    else:
        def advance(count):
            pass

        def arrive(i):
            if i == units - 2:
                swap_dy.start()
            own[i].wait()

    def columns(u, at):
        return w[u, :, :, :, :, :, at].reshape(width, CHUNK)

    def row_block(u, i):
        return w[u, i].reshape(CHUNK, width)

    def row_pair(u, i):
        return w[u, pl.ds(2 * i, 2)].reshape(2 * CHUNK, width)

    def chunk_pair(i):
        return pl.ds(pl.multiple_of(i * 2 * CHUNK, 2 * CHUNK), 2 * CHUNK)

    def chunk(i):
        return pl.ds(pl.multiple_of(i * CHUNK, CHUNK), CHUNK)

    def tile(i):
        return pl.ds(pl.multiple_of(i * TILE, TILE), TILE)

    def project(u, dst, bias, scale):
        @phase("proj", 0, width // CHUNK)
        def _(i):
            at = chunk(i)
            value = dot_nn(x[...], columns(u, at))
            if bias is not None:
                value = value + par[bias, :, at]
            if scale is not None:
                value = value * scale
            dst[:, at] = value.astype(BF16)

    lane = lax.broadcasted_iota(jnp.int32, (BLOCK, PAIR), 1)
    low_half = lane < PAIR // 2
    row_lane = lax.broadcasted_iota(jnp.int32, (1, PAIR), 1)
    first_head = jnp.where(row_lane < PAIR // 2, 1.0, 0.0).astype(BF16)
    second_head = jnp.where(row_lane < PAIR // 2, 0.0, 1.0).astype(BF16)

    def heads(value):
        return jnp.concatenate([value * first_head, value * second_head], axis=0)

    def merged(value):
        return jnp.where(low_half, value[:BLOCK], value[BLOCK:])

    def softmax(scores, usable):
        scores = jnp.where(usable, scores, MASKED)
        weight = jnp.exp(scores - jnp.max(scores, axis=0, keepdims=True))
        return weight * (1.0 / jnp.sum(weight, axis=0, keepdims=True))

    pairs = width // PAIR
    per_row = width // (2 * BLOCK)
    own_rows = pl.ds(short_rows, 2 * BLOCK)

    def pair_at(h):
        return slice(h * PAIR, (h + 1) * PAIR)

    def short_kept(s, h):
        start = (s % 4) * (pairs // per_row) + h // per_row
        col = h % per_row * 2 * BLOCK
        return s // 4, pl.ds(pl.multiple_of(start * BLOCK, BLOCK), BLOCK), slice(col, col + 2 * BLOCK)

    def long_kept(n, h):
        rows = pl.ds(pl.multiple_of(h // per_row * 4 * BLOCK, 4 * BLOCK), 4 * BLOCK)
        return 2 + n, rows, pl.ds(pl.multiple_of(h % per_row * 2 * BLOCK, 2 * BLOCK), 2 * BLOCK)

    def short_forward(s):
        rows = pl.ds(pl.multiple_of(s * BLOCK, BLOCK), BLOCK)
        usable = lax.broadcasted_iota(jnp.int32, (BLOCK, 2 * BLOCK), 0) < short_len[s]
        for h in range(pairs):
            at = pair_at(h)
            p = softmax(dot_nt(k[rows, at], heads(q[rows, at])), usable).astype(BF16)
            hid[short_kept(s, h)] = p
            g[rows, at] = merged(dot_tn(p, v[rows, at])).astype(BF16)

    def long_usable():
        key = lax.broadcasted_iota(jnp.int32, (4 * BLOCK, 2 * BLOCK), 0)
        block = key // BLOCK
        mine = key + (block + c) * BLOCK
        other = key + (block - 3 - c) * BLOCK
        return jnp.where(block < 2, mine, other) < long_len[y]

    def long_pair(h):
        return pl.ds(pl.multiple_of(h * PAIR, PAIR), PAIR)

    def long_forward(h):
        at = long_pair(h)
        usable = long_usable()
        for n in range(2):
            rows = pl.ds(short_rows + n * BLOCK, BLOCK)
            qm = heads(q[rows, at])
            scores = jnp.concatenate([dot_nt(k[own_rows, at], qm), dot_nt(kv_sib[0, :, at], qm)], axis=0)
            p = softmax(scores, usable).astype(BF16)
            hid[long_kept(n, h)] = p
            o2 = dot_tn(p[: 2 * BLOCK], v[own_rows, at]) + dot_tn(p[2 * BLOCK :], kv_sib[1, :, at])
            g[rows, at] = merged(o2).astype(BF16)

    def norm_parts(value):
        center = value - jnp.mean(value, axis=1, keepdims=True)
        scale = lax.rsqrt(jnp.mean(center * center, axis=1, keepdims=True) + EPSILON)
        return center * scale, scale

    def norm_back(grad, gain, normed, scale):
        grad = grad * gain
        return scale * (
            grad - jnp.mean(grad, axis=1, keepdims=True) - normed * jnp.mean(grad * normed, axis=1, keepdims=True))

    def row_sum(value):
        return jnp.sum(value, axis=0, keepdims=True)

    def add_sum(row, at, value):
        acc[0, row : row + 1, at] += row_sum(value)

    if remote:
        advance(2)
        cast(2, 2)
        cast(3, 3)
        for n in range(hidden_chunks):
            own[4 + n].wait()
        up_rows = [f[(4 + n) * piece : (5 + n) * piece, :].astype(BF16) for n in range(hidden_chunks)]
        for j in range(hidden_chunks):
            w[UP_UNIT + 2 * j, z, ax, y, c] = jnp.concatenate(every_fourth(up_rows, j, lanes, hidden_chunks), axis=1)
            cast(UP_UNIT + 2 * j + 1, 4 + hidden_chunks + j)
    acc[0] = jnp.zeros_like(acc[0])
    tail[...] = jnp.zeros_like(tail)
    for cp in small_loads:
        cp.wait()
    for j in range(hidden_chunks):
        if remote:
            par[U_BIAS + j] = jnp.concatenate(every_fourth([wide_par[...]], j, lanes, hidden_chunks), axis=1)
        else:
            par[U_BIAS + j] = wide_par[:, j * width : (j + 1) * width]
    for cp in loads:
        cp.wait()
    arrive(K_UNIT)
    swap_x.wait_recv()
    project(K_UNIT, k, None, None)
    arrive(V_UNIT)
    project(V_UNIT, v, V_BIAS, None)
    swap_k = misc(2, k.at[own_rows], kv_sib.at[0], core_peer)
    swap_v = misc(3, v.at[own_rows], kv_sib.at[1], core_peer)
    arrive(Q_UNIT)
    swap_k.start()
    swap_v.start()
    project(Q_UNIT, q, Q_BIAS, SCALE)

    for n in range(3):

        @phase("sf", n * nshort // 3, (n + 1) * nshort // 3)
        def _(s):
            short_forward(s)

        if n < 2:
            advance(AHEAD)
        else:
            arrive(O_UNIT)

    swap_k.wait_recv()
    swap_v.wait_recv()
    for n in range(4):

        @phase("lf", n * pairs // 4, (n + 1) * pairs // 4)
        def _(h):
            long_forward(h)

        if n < 3:
            advance(AHEAD)

    swap_k.wait_send()
    swap_v.wait_send()
    park = pltpu.make_async_copy(hid, parked, store_sem.at[4])
    park.start()
    arrive(UP_UNIT)

    @phase("wo", 0, width // CHUNK)
    def _(i):
        at = chunk(i)
        r[:, at] = x[:, at].astype(F32) + dot_nn(g[...], columns(O_UNIT, at)) + par[O_BIAS, :, at]

    advance(AHEAD)

    @phase("ln1", 0, total // TILE)
    def _(i):
        rows = tile(i)
        normed, _ = norm_parts(r[rows, :])
        value = normed * par[GAIN1] + par[SHIFT1]
        a16[rows, :] = value.astype(BF16)
        f[rows, :] = value + par[D_BIAS]

    park.wait()
    for j in range(hidden_chunks):
        up, down = UP_UNIT + 2 * j, UP_UNIT + 2 * j + 1
        if j > 0:
            arrive(up)
        else:
            advance(AHEAD)
        for n in range(2):

            @phase("up", 2 * n, 2 * n + 2)
            def _(i):
                at = chunk(i)
                value = dot_nn(a16[...], columns(up, at)) + par[U_BIAS + j, :, at]
                active, slope = gelu_parts(value)
                hid[j, :, at] = slope.astype(BF16)
                g[:, at] = active.astype(BF16)

            if n == 0:
                advance(AHEAD)

        if j == hidden_chunks - 2:
            for cp in late:
                cp.start()
        arrive(down)

        @phase("down", 0, width // CHUNK)
        def _(i):
            at = chunk(i)
            f[:, at] += dot_nn(g[...], columns(down, at))

    for cp in late:
        cp.wait()
    swap_dy.wait_recv()

    @phase("ln2", 0, total // TILE)
    def _(i):
        rows = tile(i)
        normed, scale = norm_parts(f[rows, :])
        upstream = dy[rows, :].astype(F32)
        dy[rows, :] = (normed * par[GAIN2] + par[SHIFT2]).astype(BF16)
        grad = norm_back(upstream, par[GAIN2], normed, scale)
        f[rows, :] = grad
        a16[rows, :] = grad.astype(BF16)
        add_sum(S_SUM, slice(None), upstream)
        add_sum(D_SUM, slice(None), grad)

    out_copies = [
        pltpu.make_async_copy(dy.at[pl.ds(0, short_rows)], so, store_sem.at[0]),
        pltpu.make_async_copy(dy.at[pl.ds(short_rows + BLOCK * y, BLOCK)], lo.at[y], store_sem.at[1]),
    ]
    for cp in out_copies:
        cp.start()
    swap_out = misc(4, dy.at[pl.ds(short_rows + BLOCK * (1 - y), BLOCK)], lo.at[y], y_peer)
    swap_out.start()

    pair_count = width // (2 * CHUNK)

    @phase("dg", 0, hidden_chunks * pair_count)
    def _(n):
        j = n // pair_count
        i = n % pair_count
        at = chunk_pair(i)
        value = dot_nt(a16[...], row_pair(UP_UNIT + 1 + 2 * j, i)) * hid[j, :, at].astype(F32)
        hid[j, :, at] = value.astype(BF16)
        acc[0, pl.ds(U_SUM + j, 1), at] += row_sum(value)

    @phase("da", 0, width // CHUNK)
    def _(i):
        at = chunk(i)
        value = f[:, at]
        for j in range(hidden_chunks):
            value = value + dot_nt(hid[j], row_block(UP_UNIT + 2 * j, i))
        f[:, at] = value

    unpark = pltpu.make_async_copy(parked, hid, store_sem.at[5])
    unpark.start()

    @phase("ln1b", 0, total // TILE)
    def _(i):
        rows = tile(i)
        normed, scale = norm_parts(r[rows, :])
        upstream = f[rows, :]
        grad = norm_back(upstream, par[GAIN1], normed, scale)
        r[rows, :] = grad
        a16[rows, :] = grad.astype(BF16)
        add_sum(F_SUM, slice(None), upstream)
        add_sum(O_SUM, slice(None), grad)

    def early(n):
        return misc(8 + n, acc.at[n], acc_in.at[n], partners[n])

    def finish_early(n):
        early(n).wait_recv()
        early(n).wait_send()
        acc[n + 1] = acc[n] + acc_in[n]

    def next_early(n):
        if n > 0:
            finish_early(n - 1)
        early(n).start()

    next_early(0)

    @phase("do", 0, width // CHUNK)
    def _(i):
        at = chunk(i)
        g[:, at] = dot_nt(a16[...], row_block(O_UNIT, i)).astype(BF16)

    next_early(1)
    unpark.wait()

    @phase("lb", 0, pairs)
    def _(h):
        at = long_pair(h)
        keys, values = k[own_rows, at], v[own_rows, at]
        keys_far, values_far = kv_sib[0, :, at], kv_sib[1, :, at]
        key_grad = value_grad = query_sum = 0.0
        for n in range(2):
            rows = pl.ds(short_rows + n * BLOCK, BLOCK)
            qm = heads(q[rows, at])
            om = heads(g[rows, at])
            low = hid[long_kept(n, h)]
            p = low.astype(F32)
            back = jnp.concatenate([dot_nt(values, om), dot_nt(values_far, om)], axis=0)
            ds = (p * (back - jnp.sum(back * p, axis=0, keepdims=True))).astype(BF16)
            dq = merged(dot_tn(ds[: 2 * BLOCK], keys) + dot_tn(ds[2 * BLOCK :], keys_far)) * SCALE
            q[rows, at] = dq.astype(BF16)
            query_sum = query_sum + row_sum(dq)
            key_grad = key_grad + dot_nn(ds, qm)
            value_grad = value_grad + dot_nn(low, om)
        k[own_rows, at] = key_grad[: 2 * BLOCK].astype(BF16)
        v[own_rows, at] = value_grad[: 2 * BLOCK].astype(BF16)
        kv_sib[0, :, at] = key_grad[2 * BLOCK :].astype(BF16)
        kv_sib[1, :, at] = value_grad[2 * BLOCK :].astype(BF16)
        tail[Q_SUM : Q_SUM + 1, at] += query_sum
        tail[V_SUM : V_SUM + 1, at] += row_sum(value_grad)

    def short_backward(s):
        rows = pl.ds(pl.multiple_of(s * BLOCK, BLOCK), BLOCK)
        for h in range(pairs):
            at = pair_at(h)
            qm = heads(q[rows, at])
            om = heads(g[rows, at])
            keys = k[rows, at]
            low = hid[short_kept(s, h)]
            p = low.astype(F32)
            back = dot_nt(v[rows, at], om)
            ds = (p * (back - jnp.sum(back * p, axis=0, keepdims=True))).astype(BF16)
            dq = merged(dot_tn(ds, keys)) * SCALE
            dk = dot_nn(ds, qm)
            dv = dot_nn(low, om)
            q[rows, at] = dq.astype(BF16)
            k[rows, at] = dk.astype(BF16)
            v[rows, at] = dv.astype(BF16)
            tail[Q_SUM : Q_SUM + 1, at] += row_sum(dq)
            tail[V_SUM : V_SUM + 1, at] += row_sum(dv)

    next_early(2)

    @phase("sb1", 0, 1)
    def _(s):
        short_backward(s)

    swap_dkv = misc(5, kv_sib, dkv_in, core_peer)
    swap_dkv.start()
    next_early(3)

    @phase("sb2", 1, nshort)
    def _(s):
        short_backward(s)

    steps = len(partners)

    def exchange(slots, me, others, base):
        return [misc(base + n, slots.at[me], slots.at[me], peer) for n, peer in enumerate(others)]

    seq_round = exchange(seq_in, seq, seq_peers, 8 + steps)
    dp_round = exchange(dp_in, dp, dp_peers, 8 + steps + len(seq_peers))
    seq_in[seq] = tail[...]

    for n in range(4, steps):
        next_early(n)
    swap_dkv.wait_recv()
    for cp in seq_round:
        cp.start()
    k[own_rows, :] = (k[own_rows, :].astype(F32) + dkv_in[0].astype(F32)).astype(BF16)
    v[own_rows, :] = (v[own_rows, :].astype(F32) + dkv_in[1].astype(F32)).astype(BF16)

    def input_grad(rows, i):
        at = chunk(i)
        value = r[rows, at]
        for ref, u in ((q, Q_UNIT), (k, K_UNIT), (v, V_UNIT)):
            value = value + dot_nt(ref[rows, :], row_block(u, i))
        x[rows, at] = value.astype(BF16)

    @phase("gxl", 0, width // CHUNK)
    def _(i):
        input_grad(own_rows, i)

    swap_grad = misc(6, x.at[pl.ds(short_rows + BLOCK * (1 - y), BLOCK)], lg.at[y], y_peer)
    swap_grad.start()
    finish_early(steps - 1)
    for cp in seq_round:
        cp.wait_recv()
    dp_in[dp] = sum(seq_in[n] for n in range(1, seq_size)) + seq_in[0]
    for i in range(width // CHUNK):

        @phase("gxs", i, i + 1)
        def _(n):
            input_grad(pl.ds(0, short_rows), n)

        if i == 0:
            for cp in dp_round:
                cp.start()
    for cp in dp_round:
        cp.wait_recv()
    for cp in seq_round + dp_round:
        cp.wait_send()
    sums[0:2, :] = sum(dp_in[n] for n in range(1, dp_size)) + dp_in[0]
    sums[2:6, :] = acc[steps, 0:4, :]
    hidden_sums = [acc[steps, U_SUM + j : U_SUM + j + 1, :] for j in range(hidden_chunks)]
    if remote:
        order = [hidden_sums[j][:, n * lanes : (n + 1) * lanes]
                 for n in range(width // lanes) for j in range(hidden_chunks)]
        up_sums[...] = jnp.concatenate(order, axis=1)
    else:
        up_sums[...] = jnp.concatenate(hidden_sums, axis=1)

    grad_copies = [
        pltpu.make_async_copy(x.at[pl.ds(0, short_rows)], sg, store_sem.at[2]),
        pltpu.make_async_copy(x.at[pl.ds(short_rows + BLOCK * y, BLOCK)], lg.at[y], store_sem.at[3]),
    ]
    for cp in grad_copies:
        cp.start()
    swap_out.wait_recv()
    swap_grad.wait_recv()
    for cp in out_copies + grad_copies:
        cp.wait()
    for cp in (swap_x, swap_dy, swap_out, swap_dkv, swap_grad):
        cp.wait_send()
    for key in sends:
        if key not in inner_sends:
            sends[key].wait_send()
    if inner_sends:
        @pl.when(is_inner)
        def _():
            for key in inner_sends:
                sends[key].wait_send()


def whole_step(shards, small, xs, xl, dys, dyl, short_len, long_len, remote):
    dp_size, seq_size = lax.axis_size("dp"), lax.axis_size("seq")
    width = xs.shape[1]
    nshort = xs.shape[0] // BLOCK
    total = xs.shape[0] + xl.shape[0] * BLOCK
    hidden_chunks = small[-1].shape[1] // width
    units = 4 + 2 * hidden_chunks
    lead = (width // CHUNK, 2, 2, 2, CHUNK // 8, width)
    slots = 14
    steps = (dp_size * seq_size).bit_length() - 1
    exchanges = 8 + steps + seq_size + dp_size
    anywhere = pl.BlockSpec(memory_space=pl.ANY)
    smem = pl.BlockSpec(memory_space=pltpu.SMEM)
    vmem = pl.BlockSpec(memory_space=pltpu.VMEM)
    act = pltpu.VMEM((total, width), BF16)
    wide = pltpu.VMEM((total, width), F32)
    side = pltpu.VMEM((2, 2 * BLOCK, width), BF16)
    dma = pltpu.SemaphoreType.DMA
    return pl.pallas_call(
        functools.partial(step_kernel, remote, dp_size, seq_size, nshort),
        out_shape=(
            jax.ShapeDtypeStruct(xs.shape, BF16),
            jax.ShapeDtypeStruct(xl.shape, BF16),
            jax.ShapeDtypeStruct(xs.shape, BF16),
            jax.ShapeDtypeStruct(xl.shape, BF16),
            jax.ShapeDtypeStruct((8, width), F32),
            jax.ShapeDtypeStruct((1, hidden_chunks * width), F32),
            jax.ShapeDtypeStruct((hidden_chunks, total, width), BF16),
        ),
        in_specs=[anywhere] * (len(shards) + len(small) + 4) + [smem] * 2,
        out_specs=(anywhere,) * 4 + (vmem,) * 2 + (anywhere,),
        scratch_shapes=[
            pltpu.VMEM((U_BIAS + hidden_chunks, 1, width), F32),
            pltpu.VMEM((1, hidden_chunks * width), F32),
            pltpu.VMEM((units, *lead), BF16),
            act, act, act, act, side, side, act, wide, act,
            pltpu.VMEM((hidden_chunks, total, width), BF16),
            wide, act,
            pltpu.VMEM((steps + 1, 4 + hidden_chunks, width), F32),
            pltpu.VMEM((steps, 4 + hidden_chunks, width), F32),
            pltpu.VMEM((2, width), F32),
            pltpu.VMEM((seq_size, 2, width), F32),
            pltpu.VMEM((dp_size, 2, width), F32),
            dma((units, slots)), dma((units, slots)), dma((exchanges,)), dma((exchanges,)),
            dma((units,)), dma((len(small),)), dma((4,)), dma((6,)),
        ],
        compiler_params=pltpu.CompilerParams(
            collective_id=0, has_side_effects=True, vmem_limit_bytes=67043328),
        name="whole_step",
    )(*shards, *small, xs, xl, dys, dyl, short_len, long_len)


def deliver_kernel(so, lo, sg, lg, sums, up_sums, *refs):
    outs, deltas = refs[:4], refs[4:11]
    stages, rows, in_sem, out_sem, row_sem = refs[11:15], refs[15], refs[16], refs[17], refs[18]
    ins = [pltpu.make_async_copy(ref, stage, in_sem.at[n]) for n, (ref, stage) in enumerate(zip((so, lo, sg, lg), stages))]
    gather = pltpu.make_async_copy(sums, rows, row_sem.at[0])
    for cp in ins:
        cp.start()
    gather.start()
    outs = [pltpu.make_async_copy(stage, out, out_sem.at[n]) for n, (stage, out) in enumerate(zip(stages, outs))]
    gather.wait()
    for n in range(6):
        deltas[n][...] = rows[n : n + 1, :]
    deltas[6][...] = up_sums[...]
    for n in range(4):
        ins[n].wait()
        outs[n].start()
    for n in range(4):
        outs[n].wait()


def deliver(so, lo, sg, lg, sums, up_sums):
    anywhere = pl.BlockSpec(memory_space=pl.ANY)
    vmem = pl.BlockSpec(memory_space=pltpu.VMEM)
    width = sums.shape[1]
    big = (so, lo, sg, lg)
    row = jax.ShapeDtypeStruct((1, width), F32)
    dma = pltpu.SemaphoreType.DMA
    return pl.pallas_call(
        deliver_kernel,
        out_shape=tuple(jax.ShapeDtypeStruct(a.shape, a.dtype) for a in big)
        + (row,) * 6 + (jax.ShapeDtypeStruct(up_sums.shape, F32),),
        in_specs=[anywhere] * 5 + [vmem],
        out_specs=(anywhere,) * 4 + (vmem,) * 7,
        scratch_shapes=[pltpu.VMEM(a.shape, a.dtype) for a in big]
        + [pltpu.VMEM(sums.shape, F32), dma((4,)), dma((4,)), dma((1,))],
        name="deliver",
    )(so, lo, sg, lg, sums, up_sums)


def on_device(
    short_input, long_input, short_cotangent, long_cotangent, short_lengths, long_lengths,
    query_weight, key_weight, value_weight, output_weight, upward_weight, downward_weight,
    query_bias, value_bias, output_bias, upward_bias, downward_bias,
    first_gain, first_shift, second_gain, second_shift,
):
    rows, width = query_weight.shape
    devices = lax.axis_size("dp") * lax.axis_size("seq")
    hidden_chunks = upward_weight.shape[1] // width
    shape = short_input.shape

    def permuted(value):
        lead = value.shape[:-1]
        value = value.reshape(*lead, devices, hidden_chunks, rows)
        return jnp.moveaxis(value, -2, 0).reshape(hidden_chunks, *lead, width)

    remote = rows == 32 and lax.axis_size("seq") == 4
    small = [query_bias, value_bias, output_bias, downward_bias, first_gain, first_shift, second_gain, second_shift]
    if remote:
        shards = [key_weight, value_weight, query_weight, output_weight, upward_weight, downward_weight]
        small.append(upward_bias)
    else:
        upward = permuted(upward_weight)
        downward = downward_weight.reshape(hidden_chunks, rows, width)
        parts = [key_weight, value_weight, query_weight, output_weight]
        for j in range(hidden_chunks):
            parts += [upward[j], downward[j]]
        whole = lax.all_gather(jnp.stack([part.astype(BF16) for part in parts]), ("dp", "seq"), axis=1, tiled=True)
        shards = [whole.reshape(len(parts), width // CHUNK, 2, 2, 2, CHUNK // 8, width)]
        small.append(permuted(upward_bias))
    so, lo, sg, lg, sums, up_sums, _ = whole_step(
        shards, [value.reshape(1, -1) for value in small],
        short_input.reshape(-1, width), long_input, short_cotangent.reshape(-1, width), long_cotangent,
        short_lengths, long_lengths, remote)
    so, lo, sg, lg, *deltas = deliver(so, lo, sg, lg, sums, up_sums)
    up_sums = deltas[6]
    if remote:
        upward_delta = up_sums.reshape(-1)
    else:
        upward_delta = jnp.moveaxis(up_sums.reshape(hidden_chunks, devices, rows), 0, 1).reshape(-1)
    query_delta, value_delta, output_delta, downward_delta, first_delta, second_delta = (value.reshape(-1) for value in deltas[:6])
    return (
        so.reshape(shape), lo, sg.reshape(shape), lg,
        query_delta, value_delta, output_delta, upward_delta, downward_delta, first_delta, second_delta,
    )


def solution(mesh):
    split = ("dp", "seq")
    placed = (
        P(split, None, None), P("dp", "seq", None), P(split, None, None), P("dp", "seq", None),
        P(split), P("dp"),
        *(P(split, None) for _ in range(6)), *(P() for _ in range(9)),
    )
    return jax.shard_map(
        on_device,
        mesh=mesh,
        in_specs=placed,
        out_specs=(
            P(split, None, None), P("dp", "seq", None), P(split, None, None), P("dp", "seq", None),
            *(P() for _ in range(7)),
        ),
        check_vma=False,
    )
```
